32 devices in a mesh: groups: 2 (over y), chan: 8 (over z, x), sub: 2 (over core).
Axes of the slice: x: 2, y: 2, z: 4, core: 2. Of those that a mesh axis runs over, the one named last changes fastest.
Arguments:
- predicted_sky_response: bfloat16 [16384, 8, 2, 128], P(('groups', 'chan', 'sub')), parts along dimension 0, may hold values from -0.4375 to 0.4375
- measured_correlation: bfloat16 [16384, 2, 128], P(('groups', 'chan', 'sub')), parts along dimension 0, may hold values from -6 to 6
- keep_indicator: int32 [16384, 128], P(('groups', 'chan', 'sub')), parts along dimension 0, may hold values 0 or 1
- tile_owner: int32 [16384, 1], P(('groups', 'chan', 'sub')), parts along dimension 0, may hold values from 0 to 7; in each aligned block of 512 rows (0 to 511, 512 to 1023, ...) at most 192 rows name the same one
- tile_channel: int32 [16384], P(('groups', 'chan', 'sub')), parts along dimension 0, may hold values from 0 to 3
- tile_base: int32 [16384], P(('groups', 'chan', 'sub')), parts along dimension 0, may hold values from 0 to 14
- pairs: int32 [15, 2, 128], replicated, may hold values from 0 to 61, as said below
- gains: float32 [64, 2, 62, 8], P(('groups', 'chan')), parts along dimension 0, may hold values from -5 to 5
- duals: float32 [64, 2, 62, 8], P(('groups', 'chan', 'sub')), parts along dimension 0, may hold values from -4 to 4
- consensus: float32 [8, 2, 62, 8], P('groups'), parts along dimension 0, may hold values from -5 to 5
- rho: float32 [8], replicated, may hold values from 0.3 to 3
Outputs:
- gains_new: float32 [64, 2, 62, 8], P(('groups', 'chan', 'sub')), parts along dimension 0
- consensus_new: float32 [8, 2, 62, 8], P('groups'), parts along dimension 0
- duals_new: float32 [64, 2, 62, 8], P(('groups', 'chan', 'sub')), parts along dimension 0
The draws below stay inside these ranges and needn't reach their ends.
There are 2 independent parts, one for each index of `groups`. The reference program is written for one: setup_inputs(seed, part) draws one part's arguments, and reference() takes and returns one part's arrays. A program takes and returns all parts, laid end to end along the dimension named above; an argument that names none is the same for every part. Nothing has to cross between parts.
Inputs may be any that keep to these rules, and one draw needn't show every extreme that they name: `tile_owner`: on the tiles of one device at most 192 name the same owner, a bound that some block reaches. `pairs`: the two stations of a row differ.
All inputs are finite; a program needn't handle non-finite values. No bound on the sum of `keep_indicator` on one device may be relied on, other than what follows from the above.
Results may differ from the reference program's by a relative error of at most 0.0027.
Values may be sent and summed in bfloat16 or wider, within the bound.
A program may use at most 128 MiB of HBM per device.

```python
import math
import jax
import jax.numpy as jnp
import numpy as np
from jax import lax

NS = 62
K = 8
DEG = 4
TR = 128
BT = 15
CH_DEV = 4
TILES_DEV = 512
F = 32
TILES = 8192
CAP = 192
ROWS_CH = 32768
N_CHAN = 8


def draw_pairs(key, part):
    key_first, key_offset = jax.random.split(jax.random.fold_in(key, 17))
    first_station = jax.random.randint(key_first, (BT, TR), 0, NS)
    offset = jax.random.randint(key_offset, (BT, TR), 1, NS)
    station_second = (first_station + offset) % NS
    return jnp.stack([first_station, station_second], axis=1).astype(jnp.int32)


def touch_ends(result, own_key, smallest, top_value):
    longest = result.shape.index(max(result.shape))
    spots = []
    for shift in (0, 1):
        where = [jax.random.randint(jax.random.fold_in(own_key, axis), (), 0, length) for axis, length in enumerate(result.shape)]
        where[longest] = (where[longest] + shift) % result.shape[longest]
        spots.append(tuple(where))
    return result.at[spots[0]].set(smallest).at[spots[1]].set(top_value)


def block_scale(rng, extent, pieces, low, top_value):
    factor_of, own = 1.0, jax.random.fold_in(rng, 6)
    for position, blocks in pieces:
        steps = jnp.exp(jax.random.uniform(jax.random.fold_in(own, position), (blocks,), jnp.float32, low / len(pieces), top_value / len(pieces)))
        factor_of = factor_of * jnp.repeat(steps, extent[position] // blocks).reshape([-1 if axis == position else 1 for axis in range(len(extent))])
    return factor_of


def assign_block(own_key, own, number, rows, number_of, top, bound, skew):
    order = jax.random.permutation(own_key, number_of)
    heavy_load, common = load_shares(number_of, rows * top, bound, skew, True), load_shares(number_of, rows * top, bound, skew, False)
    places = jnp.arange(number_of)

    def named(tallies, rotation):
        used = int((tallies > 0).sum())
        fixed = max(1, used // 4)
        passed = fixed + (places - fixed + rotation * (used - fixed)) % max(1, number_of - fixed)
        return jnp.zeros((number_of,), jnp.int32).at[order[jnp.where(places < fixed, places, passed)]].set(jnp.asarray(tallies, jnp.int32))

    tallies = jnp.where(number % 4 == 0, named(heavy_load, number // 4), named(common, number - number // 4 - 1))
    mixed = jax.random.permutation(jax.random.fold_in(own, 3), number_of)
    giver, taker = mixed[0:number_of // 2 * 2:2], mixed[1:number_of // 2 * 2:2]
    room = jnp.minimum(tallies[giver] - 1, bound - tallies[taker]) // 2
    room = jnp.where((giver == order[0]) | (taker == order[0]) | (tallies[taker] == 0), 0, jnp.maximum(room, 0))
    passed = jax.random.randint(jax.random.fold_in(own, 4), (number_of // 2,), 0, 1 << 20) % (room + 1)
    tallies = tallies.at[giver].add(-passed).at[taker].add(passed)
    members = jnp.searchsorted(jnp.cumsum(tallies), jnp.arange(rows * top), side="right").astype(jnp.int32)
    table = members.reshape(top, rows).T
    table = table[jax.random.permutation(jax.random.fold_in(own, 1), rows)]
    rotation = jax.random.randint(jax.random.fold_in(own, 2), (rows, 1), 0, top)
    return jnp.take_along_axis(table, (jnp.arange(top)[None, :] + rotation) % top, axis=1)


def load_shares(count, total, most, skew, full):
    loads = [(1 << 20) // math.isqrt(grade ** skew) + 1 for grade in range(1, count + 1)]
    largest = most if full else min(most, max(-(-total // count), total * loads[0] // sum(loads)))
    least = 1 if total - largest >= count - 1 else 0
    given, rest = [largest] + [least] * (count - 1), total - largest - least * (count - 1)
    while rest > 0:
        movable = [i for i in range(1, count) if given[i] < largest] or [i for i in range(1, count) if given[i] < most]
        mass, remaining = sum([loads[i] for i in movable]), rest
        for i in movable:
            more = min(most - given[i], max(1, remaining * loads[i] // mass), rest)
            given[i] = given[i] + more
            rest = rest - more
    return np.array(given)


def scatter_about(key, shape, width, most, shards=(), kind=jnp.bfloat16):
    result = jax.random.normal(key, shape, jnp.float32) * width
    if len(shards) > 0:
        result = block_scale(key, shape, shards, -0.22, 0.18) * result
    return jnp.clip(result, min=-most, max=most).astype(kind)


def setup_inputs(seed: int = 0, part: int = 0) -> dict:
    arg_keys = jax.random.split(jax.random.key(seed), 12)
    own_keys = jax.random.split(jax.random.fold_in(arg_keys[11], part), 12)
    predicted_sky_response = scatter_about(own_keys[0], (TILES, K, 2, TR), ((2 * ROWS_CH // NS) ** -0.5), 0.4375, ((0, 16),))
    measured_correlation = scatter_about(own_keys[1], (TILES, 2, TR), 1.0, 6.0, ((0, 16),))
    keep_indicator = touch_ends((jax.random.randint(own_keys[2], (TILES, TR), 0, 4) < 3).astype(jnp.int32), jax.random.fold_in(own_keys[2], 1), 0, 1)
    tile_owner_keys = jax.random.split(jax.random.fold_in(own_keys[3], 1), TILES // TILES_DEV)
    tile_owner_turns = jax.random.permutation(jax.random.fold_in(own_keys[3], 3), TILES // TILES_DEV)
    tile_owner = jax.vmap(lambda own, number: assign_block(jax.random.fold_in(own_keys[3], 2), own, number, TILES_DEV, N_CHAN, 1, CAP, 2))(tile_owner_keys, tile_owner_turns).reshape((TILES, 1))
    tile_channel = touch_ends(jax.random.randint(own_keys[4], (TILES,), 0, CH_DEV), jax.random.fold_in(own_keys[4], 1), 0, CH_DEV - 1).astype(jnp.int32)
    tile_base = touch_ends(jax.random.randint(own_keys[5], (TILES,), 0, BT), jax.random.fold_in(own_keys[5], 1), 0, BT - 1).astype(jnp.int32)
    pairs = draw_pairs(jax.random.fold_in(arg_keys[11], 71), part)
    gains = scatter_about(own_keys[7], (F, 2, NS, K), 0.8, 5.0, ((0, 8),), jnp.float32)
    duals = scatter_about(own_keys[8], (F, 2, NS, K), 0.3, 4.0, ((0, 16),), jnp.float32)
    consensus = scatter_about(own_keys[9], (DEG, 2, NS, K), 0.5, 5.0, (), jnp.float32)
    rho = jnp.clip(jnp.exp(jax.random.uniform(arg_keys[10], (K,), jnp.float32, math.log(0.3), math.log(3.0))), 0.3, 3.0)
    return dict(predicted_sky_response=predicted_sky_response, measured_correlation=measured_correlation, keep_indicator=keep_indicator, tile_owner=tile_owner, tile_channel=tile_channel, tile_base=tile_base, pairs=pairs, gains=gains, duals=duals, consensus=consensus, rho=rho)


def legendre_rows(channels):
    positions = jnp.arange(channels, dtype=jnp.float32)
    abscissa = (2.0 * positions - (channels - 1)) / max(channels - 1, 1)
    return jnp.stack([jnp.ones_like(abscissa), abscissa, 0.5 * (3.0 * abscissa * abscissa - 1.0), 0.5 * (5.0 * abscissa * abscissa * abscissa - 3.0 * abscissa)])

def outer_terms(vector_real, vector_imag, weight_real, weight_imag):
    tiles_count, row_total_count, directions = vector_real.shape
    outer_real = vector_real[..., :, None] * vector_real[..., None, :] + vector_imag[..., :, None] * vector_imag[..., None, :]
    outer_imag = vector_real[..., :, None] * vector_imag[..., None, :] - vector_imag[..., :, None] * vector_real[..., None, :]
    normal = jnp.stack([outer_real, outer_imag], axis=2).reshape(tiles_count, row_total_count, 2 * directions * directions)
    side_real = vector_real * weight_real[..., None] + vector_imag * weight_imag[..., None]
    side_imag = vector_real * weight_imag[..., None] - vector_imag * weight_real[..., None]
    right_side = jnp.stack([side_real, side_imag], axis=2).reshape(tiles_count, row_total_count, 2 * directions)
    return (normal, right_side)

def row_terms(coupling, observed, near_gain, far_gain):
    coupling_real = jnp.swapaxes(coupling[:, :, 0, :], 1, 2).astype(jnp.float32)
    coupling_imag = jnp.swapaxes(coupling[:, :, 1, :], 1, 2).astype(jnp.float32)
    near_real, near_imag = (near_gain[:, :, 0, :], near_gain[:, :, 1, :])
    far_real, far_imag = (far_gain[:, :, 0, :], far_gain[:, :, 1, :])
    slope_real = coupling_real * far_real + coupling_imag * far_imag
    slope_imag = coupling_imag * far_real - coupling_real * far_imag
    mirror_real = coupling_real * near_real - coupling_imag * near_imag
    mirror_imag = -(coupling_real * near_imag + coupling_imag * near_real)
    model_real = jnp.sum(near_real * slope_real - near_imag * slope_imag, axis=-1)
    model_imag = jnp.sum(near_real * slope_imag + near_imag * slope_real, axis=-1)
    observed_f = observed.astype(jnp.float32)
    residual_real = observed_f[:, 0, :] - model_real
    residual_imag = observed_f[:, 1, :] - model_imag
    normal_near, right_near = outer_terms(slope_real, slope_imag, residual_real, residual_imag)
    normal_far, right_far = outer_terms(mirror_real, mirror_imag, residual_real, -residual_imag)
    normal = jnp.concatenate([normal_near, normal_far], axis=1).astype(jnp.bfloat16)
    right_side = jnp.concatenate([right_near, right_far], axis=1).astype(jnp.bfloat16)
    return (normal, right_side)

def admm_update(normal, right_side, gain, dual, anchor, rho):
    count, stations = (normal.shape[0], normal.shape[1])
    directions = rho.shape[0]
    normal_blocks = normal.reshape(count, stations, 2, directions, directions)
    ridge_diag = jnp.diag(rho)
    higher_half_records = jnp.concatenate([normal_blocks[:, :, 0] + ridge_diag, -normal_blocks[:, :, 1]], axis=-1)
    lower_rows = jnp.concatenate([normal_blocks[:, :, 1], normal_blocks[:, :, 0] + ridge_diag], axis=-1)
    system = jnp.concatenate([higher_half_records, lower_rows], axis=-2)
    gain_rows = jnp.transpose(gain, (0, 2, 1, 3))
    dual_rows = jnp.transpose(dual, (0, 2, 1, 3))
    anchor_rows = jnp.transpose(anchor, (0, 2, 1, 3))
    target = right_side.reshape(count, stations, 2, directions) - dual_rows - rho * (gain_rows - anchor_rows)
    factor = jnp.linalg.cholesky(system)
    gain_step = jax.scipy.linalg.cho_solve((factor, True), target.reshape(count, stations, 2 * directions)[..., None])[..., 0]
    return gain + jnp.transpose(gain_step.reshape(count, stations, 2, directions), (0, 2, 1, 3))

def fit_consensus(poly_basis, summed):
    gram_matrix = jnp.dot(poly_basis, poly_basis.T, precision=lax.Precision.HIGHEST)
    factor = jnp.linalg.cholesky(gram_matrix)
    coeffs = jax.scipy.linalg.cho_solve((factor, True), summed.reshape(summed.shape[0], -1))
    return coeffs.reshape(summed.shape)

def reference(predicted_sky_response, measured_correlation, keep_indicator, tile_owner, tile_channel, tile_base, pairs, gains, duals, consensus, rho):
    channels = CH_DEV * N_CHAN
    retained_selector = keep_indicator > 0
    predicted_response_kept = jnp.where(retained_selector[:, None, None, :], predicted_sky_response, jnp.zeros_like(predicted_sky_response))
    measured_correlation_kept = jnp.where(retained_selector[:, None, :], measured_correlation, jnp.zeros_like(measured_correlation))
    channel_lookup = (tile_owner[:, 0] * CH_DEV + tile_channel).astype(jnp.int32)
    gain_table = jnp.transpose(gains, (0, 2, 1, 3))
    iteration_tally = predicted_sky_response.shape[0] // TILES_DEV
    normal_matrix_width = 2 * K * K

    def one_block(totals, block_item):
        normal_acc, right_acc = totals
        block_coherency, block_visibility, block_channel, block_base = block_item
        stations = pairs[block_base]
        first_station = stations[:, 0, :]
        station_second = stations[:, 1, :]
        near_gain = gain_table[block_channel[:, None], first_station]
        far_gain = gain_table[block_channel[:, None], station_second]
        normal, right_side = row_terms(block_coherency, block_visibility, near_gain, far_gain)
        normal = lax.optimization_barrier(normal).astype(jnp.float32)
        right_side = lax.optimization_barrier(right_side).astype(jnp.float32)
        segment_ids = (jnp.concatenate([first_station, station_second], axis=1) + block_channel[:, None] * NS).astype(jnp.int32)
        normal_acc = normal_acc + jax.ops.segment_sum(normal.reshape(-1, normal_matrix_width), segment_ids.reshape(-1), num_segments=channels * NS)
        right_acc = right_acc + jax.ops.segment_sum(right_side.reshape(-1, 2 * K), segment_ids.reshape(-1), num_segments=channels * NS)
        return ((normal_acc, right_acc), None)
    block_items = (predicted_response_kept.reshape((iteration_tally, TILES_DEV) + predicted_sky_response.shape[1:]), measured_correlation_kept.reshape((iteration_tally, TILES_DEV) + measured_correlation.shape[1:]), channel_lookup.reshape(iteration_tally, TILES_DEV), tile_base.reshape(iteration_tally, TILES_DEV))
    start_totals = (jnp.zeros((channels * NS, normal_matrix_width), jnp.float32), jnp.zeros((channels * NS, 2 * K), jnp.float32))
    (normal_sum, right_sum), _ = lax.scan(one_block, start_totals, block_items)
    normal_sum = normal_sum.reshape(channels, NS, normal_matrix_width)
    right_sum = right_sum.reshape(channels, NS, 2 * K)
    poly_basis = legendre_rows(channels)
    anchor = jnp.einsum('df,dcsk->fcsk', poly_basis, consensus, precision=lax.Precision.HIGHEST)
    gains_new = admm_update(normal_sum, right_sum, gains, duals, anchor, rho)
    summed = jnp.einsum('df,fcsk->dcsk', poly_basis, gains_new + duals / rho, precision=lax.Precision.HIGHEST)
    consensus_new = fit_consensus(poly_basis, summed)
    duals_new = duals + rho * (gains_new - jnp.einsum('df,dcsk->fcsk', poly_basis, consensus_new, precision=lax.Precision.HIGHEST))
    return (gains_new, consensus_new, duals_new)
```

```python
import functools

import jax
import jax.numpy as jnp
import numpy as np
from jax import lax
from jax.experimental import pallas as pl
from jax.experimental.pallas import tpu as pltpu
from jax.sharding import PartitionSpec as P

LANES = 128
GROUP = 4
UNROLL = 20


def lay_pair(load, pad, half, width):
    total = None
    for part in range(half):
        block = load(part)
        pad[part % 2, :, : block.shape[1]] = block
        value = pad[part % 2]
        if part:
            value = pltpu.roll(value, part * width, axis=1)
        total = value if total is None else total + value
    return total


def basis_of(channel, channels):
    x = (2.0 * channel - (channels - 1)) / max(channels - 1, 1)
    return [
        jnp.ones_like(x),
        x,
        0.5 * (3.0 * x * x - 1.0),
        0.5 * (5.0 * x * x * x - 3.0 * x),
    ]


def inverse_gram(channels):
    f = np.arange(channels, dtype=np.float64)
    x = (2.0 * f - (channels - 1)) / max(channels - 1, 1)
    basis = np.stack([np.ones_like(x), x, 0.5 * (3 * x * x - 1), 0.5 * (5 * x * x * x - 3 * x)])
    return np.linalg.inv(basis @ basis.T)


def hermitian_rows(real, imag, upper, sign):
    half = real.shape[0] // 2
    groups_real = [real * real + imag * imag]
    groups_imag = []
    for shift in range(1, half + 1):
        turned_real = pltpu.roll(real, 2 * half - shift, axis=0)
        turned_imag = pltpu.roll(imag, 2 * half - shift, axis=0)
        groups_real.append(real * turned_real + imag * turned_imag)
        if sign > 0:
            groups_imag.append(real * turned_imag - imag * turned_real)
        else:
            groups_imag.append(imag * turned_real - real * turned_imag)
    mixed = jnp.where(upper, groups_real.pop(), groups_imag.pop())
    return groups_real + groups_imag + [mixed]


def solve_hermitian(groups_real, groups_imag, mixed, ridge, side_real, side_imag):
    directions = side_real.shape[0]
    middle = directions // 2
    row = lax.broadcasted_iota(jnp.int32, side_real.shape, 0)
    upper = row < middle
    swapped = pltpu.roll(mixed, middle, axis=0)
    real = {0: groups_real[0] + ridge, middle: jnp.where(upper, mixed, swapped)}
    imag = {0: jnp.zeros_like(ridge), middle: jnp.where(upper, -swapped, mixed)}
    for d in range(1, middle):
        real[d], imag[d] = groups_real[d], groups_imag[d - 1]
        real[directions - d] = pltpu.roll(groups_real[d], d, axis=0)
        imag[directions - d] = -pltpu.roll(groups_imag[d - 1], d, axis=0)
    columns = []
    for l in range(directions):
        column_real, column_imag = real[l], imag[l]
        for k in range(1, directions):
            here = row == k
            d = (l - k) % directions
            column_real = jnp.where(here, real[d], column_real)
            column_imag = jnp.where(here, imag[d], column_imag)
        columns.append((column_real, column_imag))
    columns.append((side_real, side_imag))
    scale = jnp.zeros_like(ridge)
    for j in range(directions):
        pivot_real, pivot_imag = columns[j]
        inverse = 1.0 / pivot_real[j : j + 1]
        here = row == j
        scale = jnp.where(here, jnp.broadcast_to(inverse, scale.shape), scale)
        factor_real = jnp.where(here, 0.0, pivot_real * inverse)
        factor_imag = jnp.where(here, 0.0, pivot_imag * inverse)
        for l in range(j + 1, directions + 1):
            value_real, value_imag = columns[l]
            head_real, head_imag = value_real[j : j + 1], value_imag[j : j + 1]
            columns[l] = (
                value_real - (factor_real * head_real - factor_imag * head_imag),
                value_imag - (factor_real * head_imag + factor_imag * head_real),
            )
    return columns[-1][0] * scale, columns[-1][1] * scale


def encode(sums, directions):
    normal_rows = directions * directions
    side = sums[normal_rows:]
    high = side.astype(jnp.bfloat16)
    low = (side - high.astype(jnp.float32)).astype(jnp.bfloat16)
    return jnp.concatenate([sums[:normal_rows].astype(jnp.bfloat16), high, low], axis=0)


def decode(coded, directions):
    wide = coded.astype(jnp.float32)
    normal_rows = directions * directions
    side_rows = 2 * directions
    high, low = wide[normal_rows : normal_rows + side_rows], wide[normal_rows + side_rows :]
    return jnp.concatenate([wide[:normal_rows], high + low], axis=0)


def sort_tiles(owner, channel, base, codes, owners, sub_count, half, groups, entries):
    tiles = owner.shape[1]
    slots = groups * GROUP
    sub = jnp.zeros_like(channel)
    for number in range(1, sub_count):
        sub = sub + jnp.where(channel >= number * half, 1, 0)
    place = channel - sub * half
    key = owner * sub_count + sub
    entry = base * half + place
    same = jnp.where(
        lax.broadcasted_iota(jnp.int32, (owners, tiles), 0) == jnp.broadcast_to(key, (owners, tiles)), 1.0, 0.0
    )
    same_b = same.astype(jnp.bfloat16)
    until = jnp.where(
        lax.broadcasted_iota(jnp.int32, (tiles, tiles), 0) <= lax.broadcasted_iota(jnp.int32, (tiles, tiles), 1),
        1.0,
        0.0,
    ).astype(jnp.bfloat16)
    nt = (((1,), (1,)), ((), ()))
    count = jnp.dot(same_b, until, preferred_element_type=jnp.float32)

    def pieces(value):
        return jnp.floor((value + float(GROUP - 1)) * (1.0 / GROUP))

    wide = (owners, LANES)
    used = pieces(jnp.broadcast_to(count[:, tiles - 1 : tiles], wide))
    square = (owners, owners)
    row, column = lax.broadcasted_iota(jnp.int32, square, 0), lax.broadcasted_iota(jnp.int32, square, 1)
    before = jnp.where(column < row, 1.0, 0.0).astype(jnp.bfloat16)
    start = jnp.dot(before, used.astype(jnp.bfloat16), preferred_element_type=jnp.float32)
    position = jnp.sum(same * (start[:, :1] * float(GROUP) + count), axis=0, keepdims=True) - 1.0
    left = tiles - lax.broadcasted_iota(jnp.int32, (1, tiles), 1)
    features = jnp.concatenate(
        [left & 255, lax.shift_right_logical(left, 8), entry, key, jnp.zeros((4, tiles), jnp.int32)], axis=0
    )
    chosen = jnp.where(
        lax.broadcasted_iota(jnp.int32, (slots, tiles), 0)
        == jnp.broadcast_to(position.astype(jnp.int32), (slots, tiles)),
        1.0,
        0.0,
    ).astype(jnp.bfloat16)
    sorted_features = lax.dot_general(
        features.astype(jnp.float32).astype(jnp.bfloat16), chosen, nt, preferred_element_type=jnp.float32
    )
    tile = float(tiles) - (sorted_features[0:1] + 256.0 * sorted_features[1:2])
    codes[0:1, :slots] = jnp.clip(tile.astype(jnp.int32), 0, tiles)
    codes[1:2, :slots] = jnp.clip(sorted_features[2:3].astype(jnp.int32), 0, entries - 1)
    codes[2:3, :slots] = jnp.clip(sorted_features[3:4].astype(jnp.int32), 0, owners - 1)
    spread = -(-groups // LANES) * LANES
    number = lax.broadcasted_iota(jnp.int32, (owners, spread), 1).astype(jnp.float32)
    first = (jnp.broadcast_to(start[:, :1], number.shape) == number) & (
        jnp.broadcast_to(used[:, :1], number.shape) > 0.5
    )
    carried = 1.0 - jnp.max(jnp.where(first, 1.0, 0.0), axis=0, keepdims=True)
    codes[3:4, :spread] = carried.astype(jnp.int32)
    used_row = pieces(lax.dot_general(jnp.ones((8, tiles), jnp.bfloat16), same_b, nt, preferred_element_type=jnp.float32))
    upto = jnp.where(row <= column, 1.0, 0.0).astype(jnp.bfloat16)
    end = jnp.dot(used_row.astype(jnp.bfloat16), upto, preferred_element_type=jnp.float32)
    last = jnp.where(used_row > 0.5, end, 0.0).astype(jnp.int32)
    codes[4:5, :owners] = jnp.clip(last[0:1], 0, groups)


def whole_kernel(
    chan_count,
    sub_count,
    half,
    groups,
    rho_ref,
    owner_hbm,
    channel_hbm,
    base_hbm,
    coupling_hbm,
    observed_hbm,
    keep_hbm,
    pairs_hbm,
    gains_hbm,
    duals_hbm,
    consensus_hbm,
    out_ref,
    owner_ref,
    channel_ref,
    base_ref,
    coupling_ref,
    observed_ref,
    keep_ref,
    pairs_ref,
    gains_ref,
    duals_ref,
    consensus_ref,
    gain_table,
    table,
    turned,
    stations_of,
    coupling_f,
    observed_f,
    lane_mask,
    codes_v,
    codes,
    sums_ref,
    pad,
    near_src,
    near_buf,
    send_buf,
    far_buf,
    weights,
    basis_buf,
    local_sem,
    gains_send,
    gains_recv,
    near_send,
    near_recv,
    far_send,
    far_recv,
    last_send,
    last_recv,
):
    chan, sub = lax.axis_index("chan"), lax.axis_index("sub")
    owners = chan_count * sub_count
    channels = owners * half
    width = LANES // half
    directions, stations = duals_ref.shape[2], duals_ref.shape[3]
    degree = consensus_ref.shape[0]
    tiles = keep_ref.shape[0]
    tile_rows = keep_ref.shape[1]
    bases = pairs_ref.shape[0]
    me = chan * sub_count + sub
    mesh_id = pl.DeviceIdType.MESH

    def device(flat):
        return {"chan": lax.div(flat, sub_count), "sub": lax.rem(flat, sub_count)}

    barrier = pltpu.get_barrier_semaphore()
    for offset in range(1, owners):
        pl.semaphore_signal(
            barrier, inc=1, device_id=device(lax.rem(me + offset, owners)), device_id_type=mesh_id
        )

    loads = []
    for number, (source, target) in enumerate(
        [
            (gains_hbm, gains_ref),
            (owner_hbm, owner_ref),
            (channel_hbm, channel_ref),
            (base_hbm, base_ref),
            (pairs_hbm, pairs_ref),
            (coupling_hbm, coupling_ref),
            (observed_hbm, observed_ref),
            (keep_hbm, keep_ref),
            (duals_hbm, duals_ref),
            (consensus_hbm, consensus_ref),
        ]
    ):
        copy = pltpu.make_async_copy(source, target, local_sem.at[number])
        copy.start()
        loads.append(copy)

    pad[...] = jnp.zeros_like(pad)
    loads[0].wait()
    for owner in range(sub_count):
        for part in range(2):
            gain_table[me - sub + owner, part] = lay_pair(
                lambda number: gains_ref[owner * half + number, part], pad, half, width
            )
    pl.semaphore_wait(barrier, owners - 1)
    gathers = []
    for offset in range(1, chan_count):
        mine_here = gain_table.at[pl.ds(chan * sub_count, sub_count)]
        copy = pltpu.make_async_remote_copy(
            src_ref=mine_here,
            dst_ref=mine_here,
            send_sem=gains_send.at[offset],
            recv_sem=gains_recv.at[offset],
            device_id={"chan": lax.rem(chan + offset, chan_count)},
            device_id_type=mesh_id,
        )
        copy.start()
        gathers.append(copy)

    for copy in loads[1:4]:
        copy.wait()
    codes_v[...] = jnp.zeros_like(codes_v)
    sort_tiles(owner_ref[...], channel_ref[...], base_ref[...], codes_v, owners, sub_count, half, groups, bases * half)
    to_scalar = pltpu.make_async_copy(codes_v, codes, local_sem.at[len(loads)])
    to_scalar.start()

    loads[4].wait()
    turned[...] = jnp.zeros_like(turned)
    for base in range(bases):
        both = pairs_ref[base]
        turned[2 * base : 2 * base + 2, :] = both.astype(jnp.float32)
        for part in range(half):
            stations_of[base * half + part] = both + part * width
    columns = jnp.transpose(turned[...])
    lane = lax.broadcasted_iota(jnp.int32, (tile_rows, LANES), 1).astype(jnp.float32)
    for base in range(bases):
        for end in range(2):
            station = jnp.broadcast_to(columns[:, 2 * base + end : 2 * base + end + 1], lane.shape)
            for part in range(half):
                table[base * half + part, end * tile_rows : (end + 1) * tile_rows, :] = jnp.where(
                    station == lane - float(part * width), 1.0, 0.0
                ).astype(jnp.bfloat16)

    for copy in loads[5:]:
        copy.wait()
    step_rows = 2 * directions

    def widen(step, carry):
        span = pl.ds(pl.multiple_of(step * 8 * step_rows, 8 * step_rows), 8 * step_rows)
        coupling_f[span, :] = coupling_ref[span, :].astype(jnp.float32)
        return carry

    lax.fori_loop(0, tiles // 8, widen, 0)
    coupling_f[tiles * step_rows :, :] = jnp.zeros((8 * step_rows, tile_rows), jnp.float32)
    observed_f[: 2 * tiles, :] = observed_ref[...].astype(jnp.float32)
    observed_f[2 * tiles :, :] = jnp.zeros((8, tile_rows), jnp.float32)
    lane_mask[:tiles, :] = jnp.where(keep_ref[...] > 0, 0, width - 1)
    lane_mask[tiles:, :] = jnp.zeros((8, tile_rows), jnp.int32)

    shape = (directions, LANES)
    row = lax.broadcasted_iota(jnp.int32, shape, 0)
    rho = jnp.zeros(shape, jnp.float32)
    for k in range(directions):
        rho = jnp.where(row == k, rho_ref[k], rho)
    place = lax.broadcasted_iota(jnp.int32, (owners, LANES), 1)
    of = lax.broadcasted_iota(jnp.int32, (owners, LANES), 0)
    everyone = basis_of((of * half + lax.div(place, width)).astype(jnp.float32), channels)
    for d in range(degree):
        basis_buf[d] = everyone[d]

    normal_rows = directions * directions
    out_rows = normal_rows + 2 * directions
    sums_ref[0] = jnp.zeros((out_rows, LANES), jnp.float32)
    upper = row < directions // 2
    to_scalar.wait()
    for copy in gathers:
        copy.wait_recv()

    def spread(values):
        return jnp.broadcast_to(values, shape)

    def pick(values, index):
        return jnp.take_along_axis(values, index, axis=1, mode="promise_in_bounds")

    def one_tile(slot):
        tile = jnp.clip(codes[0, slot], 0, tiles)
        entry = jnp.clip(codes[1, slot], 0, bases * half - 1)
        owner = jnp.clip(codes[2, slot], 0, owners - 1)
        first = tile * step_rows
        real = coupling_f[pl.ds(first, directions, stride=2), :]
        imag = coupling_f[pl.ds(first + 1, directions, stride=2), :]
        seen_real = spread(observed_f[pl.ds(2 * tile, 1), :])
        seen_imag = spread(observed_f[pl.ds(2 * tile + 1, 1), :])
        masked = spread(lane_mask[pl.ds(tile, 1), :])
        near = spread(stations_of[entry, pl.ds(0, 1), :]) | masked
        far = spread(stations_of[entry, pl.ds(1, 1), :]) | masked
        gain_real, gain_imag = gain_table[owner, 0], gain_table[owner, 1]
        near_real, near_imag = pick(gain_real, near), pick(gain_imag, near)
        far_real, far_imag = pick(gain_real, far), pick(gain_imag, far)
        slope_real = real * far_real + imag * far_imag
        slope_imag = imag * far_real - real * far_imag
        other_real = real * near_real - imag * near_imag
        other_imag = real * near_imag + imag * near_real
        near_rows = hermitian_rows(slope_real, slope_imag, upper, 1) + [
            slope_real * seen_real + slope_imag * seen_imag,
            slope_real * seen_imag - slope_imag * seen_real,
        ]
        far_rows = hermitian_rows(other_real, other_imag, upper, -1) + [
            other_real * seen_real + other_imag * seen_imag,
            other_imag * seen_real - other_real * seen_imag,
        ]
        rows = jnp.concatenate(
            [
                jnp.concatenate(near_rows, axis=0).astype(jnp.bfloat16),
                jnp.concatenate(far_rows, axis=0).astype(jnp.bfloat16),
            ],
            axis=1,
        )
        return jnp.dot(rows, table[entry], preferred_element_type=jnp.float32)

    def some_groups(step, carry):
        base_group = step * UNROLL
        running = sums_ref[base_group]
        for number in range(UNROLL):
            group = base_group + number
            total = one_tile(group * GROUP)
            for inner in range(1, GROUP):
                total = total + one_tile(group * GROUP + inner)
            running = running * codes[3, group].astype(jnp.float32) + total
            sums_ref[group + 1] = running
        return carry

    lax.fori_loop(0, groups // UNROLL, some_groups, 0)

    def sums_of(owner):
        return sums_ref[jnp.clip(codes[4, owner], 0, groups)]

    near = {}
    order = list(range(1, chan_count)) + [0]
    for offset in order:
        target = lax.rem(chan + offset, chan_count)
        for shift in range(1, sub_count):
            other = lax.rem(sub + shift, sub_count)
            near_src[shift - 1, offset] = encode(sums_of(target * sub_count + other), directions)
            copy = pltpu.make_async_remote_copy(
                src_ref=near_src.at[shift - 1, offset],
                dst_ref=near_buf.at[shift - 1, offset],
                send_sem=near_send.at[shift - 1, offset],
                recv_sem=near_recv.at[shift - 1, offset],
                device_id={"sub": other},
                device_id_type=mesh_id,
            )
            copy.start()
            near[offset, shift] = copy

    mine = [jnp.broadcast_to(basis_buf[d, pl.ds(me, 1), :], shape) for d in range(degree)]
    duals = [
        lay_pair(lambda number: duals_ref[number, part], pad, half, width) for part in range(2)
    ]
    anchors = []
    for part in range(2):
        anchor = jnp.zeros(shape, jnp.float32)
        for d in range(degree):
            anchor = anchor + mine[d] * lay_pair(
                lambda number: consensus_ref[d, part], pad, half, width
            )
        anchors.append(anchor)

    far = []
    for offset in order:
        target = lax.rem(chan + offset, chan_count)
        total = sums_of(target * sub_count + sub)
        for shift in range(1, sub_count):
            near[offset, shift].wait_recv()
            total = total + decode(near_buf[shift - 1, offset], directions)
        if offset:
            send_buf[offset] = encode(total, directions)
            copy = pltpu.make_async_remote_copy(
                src_ref=send_buf.at[offset],
                dst_ref=far_buf.at[offset],
                send_sem=far_send.at[offset],
                recv_sem=far_recv.at[offset],
                device_id={"chan": target},
                device_id_type=mesh_id,
            )
            copy.start()
            far.append((offset, copy))
    for offset, copy in far:
        copy.wait_recv()
        total = total + decode(far_buf[offset], directions)

    middle = directions // 2
    group = [total[i * directions : (i + 1) * directions] for i in range(directions + 2)]
    solved = solve_hermitian(
        group[:middle],
        group[middle : directions - 1],
        group[directions - 1],
        rho,
        group[directions] - duals[0] + rho * anchors[0],
        group[directions + 1] - duals[1] + rho * anchors[1],
    )
    weights[me] = jnp.concatenate(
        [solved[part] + duals[part] / rho for part in range(2)], axis=0
    ).astype(jnp.bfloat16)

    last = []
    for offset in range(1, owners):
        copy = pltpu.make_async_remote_copy(
            src_ref=weights.at[me],
            dst_ref=weights.at[me],
            send_sem=last_send.at[offset],
            recv_sem=last_recv.at[offset],
            device_id=device(lax.rem(me + offset, owners)),
            device_id_type=mesh_id,
        )
        copy.start()
        last.append(copy)

    def store(first, part, value):
        for number in range(half):
            out_ref[first + number, part] = (
                pltpu.roll(value, LANES - number * width, axis=1) if number else value
            )

    for part in range(2):
        store(0, part, solved[part])
    for copy in last:
        copy.wait_recv()
    inverse = inverse_gram(channels)
    totals = []
    for d in range(degree):
        value = jnp.zeros((2 * directions, LANES), jnp.float32)
        for number in range(owners):
            value = value + basis_buf[d, number : number + 1, :] * weights[number].astype(jnp.float32)
        folded = value
        for number in range(1, half):
            folded = folded + pltpu.roll(value, number * width, axis=1)
        totals.append(folded)
    fitted = jnp.zeros((2 * directions, LANES), jnp.float32)
    for d in range(degree):
        value = sum(float(inverse[d, e]) * totals[e] for e in range(degree))
        for part in range(2):
            out_ref[half + d, part] = value[part * directions : (part + 1) * directions]
        fitted = fitted + jnp.concatenate([mine[d], mine[d]], axis=0) * value
    for part in range(2):
        fit = fitted[part * directions : (part + 1) * directions]
        store(half + degree, part, duals[part] + rho * (solved[part] - fit))
    for copy in gathers:
        copy.wait_send()
    for copy in near.values():
        copy.wait_send()
    for _, copy in far:
        copy.wait_send()
    for copy in last:
        copy.wait_send()


def deliver_kernel(result_ref, gains_out, consensus_out, duals_out):
    first = 0
    for ref in (gains_out, consensus_out, duals_out):
        count, _, _, stations = ref.shape
        for number in range(count):
            ref[number] = result_ref[first + number][:, :, :stations]
        first += count


def body(
    predicted_sky_response,
    measured_correlation,
    keep_indicator,
    tile_owner,
    tile_channel,
    tile_base,
    pairs,
    gains,
    duals,
    consensus,
    rho,
):
    channels_here, _, stations, directions = gains.shape
    chan_count = lax.axis_size("chan")
    sub_count = lax.axis_size("sub")
    half = channels_here // sub_count
    owners = chan_count * sub_count
    tiles, _, _, tile_rows = predicted_sky_response.shape
    bases = pairs.shape[0]
    degree = consensus.shape[0]
    width = LANES // half
    if width & (width - 1) or stations >= width or tile_rows != LANES:
        raise ValueError("unsupported sizes")
    groups = -(-(tiles + owners * (GROUP - 1)) // GROUP)
    groups = -(-groups // UNROLL) * UNROLL
    code_width = -(-max(groups * GROUP, owners) // LANES) * LANES
    out_rows = directions * directions + 2 * directions
    coded = out_rows + 2 * directions
    gains_t = jnp.swapaxes(gains, 2, 3)
    duals_t = jnp.swapaxes(duals, 2, 3)
    consensus_t = jnp.swapaxes(consensus, 2, 3)
    operands = [
        tile_owner.reshape(1, tiles),
        tile_channel.reshape(1, tiles),
        tile_base.reshape(1, tiles),
        predicted_sky_response.reshape(tiles * 2 * directions, tile_rows),
        measured_correlation.reshape(tiles * 2, tile_rows),
        keep_indicator,
        pairs,
        gains_t,
        duals_t,
        consensus_t,
    ]
    vmem, dma = pltpu.VMEM, pltpu.SemaphoreType.DMA
    f32, bf16, i32 = jnp.float32, jnp.bfloat16, jnp.int32
    result = pl.pallas_call(
        functools.partial(whole_kernel, chan_count, sub_count, half, groups),
        out_shape=jax.ShapeDtypeStruct((2 * half + degree, 2, directions, LANES), f32),
        in_specs=[pl.BlockSpec(memory_space=pltpu.SMEM)]
        + [pl.BlockSpec(memory_space=pl.ANY)] * len(operands),
        out_specs=pl.BlockSpec(memory_space=pltpu.VMEM),
        scratch_shapes=[vmem(x.shape, x.dtype) for x in operands]
        + [
            vmem((owners, 2, directions, LANES), f32),
            vmem((bases * half, 2 * tile_rows, LANES), bf16),
            vmem((LANES, tile_rows), f32),
            vmem((bases * half, 2, tile_rows), i32),
            vmem(((tiles + 8) * 2 * directions, tile_rows), f32),
            vmem((2 * tiles + 8, tile_rows), f32),
            vmem((tiles + 8, tile_rows), i32),
            vmem((8, code_width), i32),
            pltpu.SMEM((8, code_width), i32),
            vmem((groups + 1, out_rows, LANES), f32),
            vmem((2, directions, LANES), f32),
            vmem((sub_count - 1, chan_count, coded, LANES), bf16),
            vmem((sub_count - 1, chan_count, coded, LANES), bf16),
            vmem((chan_count, coded, LANES), bf16),
            vmem((chan_count, coded, LANES), bf16),
            vmem((owners, 2 * directions, LANES), bf16),
            vmem((degree, owners, LANES), f32),
            dma((len(operands) + 1,)),
            dma((chan_count,)),
            dma((chan_count,)),
            dma((sub_count - 1, chan_count)),
            dma((sub_count - 1, chan_count)),
            dma((chan_count,)),
            dma((chan_count,)),
            dma((owners,)),
            dma((owners,)),
        ],
        compiler_params=pltpu.CompilerParams(
            collective_id=1, has_side_effects=True, vmem_limit_bytes=60 << 20
        ),
    )(rho, *[operands[i] for i in range(len(operands))])
    outputs = pl.pallas_call(
        deliver_kernel,
        out_shape=tuple(
            jax.ShapeDtypeStruct(x.shape, f32) for x in (duals_t, consensus_t, duals_t)
        ),
        in_specs=[pl.BlockSpec(memory_space=pltpu.VMEM)],
        out_specs=tuple(pl.BlockSpec(memory_space=pltpu.VMEM) for _ in range(3)),
    )(result)
    return tuple(jnp.swapaxes(x, 2, 3) for x in outputs)


def solution(mesh):
    placed = (
        P(("groups", "chan", "sub"), None, None, None),
        P(("groups", "chan", "sub"), None, None),
        P(("groups", "chan", "sub"), None),
        P(("groups", "chan", "sub"), None),
        P(("groups", "chan", "sub")),
        P(("groups", "chan", "sub")),
        P(),
        P(("groups", "chan"), None, None, None),
        P(("groups", "chan", "sub"), None, None, None),
        P("groups", None, None, None),
        P(),
    )
    return jax.shard_map(
        body,
        mesh=mesh,
        in_specs=placed,
        out_specs=(
            P(("groups", "chan", "sub"), None, None, None),
            P("groups", None, None, None),
            P(("groups", "chan", "sub"), None, None, None),
        ),
        check_vma=False,
    )
```

```python
import functools

import jax
import jax.numpy as jnp
import numpy as np
from jax import lax
from jax.experimental import pallas as pl
from jax.experimental.pallas import tpu as pltpu
from jax.sharding import PartitionSpec as P

LANES = 128
GROUP = 4
UNROLL = 20


def lay_pair(load, pad, half, width):
    total = None
    for part in range(half):
        block = load(part)
        pad[part % 2, :, : block.shape[1]] = block
        value = pad[part % 2]
        if part:
            value = pltpu.roll(value, part * width, axis=1)
        total = value if total is None else total + value
    return total


def basis_of(channel, channels):
    x = (2.0 * channel - (channels - 1)) / max(channels - 1, 1)
    return [
        jnp.ones_like(x),
        x,
        0.5 * (3.0 * x * x - 1.0),
        0.5 * (5.0 * x * x * x - 3.0 * x),
    ]


def inverse_gram(channels):
    f = np.arange(channels, dtype=np.float64)
    x = (2.0 * f - (channels - 1)) / max(channels - 1, 1)
    basis = np.stack([np.ones_like(x), x, 0.5 * (3 * x * x - 1), 0.5 * (5 * x * x * x - 3 * x)])
    return np.linalg.inv(basis @ basis.T)


def end_rows(real, imag, seen_real, seen_imag, upper, sign, turn):
    directions = real.shape[0]
    bf16 = jnp.bfloat16
    flipped = -real if sign > 0 else -imag
    for number, value in enumerate((real, imag, flipped)):
        turn[number, :directions, :] = value
        turn[number, directions:, :] = value

    def turned(number, shift):
        return turn[number, shift : shift + directions, :]

    def pair(first, second):
        return jnp.concatenate([first, second], axis=0).astype(bf16)

    left, right = pair(real, real), pair(imag, imag)
    ahead_real, ahead_imag = pair(turned(0, 1), turned(0, 2)), pair(turned(1, 1), turned(1, 2))
    both = left * ahead_real + right * ahead_imag
    cross = left * ahead_imag - right * ahead_real if sign > 0 else right * ahead_real - left * ahead_imag
    if sign > 0:
        cross_left, cross_right = (turned(1, 3), turned(1, 4)), (turned(2, 3), turned(2, 4))
    else:
        cross_left, cross_right = (turned(2, 3), turned(2, 4)), (turned(0, 3), turned(0, 4))
    mixed_left = jnp.where(upper, turned(0, 4), cross_left[1])
    mixed_right = jnp.where(upper, turned(1, 4), cross_right[1])
    third = left * pair(turned(0, 3), mixed_left) + right * pair(turned(1, 3), mixed_right)
    last = left * pair(cross_left[0], real) + right * pair(cross_right[0], imag)
    side_real = real * seen_real + imag * seen_imag
    if sign > 0:
        side_imag = real * seen_imag - imag * seen_real
    else:
        side_imag = imag * seen_real - real * seen_imag
    return jnp.concatenate([both, cross, third, last, pair(side_real, side_imag)], axis=0)


def solve_hermitian(groups_real, groups_imag, mixed, ridge, side_real, side_imag):
    directions = side_real.shape[0]
    middle = directions // 2
    row = lax.broadcasted_iota(jnp.int32, side_real.shape, 0)
    upper = row < middle
    swapped = pltpu.roll(mixed, middle, axis=0)
    real = {0: groups_real[0] + ridge, middle: jnp.where(upper, mixed, swapped)}
    imag = {0: jnp.zeros_like(ridge), middle: jnp.where(upper, -swapped, mixed)}
    for d in range(1, middle):
        real[d], imag[d] = groups_real[d], groups_imag[d - 1]
        real[directions - d] = pltpu.roll(groups_real[d], d, axis=0)
        imag[directions - d] = -pltpu.roll(groups_imag[d - 1], d, axis=0)
    columns = []
    for l in range(directions):
        column_real, column_imag = real[l], imag[l]
        for k in range(1, directions):
            here = row == k
            d = (l - k) % directions
            column_real = jnp.where(here, real[d], column_real)
            column_imag = jnp.where(here, imag[d], column_imag)
        columns.append((column_real, column_imag))
    columns.append((side_real, side_imag))
    scale = jnp.zeros_like(ridge)
    for j in range(directions):
        pivot_real, pivot_imag = columns[j]
        inverse = 1.0 / pivot_real[j : j + 1]
        here = row == j
        scale = jnp.where(here, jnp.broadcast_to(inverse, scale.shape), scale)
        factor_real = jnp.where(here, 0.0, pivot_real * inverse)
        factor_imag = jnp.where(here, 0.0, pivot_imag * inverse)
        for l in range(j + 1, directions + 1):
            value_real, value_imag = columns[l]
            head_real, head_imag = value_real[j : j + 1], value_imag[j : j + 1]
            columns[l] = (
                value_real - (factor_real * head_real - factor_imag * head_imag),
                value_imag - (factor_real * head_imag + factor_imag * head_real),
            )
    return columns[-1][0] * scale, columns[-1][1] * scale


def encode(sums, directions):
    normal_rows = directions * directions
    side = sums[normal_rows:]
    high = side.astype(jnp.bfloat16)
    low = (side - high.astype(jnp.float32)).astype(jnp.bfloat16)
    return jnp.concatenate([sums[:normal_rows].astype(jnp.bfloat16), high, low], axis=0)


def decode(coded, directions):
    wide = coded.astype(jnp.float32)
    normal_rows = directions * directions
    side_rows = 2 * directions
    high, low = wide[normal_rows : normal_rows + side_rows], wide[normal_rows + side_rows :]
    return jnp.concatenate([wide[:normal_rows], high + low], axis=0)


def sort_tiles(owner, channel, base, codes, owners, sub_count, half, groups, entries):
    tiles = owner.shape[1]
    slots = groups * GROUP
    sub = jnp.zeros_like(channel)
    for number in range(1, sub_count):
        sub = sub + jnp.where(channel >= number * half, 1, 0)
    place = channel - sub * half
    key = owner * sub_count + sub
    entry = base * half + place
    same = jnp.where(
        lax.broadcasted_iota(jnp.int32, (owners, tiles), 0) == jnp.broadcast_to(key, (owners, tiles)), 1.0, 0.0
    )
    same_b = same.astype(jnp.bfloat16)
    until = jnp.where(
        lax.broadcasted_iota(jnp.int32, (tiles, tiles), 0) <= lax.broadcasted_iota(jnp.int32, (tiles, tiles), 1),
        1.0,
        0.0,
    ).astype(jnp.bfloat16)
    nt = (((1,), (1,)), ((), ()))
    count = jnp.dot(same_b, until, preferred_element_type=jnp.float32)

    def pieces(value):
        return jnp.floor((value + float(GROUP - 1)) * (1.0 / GROUP))

    wide = (owners, LANES)
    used = pieces(jnp.broadcast_to(count[:, tiles - 1 : tiles], wide))
    square = (owners, owners)
    row, column = lax.broadcasted_iota(jnp.int32, square, 0), lax.broadcasted_iota(jnp.int32, square, 1)
    before = jnp.where(column < row, 1.0, 0.0).astype(jnp.bfloat16)
    start = jnp.dot(before, used.astype(jnp.bfloat16), preferred_element_type=jnp.float32)
    position = jnp.sum(same * (start[:, :1] * float(GROUP) + count), axis=0, keepdims=True) - 1.0
    left = tiles - lax.broadcasted_iota(jnp.int32, (1, tiles), 1)
    features = jnp.concatenate(
        [left & 255, lax.shift_right_logical(left, 8), entry, key, jnp.zeros((4, tiles), jnp.int32)], axis=0
    )
    chosen = jnp.where(
        lax.broadcasted_iota(jnp.int32, (slots, tiles), 0)
        == jnp.broadcast_to(position.astype(jnp.int32), (slots, tiles)),
        1.0,
        0.0,
    ).astype(jnp.bfloat16)
    sorted_features = lax.dot_general(
        features.astype(jnp.float32).astype(jnp.bfloat16), chosen, nt, preferred_element_type=jnp.float32
    )
    tile = float(tiles) - (sorted_features[0:1] + 256.0 * sorted_features[1:2])
    codes[0:1, :slots] = jnp.clip(tile.astype(jnp.int32), 0, tiles)
    codes[1:2, :slots] = jnp.clip(sorted_features[2:3].astype(jnp.int32), 0, entries - 1)
    codes[2:3, :slots] = jnp.clip(sorted_features[3:4].astype(jnp.int32), 0, owners - 1)
    spread = -(-groups // LANES) * LANES
    number = lax.broadcasted_iota(jnp.int32, (owners, spread), 1).astype(jnp.float32)
    first = (jnp.broadcast_to(start[:, :1], number.shape) == number) & (
        jnp.broadcast_to(used[:, :1], number.shape) > 0.5
    )
    carried = 1.0 - jnp.max(jnp.where(first, 1.0, 0.0), axis=0, keepdims=True)
    codes[3:4, :spread] = carried.astype(jnp.int32)
    used_row = pieces(lax.dot_general(jnp.ones((8, tiles), jnp.bfloat16), same_b, nt, preferred_element_type=jnp.float32))
    upto = jnp.where(row <= column, 1.0, 0.0).astype(jnp.bfloat16)
    end = jnp.dot(used_row.astype(jnp.bfloat16), upto, preferred_element_type=jnp.float32)
    last = jnp.where(used_row > 0.5, end, 0.0).astype(jnp.int32)
    codes[4:5, :owners] = jnp.clip(last[0:1], 0, groups)


def whole_kernel(
    chan_count,
    sub_count,
    half,
    groups,
    rho_ref,
    owner_hbm,
    channel_hbm,
    base_hbm,
    coupling_hbm,
    observed_hbm,
    keep_hbm,
    pairs_hbm,
    gains_hbm,
    duals_hbm,
    consensus_hbm,
    out_ref,
    owner_ref,
    channel_ref,
    base_ref,
    coupling_ref,
    observed_ref,
    keep_ref,
    pairs_ref,
    gains_ref,
    duals_ref,
    consensus_ref,
    gain_table,
    table,
    turned,
    stations_of,
    coupling_f,
    observed_f,
    lane_mask,
    codes_v,
    codes,
    sums_ref,
    turn,
    pad,
    near_src,
    near_buf,
    send_buf,
    far_buf,
    weights,
    basis_buf,
    local_sem,
    gains_send,
    gains_recv,
    near_send,
    near_recv,
    far_send,
    far_recv,
    last_send,
    last_recv,
):
    chan, sub = lax.axis_index("chan"), lax.axis_index("sub")
    owners = chan_count * sub_count
    channels = owners * half
    width = LANES // half
    directions, stations = duals_ref.shape[2], duals_ref.shape[3]
    degree = consensus_ref.shape[0]
    tiles = keep_ref.shape[0]
    tile_rows = keep_ref.shape[1]
    bases = pairs_ref.shape[0]
    me = chan * sub_count + sub
    mesh_id = pl.DeviceIdType.MESH

    def device(flat):
        return {"chan": lax.div(flat, sub_count), "sub": lax.rem(flat, sub_count)}

    barrier = pltpu.get_barrier_semaphore()
    for offset in range(1, owners):
        pl.semaphore_signal(
            barrier, inc=1, device_id=device(lax.rem(me + offset, owners)), device_id_type=mesh_id
        )

    loads = []
    for number, (source, target) in enumerate(
        [
            (gains_hbm, gains_ref),
            (owner_hbm, owner_ref),
            (channel_hbm, channel_ref),
            (base_hbm, base_ref),
            (pairs_hbm, pairs_ref),
            (coupling_hbm, coupling_ref),
            (observed_hbm, observed_ref),
            (keep_hbm, keep_ref),
            (duals_hbm, duals_ref),
            (consensus_hbm, consensus_ref),
        ]
    ):
        copy = pltpu.make_async_copy(source, target, local_sem.at[number])
        copy.start()
        loads.append(copy)

    pad[...] = jnp.zeros_like(pad)
    loads[0].wait()
    for owner in range(sub_count):
        for part in range(2):
            gain_table[me - sub + owner, part] = lay_pair(
                lambda number: gains_ref[owner * half + number, part], pad, half, width
            )
    pl.semaphore_wait(barrier, owners - 1)
    gathers = []
    for offset in range(1, chan_count):
        mine_here = gain_table.at[pl.ds(chan * sub_count, sub_count)]
        copy = pltpu.make_async_remote_copy(
            src_ref=mine_here,
            dst_ref=mine_here,
            send_sem=gains_send.at[offset],
            recv_sem=gains_recv.at[offset],
            device_id={"chan": lax.rem(chan + offset, chan_count)},
            device_id_type=mesh_id,
        )
        copy.start()
        gathers.append(copy)

    for copy in loads[1:4]:
        copy.wait()
    codes_v[...] = jnp.zeros_like(codes_v)
    sort_tiles(owner_ref[...], channel_ref[...], base_ref[...], codes_v, owners, sub_count, half, groups, bases * half)
    to_scalar = pltpu.make_async_copy(codes_v, codes, local_sem.at[len(loads)])
    to_scalar.start()

    loads[4].wait()
    turned[...] = jnp.zeros_like(turned)
    for base in range(bases):
        both = pairs_ref[base]
        turned[2 * base : 2 * base + 2, :] = both.astype(jnp.float32)
        for part in range(half):
            stations_of[base * half + part] = both + part * width
    columns = jnp.transpose(turned[...])
    lane = lax.broadcasted_iota(jnp.int32, (tile_rows, LANES), 1).astype(jnp.float32)
    for base in range(bases):
        for end in range(2):
            station = jnp.broadcast_to(columns[:, 2 * base + end : 2 * base + end + 1], lane.shape)
            for part in range(half):
                table[base * half + part, end * tile_rows : (end + 1) * tile_rows, :] = jnp.where(
                    station == lane - float(part * width), 1.0, 0.0
                ).astype(jnp.bfloat16)

    for copy in loads[5:]:
        copy.wait()
    step_rows = 2 * directions

    def widen(step, carry):
        span = pl.ds(pl.multiple_of(step * 8 * step_rows, 8 * step_rows), 8 * step_rows)
        coupling_f[span, :] = coupling_ref[span, :].astype(jnp.float32)
        return carry

    lax.fori_loop(0, tiles // 8, widen, 0)
    coupling_f[tiles * step_rows :, :] = jnp.zeros((8 * step_rows, tile_rows), jnp.float32)
    observed_f[: 2 * tiles, :] = observed_ref[...].astype(jnp.float32)
    observed_f[2 * tiles :, :] = jnp.zeros((8, tile_rows), jnp.float32)
    lane_mask[:tiles, :] = jnp.where(keep_ref[...] > 0, 0, width - 1)
    lane_mask[tiles:, :] = jnp.zeros((8, tile_rows), jnp.int32)

    shape = (directions, LANES)
    row = lax.broadcasted_iota(jnp.int32, shape, 0)
    rho = jnp.zeros(shape, jnp.float32)
    for k in range(directions):
        rho = jnp.where(row == k, rho_ref[k], rho)
    place = lax.broadcasted_iota(jnp.int32, (owners, LANES), 1)
    of = lax.broadcasted_iota(jnp.int32, (owners, LANES), 0)
    everyone = basis_of((of * half + lax.div(place, width)).astype(jnp.float32), channels)
    for d in range(degree):
        basis_buf[d] = everyone[d]

    normal_rows = directions * directions
    out_rows = normal_rows + 2 * directions
    sums_ref[0] = jnp.zeros((out_rows, LANES), jnp.float32)
    upper = row < directions // 2
    to_scalar.wait()
    for copy in gathers:
        copy.wait_recv()

    def spread(values):
        return jnp.broadcast_to(values, shape)

    def pick(values, index):
        return lax.gather(
            values,
            index[..., None],
            lax.GatherDimensionNumbers(
                offset_dims=(),
                collapsed_slice_dims=(1,),
                start_index_map=(1,),
                operand_batching_dims=(0,),
                start_indices_batching_dims=(0,),
            ),
            slice_sizes=(1, 1),
            mode=lax.GatherScatterMode.PROMISE_IN_BOUNDS,
        )

    def one_tile(slot, spot):
        tile = jnp.clip(codes[0, slot], 0, tiles)
        entry = jnp.clip(codes[1, slot], 0, bases * half - 1)
        owner = jnp.clip(codes[2, slot], 0, owners - 1)
        first = tile * step_rows
        real = coupling_f[pl.ds(first, directions, stride=2), :]
        imag = coupling_f[pl.ds(first + 1, directions, stride=2), :]
        seen_real = spread(observed_f[pl.ds(2 * tile, 1), :])
        seen_imag = spread(observed_f[pl.ds(2 * tile + 1, 1), :])
        masked = spread(lane_mask[pl.ds(tile, 1), :])
        near = spread(stations_of[entry, pl.ds(0, 1), :]) | masked
        far = spread(stations_of[entry, pl.ds(1, 1), :]) | masked
        gain_real, gain_imag = gain_table[owner, 0], gain_table[owner, 1]
        near_real, near_imag = pick(gain_real, near), pick(gain_imag, near)
        far_real, far_imag = pick(gain_real, far), pick(gain_imag, far)
        slope_real = real * far_real + imag * far_imag
        slope_imag = imag * far_real - real * far_imag
        other_real = real * near_real - imag * near_imag
        other_imag = real * near_imag + imag * near_real
        return [
            end_rows(slope_real, slope_imag, seen_real, seen_imag, upper, 1, turn.at[2 * spot]),
            end_rows(other_real, other_imag, seen_real, seen_imag, upper, -1, turn.at[2 * spot + 1]),
        ], table[entry]

    def some_groups(step, carry):
        base_group = step * UNROLL
        running = sums_ref[base_group]
        for number in range(UNROLL):
            group = base_group + number
            rows, entries = [], []
            for inner in range(GROUP):
                ends, entry = one_tile(group * GROUP + inner, number * GROUP + inner)
                rows += ends
                entries.append(entry)
            total = jnp.dot(
                jnp.concatenate(rows, axis=1),
                jnp.concatenate(entries, axis=0),
                preferred_element_type=jnp.float32,
            )
            running = running * codes[3, group].astype(jnp.float32) + total
            sums_ref[group + 1] = running
        return carry

    lax.fori_loop(0, groups // UNROLL, some_groups, 0)

    def sums_of(owner):
        return sums_ref[jnp.clip(codes[4, owner], 0, groups)]

    near = {}
    order = list(range(1, chan_count)) + [0]
    for offset in order:
        target = lax.rem(chan + offset, chan_count)
        for shift in range(1, sub_count):
            other = lax.rem(sub + shift, sub_count)
            near_src[shift - 1, offset] = encode(sums_of(target * sub_count + other), directions)
            copy = pltpu.make_async_remote_copy(
                src_ref=near_src.at[shift - 1, offset],
                dst_ref=near_buf.at[shift - 1, offset],
                send_sem=near_send.at[shift - 1, offset],
                recv_sem=near_recv.at[shift - 1, offset],
                device_id={"sub": other},
                device_id_type=mesh_id,
            )
            copy.start()
            near[offset, shift] = copy

    mine = [jnp.broadcast_to(basis_buf[d, pl.ds(me, 1), :], shape) for d in range(degree)]
    duals = [
        lay_pair(lambda number: duals_ref[number, part], pad, half, width) for part in range(2)
    ]
    anchors = []
    for part in range(2):
        anchor = jnp.zeros(shape, jnp.float32)
        for d in range(degree):
            anchor = anchor + mine[d] * lay_pair(
                lambda number: consensus_ref[d, part], pad, half, width
            )
        anchors.append(anchor)

    far = []
    for offset in order:
        target = lax.rem(chan + offset, chan_count)
        total = sums_of(target * sub_count + sub)
        for shift in range(1, sub_count):
            near[offset, shift].wait_recv()
            total = total + decode(near_buf[shift - 1, offset], directions)
        if offset:
            send_buf[offset] = encode(total, directions)
            copy = pltpu.make_async_remote_copy(
                src_ref=send_buf.at[offset],
                dst_ref=far_buf.at[offset],
                send_sem=far_send.at[offset],
                recv_sem=far_recv.at[offset],
                device_id={"chan": target},
                device_id_type=mesh_id,
            )
            copy.start()
            far.append((offset, copy))
    for offset, copy in far:
        copy.wait_recv()
        total = total + decode(far_buf[offset], directions)

    group = [total[i * directions : (i + 1) * directions] for i in range(directions + 2)]
    solved = solve_hermitian(
        [group[7], group[0], group[1], group[4]],
        [group[2], group[3], group[6]],
        group[5],
        rho,
        group[directions] - duals[0] + rho * anchors[0],
        group[directions + 1] - duals[1] + rho * anchors[1],
    )
    weights[me] = jnp.concatenate(
        [solved[part] + duals[part] / rho for part in range(2)], axis=0
    ).astype(jnp.bfloat16)

    last = []
    for offset in range(1, owners):
        copy = pltpu.make_async_remote_copy(
            src_ref=weights.at[me],
            dst_ref=weights.at[me],
            send_sem=last_send.at[offset],
            recv_sem=last_recv.at[offset],
            device_id=device(lax.rem(me + offset, owners)),
            device_id_type=mesh_id,
        )
        copy.start()
        last.append(copy)

    def store(first, part, value):
        for number in range(half):
            out_ref[first + number, part] = (
                pltpu.roll(value, LANES - number * width, axis=1) if number else value
            )

    for part in range(2):
        store(0, part, solved[part])
    for copy in last:
        copy.wait_recv()
    inverse = inverse_gram(channels)
    totals = []
    for d in range(degree):
        value = jnp.zeros((2 * directions, LANES), jnp.float32)
        for number in range(owners):
            value = value + basis_buf[d, number : number + 1, :] * weights[number].astype(jnp.float32)
        folded = value
        for number in range(1, half):
            folded = folded + pltpu.roll(value, number * width, axis=1)
        totals.append(folded)
    fitted = jnp.zeros((2 * directions, LANES), jnp.float32)
    for d in range(degree):
        value = sum(float(inverse[d, e]) * totals[e] for e in range(degree))
        for part in range(2):
            out_ref[half + d, part] = value[part * directions : (part + 1) * directions]
        fitted = fitted + jnp.concatenate([mine[d], mine[d]], axis=0) * value
    for part in range(2):
        fit = fitted[part * directions : (part + 1) * directions]
        store(half + degree, part, duals[part] + rho * (solved[part] - fit))
    for copy in gathers:
        copy.wait_send()
    for copy in near.values():
        copy.wait_send()
    for _, copy in far:
        copy.wait_send()
    for copy in last:
        copy.wait_send()


def deliver_kernel(result_ref, gains_out, consensus_out, duals_out):
    first = 0
    for ref in (gains_out, consensus_out, duals_out):
        count, _, _, stations = ref.shape
        for number in range(count):
            ref[number] = result_ref[first + number][:, :, :stations]
        first += count


def body(
    predicted_sky_response,
    measured_correlation,
    keep_indicator,
    tile_owner,
    tile_channel,
    tile_base,
    pairs,
    gains,
    duals,
    consensus,
    rho,
):
    channels_here, _, stations, directions = gains.shape
    chan_count = lax.axis_size("chan")
    sub_count = lax.axis_size("sub")
    half = channels_here // sub_count
    owners = chan_count * sub_count
    tiles, _, _, tile_rows = predicted_sky_response.shape
    bases = pairs.shape[0]
    degree = consensus.shape[0]
    width = LANES // half
    if width & (width - 1) or stations >= width or tile_rows != LANES or directions != 8:
        raise ValueError("unsupported sizes")
    groups = -(-(tiles + owners * (GROUP - 1)) // GROUP)
    groups = -(-groups // UNROLL) * UNROLL
    code_width = -(-max(groups * GROUP, owners) // LANES) * LANES
    out_rows = directions * directions + 2 * directions
    coded = out_rows + 2 * directions
    gains_t = jnp.swapaxes(gains, 2, 3)
    duals_t = jnp.swapaxes(duals, 2, 3)
    consensus_t = jnp.swapaxes(consensus, 2, 3)
    operands = [
        tile_owner.reshape(1, tiles),
        tile_channel.reshape(1, tiles),
        tile_base.reshape(1, tiles),
        predicted_sky_response.reshape(tiles * 2 * directions, tile_rows),
        measured_correlation.reshape(tiles * 2, tile_rows),
        keep_indicator,
        pairs,
        gains_t,
        duals_t,
        consensus_t,
    ]
    vmem, dma = pltpu.VMEM, pltpu.SemaphoreType.DMA
    f32, bf16, i32 = jnp.float32, jnp.bfloat16, jnp.int32
    result = pl.pallas_call(
        functools.partial(whole_kernel, chan_count, sub_count, half, groups),
        out_shape=jax.ShapeDtypeStruct((2 * half + degree, 2, directions, LANES), f32),
        in_specs=[pl.BlockSpec(memory_space=pltpu.SMEM)]
        + [pl.BlockSpec(memory_space=pl.ANY)] * len(operands),
        out_specs=pl.BlockSpec(memory_space=pltpu.VMEM),
        scratch_shapes=[vmem(x.shape, x.dtype) for x in operands]
        + [
            vmem((owners, 2, directions, LANES), f32),
            vmem((bases * half, 2 * tile_rows, LANES), bf16),
            vmem((LANES, tile_rows), f32),
            vmem((bases * half, 2, tile_rows), i32),
            vmem(((tiles + 8) * 2 * directions, tile_rows), f32),
            vmem((2 * tiles + 8, tile_rows), f32),
            vmem((tiles + 8, tile_rows), i32),
            vmem((8, code_width), i32),
            pltpu.SMEM((8, code_width), i32),
            vmem((groups + 1, out_rows, LANES), f32),
            vmem((2 * GROUP * UNROLL, 3, 2 * directions, LANES), f32),
            vmem((2, directions, LANES), f32),
            vmem((sub_count - 1, chan_count, coded, LANES), bf16),
            vmem((sub_count - 1, chan_count, coded, LANES), bf16),
            vmem((chan_count, coded, LANES), bf16),
            vmem((chan_count, coded, LANES), bf16),
            vmem((owners, 2 * directions, LANES), bf16),
            vmem((degree, owners, LANES), f32),
            dma((len(operands) + 1,)),
            dma((chan_count,)),
            dma((chan_count,)),
            dma((sub_count - 1, chan_count)),
            dma((sub_count - 1, chan_count)),
            dma((chan_count,)),
            dma((chan_count,)),
            dma((owners,)),
            dma((owners,)),
        ],
        compiler_params=pltpu.CompilerParams(
            collective_id=1, has_side_effects=True, vmem_limit_bytes=60 << 20
        ),
    )(rho, *[operands[i] for i in range(len(operands))])
    outputs = pl.pallas_call(
        deliver_kernel,
        out_shape=tuple(
            jax.ShapeDtypeStruct(x.shape, f32) for x in (duals_t, consensus_t, duals_t)
        ),
        in_specs=[pl.BlockSpec(memory_space=pltpu.VMEM)],
        out_specs=tuple(pl.BlockSpec(memory_space=pltpu.VMEM) for _ in range(3)),
    )(result)
    return tuple(jnp.swapaxes(x, 2, 3) for x in outputs)


def solution(mesh):
    placed = (
        P(("groups", "chan", "sub"), None, None, None),
        P(("groups", "chan", "sub"), None, None),
        P(("groups", "chan", "sub"), None),
        P(("groups", "chan", "sub"), None),
        P(("groups", "chan", "sub")),
        P(("groups", "chan", "sub")),
        P(),
        P(("groups", "chan"), None, None, None),
        P(("groups", "chan", "sub"), None, None, None),
        P("groups", None, None, None),
        P(),
    )
    return jax.shard_map(
        body,
        mesh=mesh,
        in_specs=placed,
        out_specs=(
            P(("groups", "chan", "sub"), None, None, None),
            P("groups", None, None, None),
            P(("groups", "chan", "sub"), None, None, None),
        ),
        check_vma=False,
    )
```

```python
import functools

import jax
import jax.numpy as jnp
import numpy as np
from jax import lax
from jax.experimental import pallas as pl
from jax.experimental.pallas import tpu as pltpu
from jax.sharding import PartitionSpec as P

LANES = 128
GROUP = 4
UNROLL = 20


def lay_pair(load, pad, half, width):
    total = None
    for part in range(half):
        block = load(part)
        pad[part % 2, :, : block.shape[1]] = block
        value = pad[part % 2]
        if part:
            value = pltpu.roll(value, part * width, axis=1)
        total = value if total is None else total + value
    return total


def basis_of(channel, channels):
    x = (2.0 * channel - (channels - 1)) / max(channels - 1, 1)
    return [
        jnp.ones_like(x),
        x,
        0.5 * (3.0 * x * x - 1.0),
        0.5 * (5.0 * x * x * x - 3.0 * x),
    ]


def inverse_gram(channels):
    f = np.arange(channels, dtype=np.float64)
    x = (2.0 * f - (channels - 1)) / max(channels - 1, 1)
    basis = np.stack([np.ones_like(x), x, 0.5 * (3 * x * x - 1), 0.5 * (5 * x * x * x - 3 * x)])
    return np.linalg.inv(basis @ basis.T)


def end_rows(real, imag, seen_real, seen_imag, upper, sign):
    directions = real.shape[0]
    bf16 = jnp.bfloat16
    flipped = -real if sign > 0 else -imag
    def turned(number, shift):
        return pltpu.roll((real, imag, flipped)[number], directions - shift, axis=0)

    def pair(first, second):
        return jnp.concatenate([first, second], axis=0).astype(bf16)

    left, right = pair(real, real), pair(imag, imag)
    ahead_real, ahead_imag = pair(turned(0, 1), turned(0, 2)), pair(turned(1, 1), turned(1, 2))
    both = left * ahead_real + right * ahead_imag
    cross = left * ahead_imag - right * ahead_real if sign > 0 else right * ahead_real - left * ahead_imag
    if sign > 0:
        cross_left, cross_right = (turned(1, 3), turned(1, 4)), (turned(2, 3), turned(2, 4))
    else:
        cross_left, cross_right = (turned(2, 3), turned(2, 4)), (turned(0, 3), turned(0, 4))
    mixed_left = jnp.where(upper, turned(0, 4), cross_left[1])
    mixed_right = jnp.where(upper, turned(1, 4), cross_right[1])
    third = left * pair(turned(0, 3), mixed_left) + right * pair(turned(1, 3), mixed_right)
    last = left * pair(cross_left[0], real) + right * pair(cross_right[0], imag)
    side_real = real * seen_real + imag * seen_imag
    if sign > 0:
        side_imag = real * seen_imag - imag * seen_real
    else:
        side_imag = imag * seen_real - real * seen_imag
    return jnp.concatenate([both, cross, third, last, pair(side_real, side_imag)], axis=0)


def solve_hermitian(groups_real, groups_imag, mixed, ridge, side_real, side_imag):
    directions = side_real.shape[0]
    middle = directions // 2
    row = lax.broadcasted_iota(jnp.int32, side_real.shape, 0)
    upper = row < middle
    swapped = pltpu.roll(mixed, middle, axis=0)
    real = {0: groups_real[0] + ridge, middle: jnp.where(upper, mixed, swapped)}
    imag = {0: jnp.zeros_like(ridge), middle: jnp.where(upper, -swapped, mixed)}
    for d in range(1, middle):
        real[d], imag[d] = groups_real[d], groups_imag[d - 1]
        real[directions - d] = pltpu.roll(groups_real[d], d, axis=0)
        imag[directions - d] = -pltpu.roll(groups_imag[d - 1], d, axis=0)
    columns = []
    for l in range(directions):
        column_real, column_imag = real[l], imag[l]
        for k in range(1, directions):
            here = row == k
            d = (l - k) % directions
            column_real = jnp.where(here, real[d], column_real)
            column_imag = jnp.where(here, imag[d], column_imag)
        columns.append((column_real, column_imag))
    columns.append((side_real, side_imag))
    scale = jnp.zeros_like(ridge)
    for j in range(directions):
        pivot_real, pivot_imag = columns[j]
        inverse = 1.0 / pivot_real[j : j + 1]
        here = row == j
        scale = jnp.where(here, jnp.broadcast_to(inverse, scale.shape), scale)
        factor_real = jnp.where(here, 0.0, pivot_real * inverse)
        factor_imag = jnp.where(here, 0.0, pivot_imag * inverse)
        for l in range(j + 1, directions + 1):
            value_real, value_imag = columns[l]
            head_real, head_imag = value_real[j : j + 1], value_imag[j : j + 1]
            columns[l] = (
                value_real - (factor_real * head_real - factor_imag * head_imag),
                value_imag - (factor_real * head_imag + factor_imag * head_real),
            )
    return columns[-1][0] * scale, columns[-1][1] * scale


def encode(sums, directions):
    normal_rows = directions * directions
    side = sums[normal_rows:]
    high = side.astype(jnp.bfloat16)
    low = (side - high.astype(jnp.float32)).astype(jnp.bfloat16)
    return jnp.concatenate([sums[:normal_rows].astype(jnp.bfloat16), high, low], axis=0)


def decode(coded, directions):
    wide = coded.astype(jnp.float32)
    normal_rows = directions * directions
    side_rows = 2 * directions
    high, low = wide[normal_rows : normal_rows + side_rows], wide[normal_rows + side_rows :]
    return jnp.concatenate([wide[:normal_rows], high + low], axis=0)


def sort_tiles(rank, channel, base, codes, owners, sub_count, half, groups, entries):
    tiles = rank.shape[1]
    slots = groups * GROUP
    sub = jnp.zeros_like(channel)
    for number in range(1, sub_count):
        sub = sub + jnp.where(channel >= number * half, 1, 0)
    place = channel - sub * half
    key = rank * sub_count + sub
    entry = base * half + place
    same = jnp.where(
        lax.broadcasted_iota(jnp.int32, (owners, tiles), 0) == jnp.broadcast_to(key, (owners, tiles)), 1.0, 0.0
    )
    same_b = same.astype(jnp.bfloat16)
    until = jnp.where(
        lax.broadcasted_iota(jnp.int32, (tiles, tiles), 0) <= lax.broadcasted_iota(jnp.int32, (tiles, tiles), 1),
        1.0,
        0.0,
    ).astype(jnp.bfloat16)
    nt = (((1,), (1,)), ((), ()))
    count = jnp.dot(same_b, until, preferred_element_type=jnp.float32)

    def pieces(value):
        return jnp.floor((value + float(GROUP - 1)) * (1.0 / GROUP))

    wide = (owners, LANES)
    used = pieces(jnp.broadcast_to(count[:, tiles - 1 : tiles], wide))
    square = (owners, owners)
    row, column = lax.broadcasted_iota(jnp.int32, square, 0), lax.broadcasted_iota(jnp.int32, square, 1)
    before = jnp.where(column < row, 1.0, 0.0).astype(jnp.bfloat16)
    start = jnp.dot(before, used.astype(jnp.bfloat16), preferred_element_type=jnp.float32)
    position = jnp.sum(same * (start[:, :1] * float(GROUP) + count), axis=0, keepdims=True) - 1.0
    left = tiles - lax.broadcasted_iota(jnp.int32, (1, tiles), 1)
    features = jnp.concatenate(
        [left & 255, lax.shift_right_logical(left, 8), entry, key, jnp.zeros((4, tiles), jnp.int32)], axis=0
    )
    chosen = jnp.where(
        lax.broadcasted_iota(jnp.int32, (slots, tiles), 0)
        == jnp.broadcast_to(position.astype(jnp.int32), (slots, tiles)),
        1.0,
        0.0,
    ).astype(jnp.bfloat16)
    sorted_features = lax.dot_general(
        features.astype(jnp.float32).astype(jnp.bfloat16), chosen, nt, preferred_element_type=jnp.float32
    )
    tile = float(tiles) - (sorted_features[0:1] + 256.0 * sorted_features[1:2])
    codes[0:1, :slots] = jnp.clip(tile.astype(jnp.int32), 0, tiles)
    codes[1:2, :slots] = jnp.clip(sorted_features[2:3].astype(jnp.int32), 0, entries - 1)
    codes[2:3, :slots] = jnp.clip(sorted_features[3:4].astype(jnp.int32), 0, owners - 1)
    spread = -(-groups // LANES) * LANES
    number = lax.broadcasted_iota(jnp.int32, (owners, spread), 1).astype(jnp.float32)
    first = (jnp.broadcast_to(start[:, :1], number.shape) == number) & (
        jnp.broadcast_to(used[:, :1], number.shape) > 0.5
    )
    carried = 1.0 - jnp.max(jnp.where(first, 1.0, 0.0), axis=0, keepdims=True)
    codes[3:4, :spread] = carried.astype(jnp.int32)
    used_row = pieces(lax.dot_general(jnp.ones((8, tiles), jnp.bfloat16), same_b, nt, preferred_element_type=jnp.float32))
    upto = jnp.where(row <= column, 1.0, 0.0).astype(jnp.bfloat16)
    end = jnp.dot(used_row.astype(jnp.bfloat16), upto, preferred_element_type=jnp.float32)
    last = jnp.where(used_row > 0.5, end, 0.0).astype(jnp.int32)
    codes[4:5, :owners] = jnp.clip(last[0:1], 0, groups)


def whole_kernel(
    chan_count,
    sub_count,
    half,
    groups,
    rho_ref,
    owner_hbm,
    channel_hbm,
    base_hbm,
    coupling_hbm,
    observed_hbm,
    keep_hbm,
    pairs_hbm,
    gains_hbm,
    duals_hbm,
    consensus_hbm,
    out_ref,
    owner_ref,
    channel_ref,
    base_ref,
    coupling_ref,
    observed_ref,
    keep_ref,
    pairs_ref,
    gains_ref,
    duals_ref,
    consensus_ref,
    gain_table,
    table,
    turned,
    stations_of,
    coupling_f,
    coupling_t,
    observed_f,
    lane_mask,
    codes_v,
    codes,
    sums_ref,
    pad,
    near_src,
    near_buf,
    send_buf,
    far_buf,
    weights,
    basis_buf,
    local_sem,
    gains_send,
    gains_recv,
    near_send,
    near_recv,
    far_send,
    far_recv,
    last_send,
    last_recv,
):
    chan, sub = lax.axis_index("chan"), lax.axis_index("sub")
    owners = chan_count * sub_count
    channels = owners * half
    width = LANES // half
    directions, stations = duals_ref.shape[2], duals_ref.shape[3]
    degree = consensus_ref.shape[0]
    tiles = keep_ref.shape[0]
    tile_rows = keep_ref.shape[1]
    bases = pairs_ref.shape[0]
    me = chan * sub_count + sub
    mesh_id = pl.DeviceIdType.MESH

    top = chan_count - 1

    def device(flat):
        return {"chan": lax.div(flat, sub_count), "sub": lax.rem(flat, sub_count)}

    def partner(rank):
        flips, result, bit = top - rank, chan, 1
        while bit < chan_count:
            if flips & bit:
                result = result + bit * (1 - 2 * lax.rem(lax.div(chan, bit), 2))
            bit *= 2
        return result

    partners = [partner(rank) for rank in range(chan_count)]

    barrier = pltpu.get_barrier_semaphore()
    for offset in range(1, owners):
        pl.semaphore_signal(
            barrier, inc=1, device_id=device(lax.rem(me + offset, owners)), device_id_type=mesh_id
        )

    loads = []
    for number, (source, target) in enumerate(
        [
            (gains_hbm, gains_ref),
            (owner_hbm, owner_ref),
            (channel_hbm, channel_ref),
            (base_hbm, base_ref),
            (pairs_hbm, pairs_ref),
            (coupling_hbm, coupling_ref),
            (observed_hbm, observed_ref),
            (keep_hbm, keep_ref),
            (duals_hbm, duals_ref),
            (consensus_hbm, consensus_ref),
        ]
    ):
        copy = pltpu.make_async_copy(source, target, local_sem.at[number])
        copy.start()
        loads.append(copy)

    pad[...] = jnp.zeros_like(pad)
    loads[0].wait()
    for owner in range(sub_count):
        for part in range(2):
            gain_table[top * sub_count + owner, part] = lay_pair(
                lambda number: gains_ref[owner * half + number, part], pad, half, width
            )
    pl.semaphore_wait(barrier, owners - 1)
    gathers = []
    for rank in range(top):
        copy = pltpu.make_async_remote_copy(
            src_ref=gain_table.at[pl.ds(top * sub_count, sub_count)],
            dst_ref=gain_table.at[pl.ds(rank * sub_count, sub_count)],
            send_sem=gains_send.at[rank],
            recv_sem=gains_recv.at[rank],
            device_id={"chan": partners[rank]},
            device_id_type=mesh_id,
        )
        copy.start()
        gathers.append(copy)

    for copy in loads[1:4]:
        copy.wait()
    codes_v[...] = jnp.zeros_like(codes_v)
    named = owner_ref[...]
    rank_of = top - (named + chan - 2 * (named & chan))
    sort_tiles(rank_of, channel_ref[...], base_ref[...], codes_v, owners, sub_count, half, groups, bases * half)
    to_scalar = pltpu.make_async_copy(codes_v, codes, local_sem.at[len(loads)])
    to_scalar.start()

    loads[4].wait()
    turned[...] = jnp.zeros_like(turned)
    for base in range(bases):
        both = pairs_ref[base]
        turned[2 * base : 2 * base + 2, :] = both.astype(jnp.float32)
        for part in range(half):
            stations_of[base * half + part] = both + part * width
    columns = jnp.transpose(turned[...])
    lane = lax.broadcasted_iota(jnp.int32, (tile_rows, LANES), 1).astype(jnp.float32)
    for base in range(bases):
        for end in range(2):
            station = jnp.broadcast_to(columns[:, 2 * base + end : 2 * base + end + 1], lane.shape)
            for part in range(half):
                table[base * half + part, end * tile_rows : (end + 1) * tile_rows, :] = jnp.where(
                    station == lane - float(part * width), 1.0, 0.0
                ).astype(jnp.bfloat16)

    for copy in loads[5:]:
        copy.wait()
    step_rows = 2 * directions

    def widen(step, carry):
        span = pl.ds(pl.multiple_of(step * 8 * step_rows, 8 * step_rows), 8 * step_rows)
        coupling_t[...] = coupling_ref[span, :].astype(jnp.float32)
        for number in range(2):
            value = coupling_t[pl.ds(number, 8 * directions, stride=2), :]
            coupling_f[number, pl.ds(step * 8, 8)] = value.reshape(8, directions, tile_rows)
        return carry

    lax.fori_loop(0, tiles // 8, widen, 0)
    coupling_f[:, tiles:] = jnp.zeros((2, 1, directions, tile_rows), jnp.float32)
    observed_f[: 2 * tiles, :] = observed_ref[...].astype(jnp.float32)
    observed_f[2 * tiles :, :] = jnp.zeros((8, tile_rows), jnp.float32)
    lane_mask[:tiles, :] = jnp.where(keep_ref[...] > 0, 0, width - 1)
    lane_mask[tiles:, :] = jnp.zeros((8, tile_rows), jnp.int32)

    shape = (directions, LANES)
    row = lax.broadcasted_iota(jnp.int32, shape, 0)
    rho = jnp.zeros(shape, jnp.float32)
    for k in range(directions):
        rho = jnp.where(row == k, rho_ref[k], rho)
    place = lax.broadcasted_iota(jnp.int32, (owners, LANES), 1)
    of = lax.broadcasted_iota(jnp.int32, (owners, LANES), 0)
    everyone = basis_of((of * half + lax.div(place, width)).astype(jnp.float32), channels)
    for d in range(degree):
        basis_buf[d] = everyone[d]

    normal_rows = directions * directions
    out_rows = normal_rows + 2 * directions
    sums_ref[0] = jnp.zeros((out_rows, LANES), jnp.float32)
    upper = row < directions // 2
    to_scalar.wait()
    for copy in gathers:
        copy.wait_recv()

    def spread(values):
        return jnp.broadcast_to(values, shape)

    def pick(values, index):
        return lax.gather(
            values,
            index[..., None],
            lax.GatherDimensionNumbers(
                offset_dims=(),
                collapsed_slice_dims=(1,),
                start_index_map=(1,),
                operand_batching_dims=(0,),
                start_indices_batching_dims=(0,),
            ),
            slice_sizes=(1, 1),
            mode=lax.GatherScatterMode.PROMISE_IN_BOUNDS,
        )

    def one_tile(slot):
        tile = jnp.clip(codes[0, slot], 0, tiles)
        entry = jnp.clip(codes[1, slot], 0, bases * half - 1)
        owner = jnp.clip(codes[2, slot], 0, owners - 1)
        real, imag = coupling_f[0, tile], coupling_f[1, tile]
        seen_real = spread(observed_f[pl.ds(2 * tile, 1), :])
        seen_imag = spread(observed_f[pl.ds(2 * tile + 1, 1), :])
        masked = spread(lane_mask[pl.ds(tile, 1), :])
        near = spread(stations_of[entry, pl.ds(0, 1), :]) | masked
        far = spread(stations_of[entry, pl.ds(1, 1), :]) | masked
        gain_real, gain_imag = gain_table[owner, 0], gain_table[owner, 1]
        near_real, near_imag = pick(gain_real, near), pick(gain_imag, near)
        far_real, far_imag = pick(gain_real, far), pick(gain_imag, far)
        slope_real = real * far_real + imag * far_imag
        slope_imag = imag * far_real - real * far_imag
        other_real = real * near_real - imag * near_imag
        other_imag = real * near_imag + imag * near_real
        return [
            end_rows(slope_real, slope_imag, seen_real, seen_imag, upper, 1),
            end_rows(other_real, other_imag, seen_real, seen_imag, upper, -1),
        ], table[entry]

    def sums_of(rank, which):
        return sums_ref[jnp.clip(codes[4, rank * sub_count + which], 0, groups)]

    def near_copy(rank, shift):
        return pltpu.make_async_remote_copy(
            src_ref=near_src.at[shift - 1, rank],
            dst_ref=near_buf.at[shift - 1, rank],
            send_sem=near_send.at[shift - 1, rank],
            recv_sem=near_recv.at[shift - 1, rank],
            device_id={"sub": lax.rem(sub + shift, sub_count)},
            device_id_type=mesh_id,
        )

    def far_copy(rank):
        return pltpu.make_async_remote_copy(
            src_ref=send_buf.at[rank],
            dst_ref=far_buf.at[rank],
            send_sem=far_send.at[rank],
            recv_sem=far_recv.at[rank],
            device_id={"chan": partners[rank]},
            device_id_type=mesh_id,
        )

    def start_near(rank):
        for shift in range(1, sub_count):
            near_src[shift - 1, rank] = encode(sums_of(rank, lax.rem(sub + shift, sub_count)), directions)
            near_copy(rank, shift).start()

    def add_near(rank):
        total = sums_of(rank, sub)
        for shift in range(1, sub_count):
            near_copy(rank, shift).wait_recv()
            total = total + decode(near_buf[shift - 1, rank], directions)
        return total

    def start_far(rank):
        send_buf[rank] = encode(add_near(rank), directions)
        far_copy(rank).start()

    def some_groups(step, carry):
        for rank, ready in enumerate(early):

            @pl.when(step == ready)
            def _():
                start_near(rank)

            @pl.when(step == ready + 1)
            def _():
                start_far(rank)

        base_group = step * UNROLL
        running = sums_ref[base_group]
        for number in range(UNROLL):
            group = base_group + number
            rows, entries = [], []
            for inner in range(GROUP):
                ends, entry = one_tile(group * GROUP + inner)
                rows += ends
                entries.append(entry)
            total = jnp.dot(
                jnp.concatenate(rows, axis=1),
                jnp.concatenate(entries, axis=0),
                preferred_element_type=jnp.float32,
            )
            running = running * codes[3, group].astype(jnp.float32) + total
            sums_ref[group + 1] = running
        return carry

    steps = groups // UNROLL
    most = 3 * tiles // chan_count + sub_count * (GROUP - 1)
    early = []
    for rank in range(top):
        ready = -(-(rank + 1) * most // (GROUP * UNROLL))
        if ready + 1 < steps:
            early.append(ready)
    lax.fori_loop(0, steps, some_groups, 0)

    for rank in range(len(early), chan_count):
        start_near(rank)

    mine = [jnp.broadcast_to(basis_buf[d, pl.ds(me, 1), :], shape) for d in range(degree)]
    duals = [
        lay_pair(lambda number: duals_ref[number, part], pad, half, width) for part in range(2)
    ]
    anchors = []
    for part in range(2):
        anchor = jnp.zeros(shape, jnp.float32)
        for d in range(degree):
            anchor = anchor + mine[d] * lay_pair(
                lambda number: consensus_ref[d, part], pad, half, width
            )
        anchors.append(anchor)

    for rank in range(len(early), top):
        start_far(rank)
    total = add_near(top)
    for rank in range(top):
        far_copy(rank).wait_recv()
        total = total + decode(far_buf[rank], directions)

    group = [total[i * directions : (i + 1) * directions] for i in range(directions + 2)]
    solved = solve_hermitian(
        [group[7], group[0], group[1], group[4]],
        [group[2], group[3], group[6]],
        group[5],
        rho,
        group[directions] - duals[0] + rho * anchors[0],
        group[directions + 1] - duals[1] + rho * anchors[1],
    )
    weights[me] = jnp.concatenate(
        [solved[part] + duals[part] / rho for part in range(2)], axis=0
    ).astype(jnp.bfloat16)

    last = []
    for rank in range(chan_count):
        for shift in range(sub_count):
            if rank == top and shift == 0:
                continue
            number = rank * sub_count + shift
            copy = pltpu.make_async_remote_copy(
                src_ref=weights.at[me],
                dst_ref=weights.at[me],
                send_sem=last_send.at[number],
                recv_sem=last_recv.at[number],
                device_id={"chan": partners[rank], "sub": lax.rem(sub + shift, sub_count)},
                device_id_type=mesh_id,
            )
            copy.start()
            last.append(copy)

    def store(first, part, value):
        for number in range(half):
            out_ref[first + number, part] = (
                pltpu.roll(value, LANES - number * width, axis=1) if number else value
            )

    for part in range(2):
        store(0, part, solved[part])
    for copy in last:
        copy.wait_recv()
    inverse = inverse_gram(channels)
    totals = []
    for d in range(degree):
        value = jnp.zeros((2 * directions, LANES), jnp.float32)
        for number in range(owners):
            value = value + basis_buf[d, number : number + 1, :] * weights[number].astype(jnp.float32)
        folded = value
        for number in range(1, half):
            folded = folded + pltpu.roll(value, number * width, axis=1)
        totals.append(folded)
    fitted = jnp.zeros((2 * directions, LANES), jnp.float32)
    for d in range(degree):
        value = sum(float(inverse[d, e]) * totals[e] for e in range(degree))
        for part in range(2):
            out_ref[half + d, part] = value[part * directions : (part + 1) * directions]
        fitted = fitted + jnp.concatenate([mine[d], mine[d]], axis=0) * value
    for part in range(2):
        fit = fitted[part * directions : (part + 1) * directions]
        store(half + degree, part, duals[part] + rho * (solved[part] - fit))
    for copy in gathers:
        copy.wait_send()
    for rank in range(chan_count):
        for shift in range(1, sub_count):
            near_copy(rank, shift).wait_send()
        if rank < top:
            far_copy(rank).wait_send()
    for copy in last:
        copy.wait_send()


def deliver_kernel(result_ref, gains_out, consensus_out, duals_out):
    first = 0
    for ref in (gains_out, consensus_out, duals_out):
        count, _, _, stations = ref.shape
        for number in range(count):
            ref[number] = result_ref[first + number][:, :, :stations]
        first += count


def body(
    predicted_sky_response,
    measured_correlation,
    keep_indicator,
    tile_owner,
    tile_channel,
    tile_base,
    pairs,
    gains,
    duals,
    consensus,
    rho,
):
    channels_here, _, stations, directions = gains.shape
    chan_count = lax.axis_size("chan")
    sub_count = lax.axis_size("sub")
    half = channels_here // sub_count
    owners = chan_count * sub_count
    tiles, _, _, tile_rows = predicted_sky_response.shape
    bases = pairs.shape[0]
    degree = consensus.shape[0]
    width = LANES // half
    if chan_count & (chan_count - 1) or width & (width - 1) or stations >= width or tile_rows != LANES or directions != 8:
        raise ValueError("unsupported sizes")
    groups = -(-(tiles + owners * (GROUP - 1)) // GROUP)
    groups = -(-groups // UNROLL) * UNROLL
    code_width = -(-max(groups * GROUP, owners) // LANES) * LANES
    out_rows = directions * directions + 2 * directions
    coded = out_rows + 2 * directions
    gains_t = jnp.swapaxes(gains, 2, 3)
    duals_t = jnp.swapaxes(duals, 2, 3)
    consensus_t = jnp.swapaxes(consensus, 2, 3)
    operands = [
        tile_owner.reshape(1, tiles),
        tile_channel.reshape(1, tiles),
        tile_base.reshape(1, tiles),
        predicted_sky_response.reshape(tiles * 2 * directions, tile_rows),
        measured_correlation.reshape(tiles * 2, tile_rows),
        keep_indicator,
        pairs,
        gains_t,
        duals_t,
        consensus_t,
    ]
    vmem, dma = pltpu.VMEM, pltpu.SemaphoreType.DMA
    f32, bf16, i32 = jnp.float32, jnp.bfloat16, jnp.int32
    result = pl.pallas_call(
        functools.partial(whole_kernel, chan_count, sub_count, half, groups),
        out_shape=pltpu.VMEM((2 * half + degree, 2, directions, LANES), f32),
        in_specs=[pl.BlockSpec(memory_space=pltpu.SMEM)]
        + [pl.BlockSpec(memory_space=pl.ANY)] * len(operands),
        out_specs=pl.BlockSpec(memory_space=pltpu.VMEM),
        scratch_shapes=[vmem(x.shape, x.dtype) for x in operands]
        + [
            vmem((owners, 2, directions, LANES), f32),
            vmem((bases * half, 2 * tile_rows, LANES), bf16),
            vmem((LANES, tile_rows), f32),
            vmem((bases * half, 2, tile_rows), i32),
            vmem((2, tiles + 1, directions, tile_rows), f32),
            vmem((8 * 2 * directions, tile_rows), f32),
            vmem((2 * tiles + 8, tile_rows), f32),
            vmem((tiles + 8, tile_rows), i32),
            vmem((8, code_width), i32),
            pltpu.SMEM((8, code_width), i32),
            vmem((groups + 1, out_rows, LANES), f32),
            vmem((2, directions, LANES), f32),
            vmem((sub_count - 1, chan_count, coded, LANES), bf16),
            vmem((sub_count - 1, chan_count, coded, LANES), bf16),
            vmem((chan_count, coded, LANES), bf16),
            vmem((chan_count, coded, LANES), bf16),
            vmem((owners, 2 * directions, LANES), bf16),
            vmem((degree, owners, LANES), f32),
            dma((len(operands) + 1,)),
            dma((chan_count,)),
            dma((chan_count,)),
            dma((sub_count - 1, chan_count)),
            dma((sub_count - 1, chan_count)),
            dma((chan_count,)),
            dma((chan_count,)),
            dma((owners,)),
            dma((owners,)),
        ],
        compiler_params=pltpu.CompilerParams(
            collective_id=1, has_side_effects=True, vmem_limit_bytes=60 << 20
        ),
    )(rho, *[operands[i] for i in range(len(operands))])
    outputs = pl.pallas_call(
        deliver_kernel,
        out_shape=tuple(
            jax.ShapeDtypeStruct(x.shape, f32) for x in (duals_t, consensus_t, duals_t)
        ),
        in_specs=[pl.BlockSpec(memory_space=pltpu.VMEM)],
        out_specs=tuple(pl.BlockSpec(memory_space=pltpu.VMEM) for _ in range(3)),
    )(pltpu.with_memory_space_constraint(result, pltpu.VMEM))
    return tuple(jnp.swapaxes(x, 2, 3) for x in outputs)


def solution(mesh):
    placed = (
        P(("groups", "chan", "sub"), None, None, None),
        P(("groups", "chan", "sub"), None, None),
        P(("groups", "chan", "sub"), None),
        P(("groups", "chan", "sub"), None),
        P(("groups", "chan", "sub")),
        P(("groups", "chan", "sub")),
        P(),
        P(("groups", "chan"), None, None, None),
        P(("groups", "chan", "sub"), None, None, None),
        P("groups", None, None, None),
        P(),
    )
    return jax.shard_map(
        body,
        mesh=mesh,
        in_specs=placed,
        out_specs=(
            P(("groups", "chan", "sub"), None, None, None),
            P("groups", None, None, None),
            P(("groups", "chan", "sub"), None, None, None),
        ),
        check_vma=False,
    )
```

```python
import functools

import jax
import jax.numpy as jnp
import numpy as np
from jax import lax
from jax.experimental import pallas as pl
from jax.experimental.pallas import tpu as pltpu
from jax.sharding import PartitionSpec as P

LANES = 128
GROUP = 4
UNROLL = 20
GAIN_MOST = 5.0
CODE_MOST = 32767.0


def lay_pair(load, pad, half, width):
    total = None
    for part in range(half):
        block = load(part)
        pad[part % 2, :, : block.shape[1]] = block
        value = pad[part % 2]
        if part:
            value = pltpu.roll(value, part * width, axis=1)
        total = value if total is None else total + value
    return total


def basis_of(channel, channels):
    x = (2.0 * channel - (channels - 1)) / max(channels - 1, 1)
    return [
        jnp.ones_like(x),
        x,
        0.5 * (3.0 * x * x - 1.0),
        0.5 * (5.0 * x * x * x - 3.0 * x),
    ]


def inverse_gram(channels):
    f = np.arange(channels, dtype=np.float64)
    x = (2.0 * f - (channels - 1)) / max(channels - 1, 1)
    basis = np.stack([np.ones_like(x), x, 0.5 * (3 * x * x - 1), 0.5 * (5 * x * x * x - 3 * x)])
    return np.linalg.inv(basis @ basis.T)


def end_rows(real, imag, seen_real, seen_imag, upper, turn, sign):
    directions = real.shape[0]

    def pair(first, second):
        return jnp.concatenate([first, second], axis=0).astype(jnp.bfloat16)

    def turned(value, shift):
        return pltpu.roll(value, directions - shift, axis=0)

    left, right = pair(real, real), pair(imag, imag)
    ahead_real = pair(turned(real, 1), turned(real, 2))
    ahead_imag = pair(turned(imag, 1), turned(imag, 2))
    both = left * ahead_real + right * ahead_imag
    third_real, third_imag = turned(real, 3), turned(imag, 3)
    fourth_real, fourth_imag = turned(real, 4), turned(imag, 4)
    ahead_one = pair(third_imag, jnp.where(upper, fourth_real, fourth_imag))
    ahead_two = pair(third_real, jnp.where(upper, fourth_imag, fourth_real))
    if sign > 0:
        cross = left * ahead_imag - right * ahead_real
        mixed = left * ahead_one + right * turn * ahead_two
        side_imag = real * seen_imag - imag * seen_real
    else:
        cross = right * ahead_real - left * ahead_imag
        mixed = left * turn * ahead_one + right * ahead_two
        side_imag = imag * seen_real - real * seen_imag
    plain = left * pair(third_real, real) + right * pair(third_imag, imag)
    side_real = real * seen_real + imag * seen_imag
    return jnp.concatenate([both, cross, mixed, plain, pair(side_real, side_imag)], axis=0)


def solve_hermitian(groups_real, groups_imag, mixed, ridge, side_real, side_imag):
    directions = side_real.shape[0]
    middle = directions // 2
    row = lax.broadcasted_iota(jnp.int32, side_real.shape, 0)
    upper = row < middle
    swapped = pltpu.roll(mixed, middle, axis=0)
    real = {0: groups_real[0] + ridge, middle: jnp.where(upper, mixed, swapped)}
    imag = {0: jnp.zeros_like(ridge), middle: jnp.where(upper, -swapped, mixed)}
    for d in range(1, middle):
        real[d], imag[d] = groups_real[d], groups_imag[d - 1]
        real[directions - d] = pltpu.roll(groups_real[d], d, axis=0)
        imag[directions - d] = -pltpu.roll(groups_imag[d - 1], d, axis=0)
    columns = []
    for l in range(directions):
        column_real, column_imag = real[l], imag[l]
        for k in range(1, directions):
            here = row == k
            d = (l - k) % directions
            column_real = jnp.where(here, real[d], column_real)
            column_imag = jnp.where(here, imag[d], column_imag)
        columns.append((column_real, column_imag))
    columns.append((side_real, side_imag))
    scale = jnp.zeros_like(ridge)
    for j in range(directions):
        pivot_real, pivot_imag = columns[j]
        inverse = 1.0 / pivot_real[j : j + 1]
        here = row == j
        scale = jnp.where(here, jnp.broadcast_to(inverse, scale.shape), scale)
        factor_real = jnp.where(here, 0.0, pivot_real * inverse)
        factor_imag = jnp.where(here, 0.0, pivot_imag * inverse)
        for l in range(j + 1, directions + 1):
            value_real, value_imag = columns[l]
            head_real, head_imag = value_real[j : j + 1], value_imag[j : j + 1]
            columns[l] = (
                value_real - (factor_real * head_real - factor_imag * head_imag),
                value_imag - (factor_real * head_imag + factor_imag * head_real),
            )
    return columns[-1][0] * scale, columns[-1][1] * scale


def encode(sums, directions):
    normal_rows = directions * directions
    side = sums[normal_rows:]
    high = side.astype(jnp.bfloat16)
    low = (side - high.astype(jnp.float32)).astype(jnp.bfloat16)
    return jnp.concatenate([sums[:normal_rows].astype(jnp.bfloat16), high, low], axis=0)


def decode(coded, directions):
    wide = coded.astype(jnp.float32)
    normal_rows = directions * directions
    side_rows = 2 * directions
    high, low = wide[normal_rows : normal_rows + side_rows], wide[normal_rows + side_rows :]
    return jnp.concatenate([wide[:normal_rows], high + low], axis=0)


def sort_tiles(rank, channel, base, codes, owners, sub_count, half, groups, entries):
    tiles = rank.shape[1]
    slots = groups * GROUP
    sub = jnp.zeros_like(channel)
    for number in range(1, sub_count):
        sub = sub + jnp.where(channel >= number * half, 1, 0)
    place = channel - sub * half
    key = rank * sub_count + sub
    entry = base * half + place
    same = jnp.where(
        lax.broadcasted_iota(jnp.int32, (owners, tiles), 0) == jnp.broadcast_to(key, (owners, tiles)), 1.0, 0.0
    )
    same_b = same.astype(jnp.bfloat16)
    until = jnp.where(
        lax.broadcasted_iota(jnp.int32, (tiles, tiles), 0) <= lax.broadcasted_iota(jnp.int32, (tiles, tiles), 1),
        1.0,
        0.0,
    ).astype(jnp.bfloat16)
    nt = (((1,), (1,)), ((), ()))
    count = jnp.dot(same_b, until, preferred_element_type=jnp.float32)

    def pieces(value):
        return jnp.floor((value + float(GROUP - 1)) * (1.0 / GROUP))

    wide = (owners, LANES)
    used = pieces(jnp.broadcast_to(count[:, tiles - 1 : tiles], wide))
    square = (owners, owners)
    row, column = lax.broadcasted_iota(jnp.int32, square, 0), lax.broadcasted_iota(jnp.int32, square, 1)
    before = jnp.where(column < row, 1.0, 0.0).astype(jnp.bfloat16)
    start = jnp.dot(before, used.astype(jnp.bfloat16), preferred_element_type=jnp.float32)
    position = jnp.sum(same * (start[:, :1] * float(GROUP) + count), axis=0, keepdims=True) - 1.0
    left = tiles - lax.broadcasted_iota(jnp.int32, (1, tiles), 1)
    features = jnp.concatenate(
        [left & 255, lax.shift_right_logical(left, 8), entry, key, jnp.zeros((4, tiles), jnp.int32)], axis=0
    )
    chosen = jnp.where(
        lax.broadcasted_iota(jnp.int32, (slots, tiles), 0)
        == jnp.broadcast_to(position.astype(jnp.int32), (slots, tiles)),
        1.0,
        0.0,
    ).astype(jnp.bfloat16)
    sorted_features = lax.dot_general(
        features.astype(jnp.float32).astype(jnp.bfloat16), chosen, nt, preferred_element_type=jnp.float32
    )
    tile = float(tiles) - (sorted_features[0:1] + 256.0 * sorted_features[1:2])
    codes[0:1, :slots] = jnp.clip(tile.astype(jnp.int32), 0, tiles)
    codes[1:2, :slots] = jnp.clip(sorted_features[2:3].astype(jnp.int32), 0, entries - 1)
    codes[2:3, :slots] = jnp.clip(sorted_features[3:4].astype(jnp.int32), 0, owners - 1)
    spread = -(-groups // LANES) * LANES
    number = lax.broadcasted_iota(jnp.int32, (owners, spread), 1).astype(jnp.float32)
    first = (jnp.broadcast_to(start[:, :1], number.shape) == number) & (
        jnp.broadcast_to(used[:, :1], number.shape) > 0.5
    )
    carried = 1.0 - jnp.max(jnp.where(first, 1.0, 0.0), axis=0, keepdims=True)
    codes[3:4, :spread] = carried.astype(jnp.int32)
    used_row = pieces(lax.dot_general(jnp.ones((8, tiles), jnp.bfloat16), same_b, nt, preferred_element_type=jnp.float32))
    upto = jnp.where(row <= column, 1.0, 0.0).astype(jnp.bfloat16)
    end = jnp.dot(used_row.astype(jnp.bfloat16), upto, preferred_element_type=jnp.float32)
    last = jnp.where(used_row > 0.5, end, 0.0).astype(jnp.int32)
    codes[4:5, :owners] = jnp.clip(last[0:1], 0, groups)


def whole_kernel(
    chan_count,
    sub_count,
    half,
    groups,
    rho_ref,
    owner_hbm,
    channel_hbm,
    base_hbm,
    coupling_hbm,
    observed_hbm,
    keep_hbm,
    pairs_hbm,
    gains_hbm,
    duals_hbm,
    consensus_hbm,
    out_ref,
    owner_ref,
    channel_ref,
    base_ref,
    coupling_ref,
    observed_ref,
    keep_ref,
    pairs_ref,
    gains_ref,
    duals_ref,
    consensus_ref,
    gain_table,
    gain_codes,
    table,
    turned,
    stations_of,
    coupling_f,
    coupling_t,
    observed_f,
    lane_mask,
    codes_v,
    codes,
    sums_ref,
    pad,
    near_src,
    near_buf,
    send_buf,
    far_buf,
    weights,
    basis_buf,
    local_sem,
    gains_send,
    gains_recv,
    near_send,
    near_recv,
    far_send,
    far_recv,
    last_send,
    last_recv,
):
    chan, sub = lax.axis_index("chan"), lax.axis_index("sub")
    owners = chan_count * sub_count
    channels = owners * half
    width = LANES // half
    directions, stations = duals_ref.shape[2], duals_ref.shape[3]
    degree = consensus_ref.shape[0]
    tiles = keep_ref.shape[0]
    tile_rows = keep_ref.shape[1]
    bases = pairs_ref.shape[0]
    me = chan * sub_count + sub
    mesh_id = pl.DeviceIdType.MESH

    top = chan_count - 1

    def device(flat):
        return {"chan": lax.div(flat, sub_count), "sub": lax.rem(flat, sub_count)}

    def partner(rank):
        flips, result, bit = top - rank, chan, 1
        while bit < chan_count:
            if flips & bit:
                result = result + bit * (1 - 2 * lax.rem(lax.div(chan, bit), 2))
            bit *= 2
        return result

    partners = [partner(rank) for rank in range(chan_count)]

    barrier = pltpu.get_barrier_semaphore()
    for offset in range(1, owners):
        pl.semaphore_signal(
            barrier, inc=1, device_id=device(lax.rem(me + offset, owners)), device_id_type=mesh_id
        )

    loads = []
    for number, (source, target) in enumerate(
        [
            (gains_hbm, gains_ref),
            (owner_hbm, owner_ref),
            (channel_hbm, channel_ref),
            (base_hbm, base_ref),
            (pairs_hbm, pairs_ref),
            (coupling_hbm, coupling_ref),
            (observed_hbm, observed_ref),
            (keep_hbm, keep_ref),
            (duals_hbm, duals_ref),
            (consensus_hbm, consensus_ref),
        ]
    ):
        copy = pltpu.make_async_copy(source, target, local_sem.at[number])
        copy.start()
        loads.append(copy)

    pad[...] = jnp.zeros_like(pad)
    loads[0].wait()
    for owner in range(sub_count):
        for part in range(2):
            here = lay_pair(lambda number: gains_ref[owner * half + number, part], pad, half, width)
            gain_table[top * sub_count + owner, part] = here
            gain_codes[top * sub_count + owner, part] = (
                jnp.round(jnp.clip(here, -GAIN_MOST, GAIN_MOST) * (CODE_MOST / GAIN_MOST))
                .astype(jnp.int32)
                .astype(jnp.int16)
            )
    pl.semaphore_wait(barrier, owners - 1)
    gathers = []
    for rank in range(top):
        copy = pltpu.make_async_remote_copy(
            src_ref=gain_codes.at[pl.ds(top * sub_count, sub_count)],
            dst_ref=gain_codes.at[pl.ds(rank * sub_count, sub_count)],
            send_sem=gains_send.at[rank],
            recv_sem=gains_recv.at[rank],
            device_id={"chan": partners[rank]},
            device_id_type=mesh_id,
        )
        copy.start()
        gathers.append(copy)

    for copy in loads[1:4]:
        copy.wait()
    codes_v[...] = jnp.zeros_like(codes_v)
    named = owner_ref[...]
    rank_of = top - (named + chan - 2 * (named & chan))
    sort_tiles(rank_of, channel_ref[...], base_ref[...], codes_v, owners, sub_count, half, groups, bases * half)
    to_scalar = pltpu.make_async_copy(codes_v, codes, local_sem.at[len(loads)])
    to_scalar.start()

    loads[4].wait()
    turned[...] = jnp.zeros_like(turned)
    for base in range(bases):
        both = pairs_ref[base]
        turned[2 * base : 2 * base + 2, :] = both.astype(jnp.float32)
        for part in range(half):
            stations_of[base * half + part] = both + part * width
    columns = jnp.transpose(turned[...])
    lane = lax.broadcasted_iota(jnp.int32, (tile_rows, LANES), 1).astype(jnp.float32)
    for base in range(bases):
        for end in range(2):
            station = jnp.broadcast_to(columns[:, 2 * base + end : 2 * base + end + 1], lane.shape)
            for part in range(half):
                table[base * half + part, end * tile_rows : (end + 1) * tile_rows, :] = jnp.where(
                    station == lane - float(part * width), 1.0, 0.0
                ).astype(jnp.bfloat16)

    for copy in loads[5:]:
        copy.wait()
    step_rows = 2 * directions

    def widen(step, carry):
        span = pl.ds(pl.multiple_of(step * 8 * step_rows, 8 * step_rows), 8 * step_rows)
        coupling_t[...] = coupling_ref[span, :].astype(jnp.float32)
        for number in range(2):
            value = coupling_t[pl.ds(number, 8 * directions, stride=2), :]
            coupling_f[number, pl.ds(step * 8, 8)] = value.reshape(8, directions, tile_rows)
        return carry

    lax.fori_loop(0, tiles // 8, widen, 0)
    coupling_f[:, tiles:] = jnp.zeros((2, 1, directions, tile_rows), jnp.float32)
    observed_f[: 2 * tiles, :] = observed_ref[...].astype(jnp.float32)
    observed_f[2 * tiles :, :] = jnp.zeros((8, tile_rows), jnp.float32)
    lane_mask[:tiles, :] = jnp.where(keep_ref[...] > 0, 0, width - 1)
    lane_mask[tiles:, :] = jnp.zeros((8, tile_rows), jnp.int32)

    shape = (directions, LANES)
    row = lax.broadcasted_iota(jnp.int32, shape, 0)
    rho = jnp.zeros(shape, jnp.float32)
    for k in range(directions):
        rho = jnp.where(row == k, rho_ref[k], rho)
    place = lax.broadcasted_iota(jnp.int32, (owners, LANES), 1)
    of = lax.broadcasted_iota(jnp.int32, (owners, LANES), 0)
    everyone = basis_of((of * half + lax.div(place, width)).astype(jnp.float32), channels)
    for d in range(degree):
        basis_buf[d] = everyone[d]

    normal_rows = directions * directions
    out_rows = normal_rows + 2 * directions
    sums_ref[0] = jnp.zeros((out_rows, LANES), jnp.float32)
    upper = row < directions // 2
    tall = lax.broadcasted_iota(jnp.int32, (2 * directions, LANES), 0)
    turn = jnp.where((tall >= directions) & (tall < directions + directions // 2), 1.0, -1.0).astype(jnp.bfloat16)
    to_scalar.wait()
    for rank, copy in enumerate(gathers):
        copy.wait_recv()
        span = pl.ds(rank * sub_count, sub_count)
        gain_table[span] = gain_codes[span].astype(jnp.int32).astype(jnp.float32) * (GAIN_MOST / CODE_MOST)

    def spread(values):
        return jnp.broadcast_to(values, shape)

    def pick(values, index):
        return lax.gather(
            values,
            index[..., None],
            lax.GatherDimensionNumbers(
                offset_dims=(),
                collapsed_slice_dims=(1,),
                start_index_map=(1,),
                operand_batching_dims=(0,),
                start_indices_batching_dims=(0,),
            ),
            slice_sizes=(1, 1),
            mode=lax.GatherScatterMode.PROMISE_IN_BOUNDS,
        )

    def one_tile(slot):
        tile = jnp.clip(codes[0, slot], 0, tiles)
        entry = jnp.clip(codes[1, slot], 0, bases * half - 1)
        owner = jnp.clip(codes[2, slot], 0, owners - 1)
        real, imag = coupling_f[0, tile], coupling_f[1, tile]
        seen_real = spread(observed_f[pl.ds(2 * tile, 1), :])
        seen_imag = spread(observed_f[pl.ds(2 * tile + 1, 1), :])
        masked = spread(lane_mask[pl.ds(tile, 1), :])
        near = spread(stations_of[entry, pl.ds(0, 1), :]) | masked
        far = spread(stations_of[entry, pl.ds(1, 1), :]) | masked
        gain_real, gain_imag = gain_table[owner, 0], gain_table[owner, 1]
        near_real, near_imag = pick(gain_real, near), pick(gain_imag, near)
        far_real, far_imag = pick(gain_real, far), pick(gain_imag, far)
        slope_real = real * far_real + imag * far_imag
        slope_imag = imag * far_real - real * far_imag
        other_real = real * near_real - imag * near_imag
        other_imag = real * near_imag + imag * near_real
        return [
            end_rows(slope_real, slope_imag, seen_real, seen_imag, upper, turn, 1),
            end_rows(other_real, other_imag, seen_real, seen_imag, upper, turn, -1),
        ], table[entry]

    def sums_of(rank, which):
        return sums_ref[jnp.clip(codes[4, rank * sub_count + which], 0, groups)]

    def near_copy(rank, shift):
        return pltpu.make_async_remote_copy(
            src_ref=near_src.at[shift - 1, rank],
            dst_ref=near_buf.at[shift - 1, rank],
            send_sem=near_send.at[shift - 1, rank],
            recv_sem=near_recv.at[shift - 1, rank],
            device_id={"sub": lax.rem(sub + shift, sub_count)},
            device_id_type=mesh_id,
        )

    def far_copy(rank):
        return pltpu.make_async_remote_copy(
            src_ref=send_buf.at[rank],
            dst_ref=far_buf.at[rank],
            send_sem=far_send.at[rank],
            recv_sem=far_recv.at[rank],
            device_id={"chan": partners[rank]},
            device_id_type=mesh_id,
        )

    def start_near(rank):
        for shift in range(1, sub_count):
            near_src[shift - 1, rank] = encode(sums_of(rank, lax.rem(sub + shift, sub_count)), directions)
            near_copy(rank, shift).start()

    def add_near(rank):
        total = sums_of(rank, sub)
        for shift in range(1, sub_count):
            near_copy(rank, shift).wait_recv()
            total = total + decode(near_buf[shift - 1, rank], directions)
        return total

    def start_far(rank):
        send_buf[rank] = encode(add_near(rank), directions)
        far_copy(rank).start()

    def some_groups(step, carry):
        for rank, ready in enumerate(early):

            @pl.when(step == ready)
            def _():
                start_near(rank)

            @pl.when(step == ready + 1)
            def _():
                start_far(rank)

        base_group = step * UNROLL
        running = sums_ref[base_group]
        for number in range(UNROLL):
            group = base_group + number
            rows, entries = [], []
            for inner in range(GROUP):
                ends, entry = one_tile(group * GROUP + inner)
                rows.append(jnp.concatenate(ends, axis=1))
                entries.append(entry)
            total = None
            for inner in range(0, GROUP, 2):
                value = jnp.dot(
                    jnp.concatenate(rows[inner : inner + 2], axis=0),
                    jnp.concatenate(entries[inner : inner + 2], axis=1),
                    preferred_element_type=jnp.float32,
                )
                value = value[:out_rows, :LANES] + value[out_rows:, LANES:]
                total = value if total is None else total + value
            running = running * codes[3, group].astype(jnp.float32) + total
            sums_ref[group + 1] = running
        return carry

    steps = groups // UNROLL
    most = 3 * tiles // chan_count + sub_count * (GROUP - 1)
    early = []
    for rank in range(top):
        ready = -(-(rank + 1) * most // (GROUP * UNROLL))
        if ready + 1 < steps:
            early.append(ready)
    lax.fori_loop(0, steps, some_groups, 0)

    for rank in range(len(early), chan_count):
        start_near(rank)

    mine = [jnp.broadcast_to(basis_buf[d, pl.ds(me, 1), :], shape) for d in range(degree)]
    duals = [
        lay_pair(lambda number: duals_ref[number, part], pad, half, width) for part in range(2)
    ]
    anchors = []
    for part in range(2):
        anchor = jnp.zeros(shape, jnp.float32)
        for d in range(degree):
            anchor = anchor + mine[d] * lay_pair(
                lambda number: consensus_ref[d, part], pad, half, width
            )
        anchors.append(anchor)

    for rank in range(len(early), top):
        start_far(rank)
    total = add_near(top)
    for rank in range(top):
        far_copy(rank).wait_recv()
        total = total + decode(far_buf[rank], directions)

    group = [total[i * directions : (i + 1) * directions] for i in range(directions + 2)]
    solved = solve_hermitian(
        [group[7], group[0], group[1], group[6]],
        [group[2], group[3], group[4]],
        group[5],
        rho,
        group[directions] - duals[0] + rho * anchors[0],
        group[directions + 1] - duals[1] + rho * anchors[1],
    )
    weights[me] = jnp.concatenate(
        [solved[part] + duals[part] / rho for part in range(2)], axis=0
    ).astype(jnp.bfloat16)

    last = []
    for rank in range(chan_count):
        for shift in range(sub_count):
            if rank == top and shift == 0:
                continue
            number = rank * sub_count + shift
            copy = pltpu.make_async_remote_copy(
                src_ref=weights.at[me],
                dst_ref=weights.at[me],
                send_sem=last_send.at[number],
                recv_sem=last_recv.at[number],
                device_id={"chan": partners[rank], "sub": lax.rem(sub + shift, sub_count)},
                device_id_type=mesh_id,
            )
            copy.start()
            last.append(copy)

    def store(first, part, value):
        for number in range(half):
            out_ref[first + number, part] = (
                pltpu.roll(value, LANES - number * width, axis=1) if number else value
            )

    for part in range(2):
        store(0, part, solved[part])
    for copy in last:
        copy.wait_recv()
    inverse = inverse_gram(channels)
    totals = []
    for d in range(degree):
        value = jnp.zeros((2 * directions, LANES), jnp.float32)
        for number in range(owners):
            value = value + basis_buf[d, number : number + 1, :] * weights[number].astype(jnp.float32)
        folded = value
        for number in range(1, half):
            folded = folded + pltpu.roll(value, number * width, axis=1)
        totals.append(folded)
    fitted = jnp.zeros((2 * directions, LANES), jnp.float32)
    for d in range(degree):
        value = sum(float(inverse[d, e]) * totals[e] for e in range(degree))
        for part in range(2):
            out_ref[half + d, part] = value[part * directions : (part + 1) * directions]
        fitted = fitted + jnp.concatenate([mine[d], mine[d]], axis=0) * value
    for part in range(2):
        fit = fitted[part * directions : (part + 1) * directions]
        store(half + degree, part, duals[part] + rho * (solved[part] - fit))
    for copy in gathers:
        copy.wait_send()
    for rank in range(chan_count):
        for shift in range(1, sub_count):
            near_copy(rank, shift).wait_send()
        if rank < top:
            far_copy(rank).wait_send()
    for copy in last:
        copy.wait_send()


def deliver_kernel(result_ref, gains_out, consensus_out, duals_out):
    first = 0
    for ref in (gains_out, consensus_out, duals_out):
        count, _, _, stations = ref.shape
        for number in range(count):
            ref[number] = result_ref[first + number][:, :, :stations]
        first += count


def body(
    predicted_sky_response,
    measured_correlation,
    keep_indicator,
    tile_owner,
    tile_channel,
    tile_base,
    pairs,
    gains,
    duals,
    consensus,
    rho,
):
    channels_here, _, stations, directions = gains.shape
    chan_count = lax.axis_size("chan")
    sub_count = lax.axis_size("sub")
    half = channels_here // sub_count
    owners = chan_count * sub_count
    tiles, _, _, tile_rows = predicted_sky_response.shape
    bases = pairs.shape[0]
    degree = consensus.shape[0]
    width = LANES // half
    if chan_count & (chan_count - 1) or width & (width - 1) or stations >= width or tile_rows != LANES or directions != 8:
        raise ValueError("unsupported sizes")
    groups = -(-(tiles + owners * (GROUP - 1)) // GROUP)
    groups = -(-groups // UNROLL) * UNROLL
    code_width = -(-max(groups * GROUP, owners) // LANES) * LANES
    out_rows = directions * directions + 2 * directions
    coded = out_rows + 2 * directions
    gains_t = jnp.swapaxes(gains, 2, 3)
    duals_t = jnp.swapaxes(duals, 2, 3)
    consensus_t = jnp.swapaxes(consensus, 2, 3)
    operands = [
        tile_owner.reshape(1, tiles),
        tile_channel.reshape(1, tiles),
        tile_base.reshape(1, tiles),
        predicted_sky_response.reshape(tiles * 2 * directions, tile_rows),
        measured_correlation.reshape(tiles * 2, tile_rows),
        keep_indicator,
        pairs,
        gains_t,
        duals_t,
        consensus_t,
    ]
    vmem, dma = pltpu.VMEM, pltpu.SemaphoreType.DMA
    f32, bf16, i32 = jnp.float32, jnp.bfloat16, jnp.int32
    result = pl.pallas_call(
        functools.partial(whole_kernel, chan_count, sub_count, half, groups),
        out_shape=pltpu.VMEM((2 * half + degree, 2, directions, LANES), f32),
        in_specs=[pl.BlockSpec(memory_space=pltpu.SMEM)]
        + [pl.BlockSpec(memory_space=pl.ANY)] * len(operands),
        out_specs=pl.BlockSpec(memory_space=pltpu.VMEM),
        scratch_shapes=[vmem(x.shape, x.dtype) for x in operands]
        + [
            vmem((owners, 2, directions, LANES), f32),
            vmem((owners, 2, directions, LANES), jnp.int16),
            vmem((bases * half, 2 * tile_rows, LANES), bf16),
            vmem((LANES, tile_rows), f32),
            vmem((bases * half, 2, tile_rows), i32),
            vmem((2, tiles + 1, directions, tile_rows), f32),
            vmem((8 * 2 * directions, tile_rows), f32),
            vmem((2 * tiles + 8, tile_rows), f32),
            vmem((tiles + 8, tile_rows), i32),
            vmem((8, code_width), i32),
            pltpu.SMEM((8, code_width), i32),
            vmem((groups + 1, out_rows, LANES), f32),
            vmem((2, directions, LANES), f32),
            vmem((sub_count - 1, chan_count, coded, LANES), bf16),
            vmem((sub_count - 1, chan_count, coded, LANES), bf16),
            vmem((chan_count, coded, LANES), bf16),
            vmem((chan_count, coded, LANES), bf16),
            vmem((owners, 2 * directions, LANES), bf16),
            vmem((degree, owners, LANES), f32),
            dma((len(operands) + 1,)),
            dma((chan_count,)),
            dma((chan_count,)),
            dma((sub_count - 1, chan_count)),
            dma((sub_count - 1, chan_count)),
            dma((chan_count,)),
            dma((chan_count,)),
            dma((owners,)),
            dma((owners,)),
        ],
        compiler_params=pltpu.CompilerParams(
            collective_id=1, has_side_effects=True, vmem_limit_bytes=60 << 20
        ),
    )(rho, *[operands[i] for i in range(len(operands))])
    outputs = pl.pallas_call(
        deliver_kernel,
        out_shape=tuple(
            jax.ShapeDtypeStruct(x.shape, f32) for x in (duals_t, consensus_t, duals_t)
        ),
        in_specs=[pl.BlockSpec(memory_space=pltpu.VMEM)],
        out_specs=tuple(pl.BlockSpec(memory_space=pltpu.VMEM) for _ in range(3)),
    )(pltpu.with_memory_space_constraint(result, pltpu.VMEM))
    return tuple(jnp.swapaxes(x, 2, 3) for x in outputs)


def solution(mesh):
    placed = (
        P(("groups", "chan", "sub"), None, None, None),
        P(("groups", "chan", "sub"), None, None),
        P(("groups", "chan", "sub"), None),
        P(("groups", "chan", "sub"), None),
        P(("groups", "chan", "sub")),
        P(("groups", "chan", "sub")),
        P(),
        P(("groups", "chan"), None, None, None),
        P(("groups", "chan", "sub"), None, None, None),
        P("groups", None, None, None),
        P(),
    )
    return jax.shard_map(
        body,
        mesh=mesh,
        in_specs=placed,
        out_specs=(
            P(("groups", "chan", "sub"), None, None, None),
            P("groups", None, None, None),
            P(("groups", "chan", "sub"), None, None, None),
        ),
        check_vma=False,
    )
```

```python
import functools

import jax
import jax.numpy as jnp
import numpy as np
from jax import lax
from jax.experimental import pallas as pl
from jax.experimental.pallas import tpu as pltpu
from jax.sharding import PartitionSpec as P

LANES = 128
GROUP = 2
UNROLL = 66
GAIN_MOST = 5.0
CODE_MOST = 32767.0


def lay_pair(load, pad, half, width):
    total = None
    for part in range(half):
        block = load(part)
        pad[part % 2, :, : block.shape[1]] = block
        value = pad[part % 2]
        if part:
            value = pltpu.roll(value, part * width, axis=1)
        total = value if total is None else total + value
    return total


def basis_of(channel, channels):
    x = (2.0 * channel - (channels - 1)) / max(channels - 1, 1)
    return [
        jnp.ones_like(x),
        x,
        0.5 * (3.0 * x * x - 1.0),
        0.5 * (5.0 * x * x * x - 3.0 * x),
    ]


def inverse_gram(channels):
    f = np.arange(channels, dtype=np.float64)
    x = (2.0 * f - (channels - 1)) / max(channels - 1, 1)
    basis = np.stack([np.ones_like(x), x, 0.5 * (3 * x * x - 1), 0.5 * (5 * x * x * x - 3 * x)])
    return np.linalg.inv(basis @ basis.T)


def end_rows(real, imag, seen_real, seen_imag, upper, turn, sign):
    directions = real.shape[0]

    def pair(first, second):
        return jnp.concatenate([first, second], axis=0).astype(jnp.bfloat16)

    def turned(value, shift):
        return pltpu.roll(value, directions - shift, axis=0)

    left, right = pair(real, real), pair(imag, imag)
    ahead_real = pair(turned(real, 1), turned(real, 2))
    ahead_imag = pair(turned(imag, 1), turned(imag, 2))
    both = left * ahead_real + right * ahead_imag
    third_real, third_imag = turned(real, 3), turned(imag, 3)
    fourth_real, fourth_imag = turned(real, 4), turned(imag, 4)
    ahead_one = pair(third_imag, jnp.where(upper, fourth_real, fourth_imag))
    ahead_two = pair(third_real, jnp.where(upper, fourth_imag, fourth_real))
    if sign > 0:
        cross = left * ahead_imag - right * ahead_real
        mixed = left * ahead_one + right * turn * ahead_two
        side_imag = real * seen_imag - imag * seen_real
    else:
        cross = right * ahead_real - left * ahead_imag
        mixed = left * turn * ahead_one + right * ahead_two
        side_imag = imag * seen_real - real * seen_imag
    plain = left * pair(third_real, real) + right * pair(third_imag, imag)
    side_real = real * seen_real + imag * seen_imag
    return jnp.concatenate([both, cross, mixed, plain, pair(side_real, side_imag)], axis=0)


def solve_hermitian(groups_real, groups_imag, mixed, ridge, side_real, side_imag):
    directions = side_real.shape[0]
    middle = directions // 2
    row = lax.broadcasted_iota(jnp.int32, side_real.shape, 0)
    upper = row < middle
    swapped = pltpu.roll(mixed, middle, axis=0)
    real = {0: groups_real[0] + ridge, middle: jnp.where(upper, mixed, swapped)}
    imag = {0: jnp.zeros_like(ridge), middle: jnp.where(upper, -swapped, mixed)}
    for d in range(1, middle):
        real[d], imag[d] = groups_real[d], groups_imag[d - 1]
        real[directions - d] = pltpu.roll(groups_real[d], d, axis=0)
        imag[directions - d] = -pltpu.roll(groups_imag[d - 1], d, axis=0)
    columns = []
    for l in range(directions):
        column_real, column_imag = real[l], imag[l]
        for k in range(1, directions):
            here = row == k
            d = (l - k) % directions
            column_real = jnp.where(here, real[d], column_real)
            column_imag = jnp.where(here, imag[d], column_imag)
        columns.append((column_real, column_imag))
    columns.append((side_real, side_imag))
    scale = jnp.zeros_like(ridge)
    for j in range(directions):
        pivot_real, pivot_imag = columns[j]
        inverse = 1.0 / pivot_real[j : j + 1]
        here = row == j
        scale = jnp.where(here, jnp.broadcast_to(inverse, scale.shape), scale)
        factor_real = jnp.where(here, 0.0, pivot_real * inverse)
        factor_imag = jnp.where(here, 0.0, pivot_imag * inverse)
        for l in range(j + 1, directions + 1):
            value_real, value_imag = columns[l]
            head_real, head_imag = value_real[j : j + 1], value_imag[j : j + 1]
            columns[l] = (
                value_real - (factor_real * head_real - factor_imag * head_imag),
                value_imag - (factor_real * head_imag + factor_imag * head_real),
            )
    return columns[-1][0] * scale, columns[-1][1] * scale


def encode(sums, directions):
    normal_rows = directions * directions
    side = sums[normal_rows:]
    high = side.astype(jnp.bfloat16)
    low = (side - high.astype(jnp.float32)).astype(jnp.bfloat16)
    return jnp.concatenate([sums[:normal_rows].astype(jnp.bfloat16), high, low], axis=0)


def decode(coded, directions):
    wide = coded.astype(jnp.float32)
    normal_rows = directions * directions
    side_rows = 2 * directions
    high, low = wide[normal_rows : normal_rows + side_rows], wide[normal_rows + side_rows :]
    return jnp.concatenate([wide[:normal_rows], high + low], axis=0)


def sort_tiles(rank, channel, base, codes, owners, sub_count, half, groups, entries):
    tiles = rank.shape[1]
    slots = groups * GROUP
    sub = jnp.zeros_like(channel)
    for number in range(1, sub_count):
        sub = sub + jnp.where(channel >= number * half, 1, 0)
    place = channel - sub * half
    key = rank * sub_count + sub
    entry = base * half + place
    same = jnp.where(
        lax.broadcasted_iota(jnp.int32, (owners, tiles), 0) == jnp.broadcast_to(key, (owners, tiles)), 1.0, 0.0
    )
    same_b = same.astype(jnp.bfloat16)
    until = jnp.where(
        lax.broadcasted_iota(jnp.int32, (tiles, tiles), 0) <= lax.broadcasted_iota(jnp.int32, (tiles, tiles), 1),
        1.0,
        0.0,
    ).astype(jnp.bfloat16)
    nt = (((1,), (1,)), ((), ()))
    count = jnp.dot(same_b, until, preferred_element_type=jnp.float32)

    def pieces(value):
        return jnp.floor((value + float(GROUP - 1)) * (1.0 / GROUP))

    wide = (owners, LANES)
    used = pieces(jnp.broadcast_to(count[:, tiles - 1 : tiles], wide))
    square = (owners, owners)
    row, column = lax.broadcasted_iota(jnp.int32, square, 0), lax.broadcasted_iota(jnp.int32, square, 1)
    before = jnp.where(column < row, 1.0, 0.0).astype(jnp.bfloat16)
    start = jnp.dot(before, used.astype(jnp.bfloat16), preferred_element_type=jnp.float32)
    position = jnp.sum(same * (start[:, :1] * float(GROUP) + count), axis=0, keepdims=True) - 1.0
    left = tiles - lax.broadcasted_iota(jnp.int32, (1, tiles), 1)
    features = jnp.concatenate(
        [left & 255, lax.shift_right_logical(left, 8), entry, key, jnp.zeros((4, tiles), jnp.int32)], axis=0
    )
    chosen = jnp.where(
        lax.broadcasted_iota(jnp.int32, (slots, tiles), 0)
        == jnp.broadcast_to(position.astype(jnp.int32), (slots, tiles)),
        1.0,
        0.0,
    ).astype(jnp.bfloat16)
    sorted_features = lax.dot_general(
        features.astype(jnp.float32).astype(jnp.bfloat16), chosen, nt, preferred_element_type=jnp.float32
    )
    tile = float(tiles) - (sorted_features[0:1] + 256.0 * sorted_features[1:2])
    codes[0:1, :slots] = jnp.clip(tile.astype(jnp.int32), 0, tiles)
    codes[1:2, :slots] = jnp.clip(sorted_features[2:3].astype(jnp.int32), 0, entries - 1)
    codes[2:3, :slots] = jnp.clip(sorted_features[3:4].astype(jnp.int32), 0, owners - 1)
    spread = -(-groups // LANES) * LANES
    number = lax.broadcasted_iota(jnp.int32, (owners, spread), 1).astype(jnp.float32)
    first = (jnp.broadcast_to(start[:, :1], number.shape) == number) & (
        jnp.broadcast_to(used[:, :1], number.shape) > 0.5
    )
    carried = 1.0 - jnp.max(jnp.where(first, 1.0, 0.0), axis=0, keepdims=True)
    codes[3:4, :spread] = carried.astype(jnp.int32)
    used_row = pieces(lax.dot_general(jnp.ones((8, tiles), jnp.bfloat16), same_b, nt, preferred_element_type=jnp.float32))
    upto = jnp.where(row <= column, 1.0, 0.0).astype(jnp.bfloat16)
    end = jnp.dot(used_row.astype(jnp.bfloat16), upto, preferred_element_type=jnp.float32)
    last = jnp.where(used_row > 0.5, end, 0.0).astype(jnp.int32)
    codes[4:5, :owners] = jnp.clip(last[0:1], 0, groups)


def whole_kernel(
    chan_count,
    sub_count,
    half,
    groups,
    rho_hbm,
    owner_hbm,
    channel_hbm,
    base_hbm,
    coupling_hbm,
    observed_hbm,
    keep_hbm,
    pairs_hbm,
    gains_hbm,
    duals_hbm,
    consensus_hbm,
    out_ref,
    rho_ref,
    owner_ref,
    channel_ref,
    base_ref,
    coupling_ref,
    observed_ref,
    keep_ref,
    pairs_ref,
    gains_ref,
    duals_ref,
    consensus_ref,
    gain_table,
    gain_codes,
    table,
    turned,
    stations_of,
    coupling_f,
    coupling_t,
    observed_f,
    lane_mask,
    codes_v,
    codes,
    sums_ref,
    pad,
    near_src,
    near_buf,
    send_buf,
    far_buf,
    weights,
    basis_buf,
    local_sem,
    gains_send,
    gains_recv,
    near_send,
    near_recv,
    far_send,
    far_recv,
    last_send,
    last_recv,
):
    chan, sub = lax.axis_index("chan"), lax.axis_index("sub")
    owners = chan_count * sub_count
    channels = owners * half
    width = LANES // half
    directions, stations = duals_ref.shape[2], duals_ref.shape[3]
    degree = consensus_ref.shape[0]
    tiles = keep_ref.shape[0]
    tile_rows = keep_ref.shape[1]
    bases = pairs_ref.shape[0]
    me = chan * sub_count + sub
    mesh_id = pl.DeviceIdType.MESH

    top = chan_count - 1

    def partner(rank):
        flips, result, bit = top - rank, chan, 1
        while bit < chan_count:
            if flips & bit:
                result = result + bit * (1 - 2 * lax.rem(lax.div(chan, bit), 2))
            bit *= 2
        return result

    partners = [partner(rank) for rank in range(chan_count)]

    barrier = pltpu.get_barrier_semaphore()
    for rank in range(chan_count):
        for shift in range(sub_count):
            if rank < top or shift:
                pl.semaphore_signal(
                    barrier,
                    inc=1,
                    device_id={"chan": partners[rank], "sub": lax.rem(sub + shift, sub_count)},
                    device_id_type=mesh_id,
                )

    loads = []
    for number, (source, target) in enumerate(
        [
            (gains_hbm, gains_ref),
            (owner_hbm, owner_ref),
            (channel_hbm, channel_ref),
            (base_hbm, base_ref),
            (pairs_hbm, pairs_ref),
            (coupling_hbm, coupling_ref),
            (observed_hbm, observed_ref),
            (keep_hbm, keep_ref),
            (duals_hbm, duals_ref),
            (consensus_hbm, consensus_ref),
            (rho_hbm, rho_ref),
        ]
    ):
        copy = pltpu.make_async_copy(source, target, local_sem.at[number])
        copy.start()
        loads.append(copy)

    pad[...] = jnp.zeros_like(pad)
    loads[0].wait()
    for owner in range(sub_count):
        for part in range(2):
            here = lay_pair(lambda number: gains_ref[owner * half + number, part], pad, half, width)
            gain_table[top * sub_count + owner, part] = here
            gain_codes[top * sub_count + owner, part] = (
                jnp.round(jnp.clip(here, -GAIN_MOST, GAIN_MOST) * (CODE_MOST / GAIN_MOST))
                .astype(jnp.int32)
                .astype(jnp.int16)
            )
    pl.semaphore_wait(barrier, owners - 1)
    gathers = []
    for rank in range(top):
        copy = pltpu.make_async_remote_copy(
            src_ref=gain_codes.at[pl.ds(top * sub_count, sub_count)],
            dst_ref=gain_codes.at[pl.ds(rank * sub_count, sub_count)],
            send_sem=gains_send.at[rank],
            recv_sem=gains_recv.at[rank],
            device_id={"chan": partners[rank]},
            device_id_type=mesh_id,
        )
        copy.start()
        gathers.append(copy)

    for copy in loads[1:4]:
        copy.wait()
    codes_v[...] = jnp.zeros_like(codes_v)
    named = owner_ref[...]
    rank_of = top - (named + chan - 2 * (named & chan))
    sort_tiles(rank_of, channel_ref[...], base_ref[...], codes_v, owners, sub_count, half, groups, bases * half)
    to_scalar = pltpu.make_async_copy(codes_v, codes, local_sem.at[len(loads)])
    to_scalar.start()

    loads[4].wait()
    turned[...] = jnp.zeros_like(turned)
    for base in range(bases):
        both = pairs_ref[base]
        turned[2 * base : 2 * base + 2, :] = both.astype(jnp.float32)
        for part in range(half):
            stations_of[base * half + part] = both + part * width
    columns = jnp.transpose(turned[...])
    lane = lax.broadcasted_iota(jnp.int32, (tile_rows, LANES), 1).astype(jnp.float32)
    for base in range(bases):
        for end in range(2):
            station = jnp.broadcast_to(columns[:, 2 * base + end : 2 * base + end + 1], lane.shape)
            for part in range(half):
                table[base * half + part, end * tile_rows : (end + 1) * tile_rows, :] = jnp.where(
                    station == lane - float(part * width), 1.0, 0.0
                ).astype(jnp.bfloat16)

    for copy in loads[5:]:
        copy.wait()
    step_rows = 2 * directions

    def widen(step, carry):
        span = pl.ds(pl.multiple_of(step * 8 * step_rows, 8 * step_rows), 8 * step_rows)
        coupling_t[...] = coupling_ref[span, :].astype(jnp.float32)
        for number in range(2):
            value = coupling_t[pl.ds(number, 8 * directions, stride=2), :]
            coupling_f[number, pl.ds(step * 8, 8)] = value.reshape(8, directions, tile_rows)
        return carry

    lax.fori_loop(0, tiles // 8, widen, 0)
    coupling_f[:, tiles:] = jnp.zeros((2, 1, directions, tile_rows), jnp.float32)
    observed_f[: 2 * tiles, :] = observed_ref[...].astype(jnp.float32)
    observed_f[2 * tiles :, :] = jnp.zeros((8, tile_rows), jnp.float32)
    lane_mask[:tiles, :] = jnp.where(keep_ref[...] > 0, 0, width - 1)
    lane_mask[tiles:, :] = jnp.zeros((8, tile_rows), jnp.int32)

    shape = (directions, LANES)
    row = lax.broadcasted_iota(jnp.int32, shape, 0)
    rho = jnp.zeros(shape, jnp.float32)
    for k in range(directions):
        rho = jnp.where(row == k, rho_ref[k], rho)
    place = lax.broadcasted_iota(jnp.int32, (owners, LANES), 1)
    of = lax.broadcasted_iota(jnp.int32, (owners, LANES), 0)
    everyone = basis_of((of * half + lax.div(place, width)).astype(jnp.float32), channels)
    for d in range(degree):
        basis_buf[d] = everyone[d]

    normal_rows = directions * directions
    out_rows = normal_rows + 2 * directions
    sums_ref[0] = jnp.zeros((out_rows, LANES), jnp.float32)
    upper = row < directions // 2
    tall = lax.broadcasted_iota(jnp.int32, (2 * directions, LANES), 0)
    turn = jnp.where((tall >= directions) & (tall < directions + directions // 2), 1.0, -1.0).astype(jnp.bfloat16)
    to_scalar.wait()
    for rank, copy in enumerate(gathers):
        copy.wait_recv()
        span = pl.ds(rank * sub_count, sub_count)
        gain_table[span] = gain_codes[span].astype(jnp.int32).astype(jnp.float32) * (GAIN_MOST / CODE_MOST)

    def spread(values):
        return jnp.broadcast_to(values, shape)

    def pick(values, index):
        return lax.gather(
            values,
            index[..., None],
            lax.GatherDimensionNumbers(
                offset_dims=(),
                collapsed_slice_dims=(1,),
                start_index_map=(1,),
                operand_batching_dims=(0,),
                start_indices_batching_dims=(0,),
            ),
            slice_sizes=(1, 1),
            mode=lax.GatherScatterMode.PROMISE_IN_BOUNDS,
        )

    def one_tile(slot):
        tile = jnp.clip(codes[0, slot], 0, tiles)
        entry = jnp.clip(codes[1, slot], 0, bases * half - 1)
        owner = jnp.clip(codes[2, slot], 0, owners - 1)
        real, imag = coupling_f[0, tile], coupling_f[1, tile]
        seen_real = spread(observed_f[pl.ds(2 * tile, 1), :])
        seen_imag = spread(observed_f[pl.ds(2 * tile + 1, 1), :])
        masked = spread(lane_mask[pl.ds(tile, 1), :])
        near = spread(stations_of[entry, pl.ds(0, 1), :]) | masked
        far = spread(stations_of[entry, pl.ds(1, 1), :]) | masked
        gain_real, gain_imag = gain_table[owner, 0], gain_table[owner, 1]
        near_real, near_imag = pick(gain_real, near), pick(gain_imag, near)
        far_real, far_imag = pick(gain_real, far), pick(gain_imag, far)
        slope_real = real * far_real + imag * far_imag
        slope_imag = imag * far_real - real * far_imag
        other_real = real * near_real - imag * near_imag
        other_imag = real * near_imag + imag * near_real
        return [
            end_rows(slope_real, slope_imag, seen_real, seen_imag, upper, turn, 1),
            end_rows(other_real, other_imag, seen_real, seen_imag, upper, turn, -1),
        ], table[entry]

    def sums_of(rank, which):
        return sums_ref[jnp.clip(codes[4, rank * sub_count + which], 0, groups)]

    def near_copy(rank, shift):
        return pltpu.make_async_remote_copy(
            src_ref=near_src.at[shift - 1, rank],
            dst_ref=near_buf.at[shift - 1, rank],
            send_sem=near_send.at[shift - 1, rank],
            recv_sem=near_recv.at[shift - 1, rank],
            device_id={"sub": lax.rem(sub + shift, sub_count)},
            device_id_type=mesh_id,
        )

    def far_copy(rank):
        return pltpu.make_async_remote_copy(
            src_ref=send_buf.at[rank],
            dst_ref=far_buf.at[rank],
            send_sem=far_send.at[rank],
            recv_sem=far_recv.at[rank],
            device_id={"chan": partners[rank]},
            device_id_type=mesh_id,
        )

    def start_near(rank):
        for shift in range(1, sub_count):
            near_src[shift - 1, rank] = encode(sums_of(rank, lax.rem(sub + shift, sub_count)), directions)
            near_copy(rank, shift).start()

    def add_near(rank):
        total = sums_of(rank, sub)
        for shift in range(1, sub_count):
            near_copy(rank, shift).wait_recv()
            total = total + decode(near_buf[shift - 1, rank], directions)
        return total

    def start_far(rank):
        send_buf[rank] = encode(add_near(rank), directions)
        far_copy(rank).start()

    def some_groups(step, carry):
        for rank, ready in enumerate(early):

            @pl.when(step == ready)
            def _():
                start_near(rank)

            @pl.when(step == ready + 1)
            def _():
                start_far(rank)

        base_group = step * UNROLL
        running = sums_ref[base_group]
        for number in range(UNROLL):
            group = base_group + number
            rows, entries = [], []
            for inner in range(GROUP):
                ends, entry = one_tile(group * GROUP + inner)
                rows.append(jnp.concatenate(ends, axis=1))
                entries.append(entry)
            total = None
            for inner in range(0, GROUP, 2):
                value = jnp.dot(
                    jnp.concatenate(rows[inner : inner + 2], axis=0),
                    jnp.concatenate(entries[inner : inner + 2], axis=1),
                    preferred_element_type=jnp.float32,
                )
                value = value[:out_rows, :LANES] + value[out_rows:, LANES:]
                total = value if total is None else total + value
            running = running * codes[3, group].astype(jnp.float32) + total
            sums_ref[group + 1] = running
        return carry

    steps = groups // UNROLL
    most = 3 * tiles // chan_count + sub_count * (GROUP - 1)
    early = []
    for rank in range(top):
        ready = -(-(rank + 1) * most // (GROUP * UNROLL))
        if ready + 1 < steps:
            early.append(ready)
    lax.fori_loop(0, steps, some_groups, 0)

    for rank in range(len(early), chan_count):
        start_near(rank)

    mine = [jnp.broadcast_to(basis_buf[d, pl.ds(me, 1), :], shape) for d in range(degree)]
    duals = [
        lay_pair(lambda number: duals_ref[number, part], pad, half, width) for part in range(2)
    ]
    anchors = []
    for part in range(2):
        anchor = jnp.zeros(shape, jnp.float32)
        for d in range(degree):
            anchor = anchor + mine[d] * lay_pair(
                lambda number: consensus_ref[d, part], pad, half, width
            )
        anchors.append(anchor)

    for rank in range(len(early), top):
        start_far(rank)
    total = add_near(top)
    for rank in range(top):
        far_copy(rank).wait_recv()
        total = total + decode(far_buf[rank], directions)

    group = [total[i * directions : (i + 1) * directions] for i in range(directions + 2)]
    solved = solve_hermitian(
        [group[7], group[0], group[1], group[6]],
        [group[2], group[3], group[4]],
        group[5],
        rho,
        group[directions] - duals[0] + rho * anchors[0],
        group[directions + 1] - duals[1] + rho * anchors[1],
    )
    weights[me] = jnp.concatenate(
        [solved[part] + duals[part] / rho for part in range(2)], axis=0
    ).astype(jnp.bfloat16)

    last = []
    for rank in range(chan_count):
        for shift in range(sub_count):
            if rank == top and shift == 0:
                continue
            number = rank * sub_count + shift
            copy = pltpu.make_async_remote_copy(
                src_ref=weights.at[me],
                dst_ref=weights.at[me],
                send_sem=last_send.at[number],
                recv_sem=last_recv.at[number],
                device_id={"chan": partners[rank], "sub": lax.rem(sub + shift, sub_count)},
                device_id_type=mesh_id,
            )
            copy.start()
            last.append(copy)

    def store(first, part, value):
        for number in range(half):
            out_ref[first + number, part] = (
                pltpu.roll(value, LANES - number * width, axis=1) if number else value
            )

    for part in range(2):
        store(0, part, solved[part])
    for copy in last:
        copy.wait_recv()
    inverse = inverse_gram(channels)
    totals = []
    for d in range(degree):
        value = jnp.zeros((2 * directions, LANES), jnp.float32)
        for number in range(owners):
            value = value + basis_buf[d, number : number + 1, :] * weights[number].astype(jnp.float32)
        folded = value
        for number in range(1, half):
            folded = folded + pltpu.roll(value, number * width, axis=1)
        totals.append(folded)
    fitted = jnp.zeros((2 * directions, LANES), jnp.float32)
    for d in range(degree):
        value = sum(float(inverse[d, e]) * totals[e] for e in range(degree))
        for part in range(2):
            out_ref[half + d, part] = value[part * directions : (part + 1) * directions]
        fitted = fitted + jnp.concatenate([mine[d], mine[d]], axis=0) * value
    for part in range(2):
        fit = fitted[part * directions : (part + 1) * directions]
        store(half + degree, part, duals[part] + rho * (solved[part] - fit))
    for copy in gathers:
        copy.wait_send()
    for rank in range(chan_count):
        for shift in range(1, sub_count):
            near_copy(rank, shift).wait_send()
        if rank < top:
            far_copy(rank).wait_send()
    for copy in last:
        copy.wait_send()


def deliver_kernel(result_ref, gains_out, consensus_out, duals_out):
    first = 0
    for ref in (gains_out, consensus_out, duals_out):
        count, _, _, stations = ref.shape
        for number in range(count):
            ref[number] = result_ref[first + number][:, :, :stations]
        first += count


def body(
    predicted_sky_response,
    measured_correlation,
    keep_indicator,
    tile_owner,
    tile_channel,
    tile_base,
    pairs,
    gains,
    duals,
    consensus,
    rho,
):
    channels_here, _, stations, directions = gains.shape
    chan_count = lax.axis_size("chan")
    sub_count = lax.axis_size("sub")
    half = channels_here // sub_count
    owners = chan_count * sub_count
    tiles, _, _, tile_rows = predicted_sky_response.shape
    bases = pairs.shape[0]
    degree = consensus.shape[0]
    width = LANES // half
    if chan_count & (chan_count - 1) or width & (width - 1) or stations >= width or tile_rows != LANES or directions != 8:
        raise ValueError("unsupported sizes")
    groups = -(-(tiles + owners * (GROUP - 1)) // GROUP)
    groups = -(-groups // UNROLL) * UNROLL
    code_width = -(-max(groups * GROUP, owners) // LANES) * LANES
    out_rows = directions * directions + 2 * directions
    coded = out_rows + 2 * directions
    gains_t = jnp.swapaxes(gains, 2, 3)
    duals_t = jnp.swapaxes(duals, 2, 3)
    consensus_t = jnp.swapaxes(consensus, 2, 3)
    operands = [
        tile_owner.reshape(1, tiles),
        tile_channel.reshape(1, tiles),
        tile_base.reshape(1, tiles),
        predicted_sky_response.reshape(tiles * 2 * directions, tile_rows),
        measured_correlation.reshape(tiles * 2, tile_rows),
        keep_indicator,
        pairs,
        gains_t,
        duals_t,
        consensus_t,
    ]
    vmem, dma = pltpu.VMEM, pltpu.SemaphoreType.DMA
    f32, bf16, i32 = jnp.float32, jnp.bfloat16, jnp.int32
    result = pl.pallas_call(
        functools.partial(whole_kernel, chan_count, sub_count, half, groups),
        out_shape=pltpu.VMEM((2 * half + degree, 2, directions, LANES), f32),
        in_specs=[pl.BlockSpec(memory_space=pl.ANY)] * (len(operands) + 1),
        out_specs=pl.BlockSpec(memory_space=pltpu.VMEM),
        scratch_shapes=[pltpu.SMEM(rho.shape, f32)]
        + [vmem(x.shape, x.dtype) for x in operands]
        + [
            vmem((owners, 2, directions, LANES), f32),
            vmem((owners, 2, directions, LANES), jnp.int16),
            vmem((bases * half, 2 * tile_rows, LANES), bf16),
            vmem((LANES, tile_rows), f32),
            vmem((bases * half, 2, tile_rows), i32),
            vmem((2, tiles + 1, directions, tile_rows), f32),
            vmem((8 * 2 * directions, tile_rows), f32),
            vmem((2 * tiles + 8, tile_rows), f32),
            vmem((tiles + 8, tile_rows), i32),
            vmem((8, code_width), i32),
            pltpu.SMEM((8, code_width), i32),
            vmem((groups + 1, out_rows, LANES), f32),
            vmem((2, directions, LANES), f32),
            vmem((sub_count - 1, chan_count, coded, LANES), bf16),
            vmem((sub_count - 1, chan_count, coded, LANES), bf16),
            vmem((chan_count, coded, LANES), bf16),
            vmem((chan_count, coded, LANES), bf16),
            vmem((owners, 2 * directions, LANES), bf16),
            vmem((degree, owners, LANES), f32),
            dma((len(operands) + 2,)),
            dma((chan_count,)),
            dma((chan_count,)),
            dma((sub_count - 1, chan_count)),
            dma((sub_count - 1, chan_count)),
            dma((chan_count,)),
            dma((chan_count,)),
            dma((owners,)),
            dma((owners,)),
        ],
        compiler_params=pltpu.CompilerParams(
            collective_id=1, has_side_effects=True, vmem_limit_bytes=60 << 20
        ),
    )(rho, *operands)
    outputs = pl.pallas_call(
        deliver_kernel,
        out_shape=tuple(
            jax.ShapeDtypeStruct(x.shape, f32) for x in (duals_t, consensus_t, duals_t)
        ),
        in_specs=[pl.BlockSpec(memory_space=pltpu.VMEM)],
        out_specs=tuple(pl.BlockSpec(memory_space=pltpu.VMEM) for _ in range(3)),
    )(pltpu.with_memory_space_constraint(result, pltpu.VMEM))
    return tuple(jnp.swapaxes(x, 2, 3) for x in outputs)


def solution(mesh):
    placed = (
        P(("groups", "chan", "sub"), None, None, None),
        P(("groups", "chan", "sub"), None, None),
        P(("groups", "chan", "sub"), None),
        P(("groups", "chan", "sub"), None),
        P(("groups", "chan", "sub")),
        P(("groups", "chan", "sub")),
        P(),
        P(("groups", "chan"), None, None, None),
        P(("groups", "chan", "sub"), None, None, None),
        P("groups", None, None, None),
        P(),
    )
    return jax.shard_map(
        body,
        mesh=mesh,
        in_specs=placed,
        out_specs=(
            P(("groups", "chan", "sub"), None, None, None),
            P("groups", None, None, None),
            P(("groups", "chan", "sub"), None, None, None),
        ),
        check_vma=False,
    )
```

```python
import functools

import jax
import jax.numpy as jnp
import numpy as np
from jax import lax
from jax.experimental import pallas as pl
from jax.experimental.pallas import tpu as pltpu
from jax.sharding import PartitionSpec as P

LANES = 128
GROUP = 2
UNROLL = 66
GAIN_MOST = 5.0
CODE_MOST = 32767.0


def lay_pair(load, pad, half, width):
    total = None
    for part in range(half):
        block = load(part)
        pad[part % 2, :, : block.shape[1]] = block
        value = pad[part % 2]
        if part:
            value = pltpu.roll(value, part * width, axis=1)
        total = value if total is None else total + value
    return total


def basis_of(channel, channels):
    x = (2.0 * channel - (channels - 1)) / max(channels - 1, 1)
    return [
        jnp.ones_like(x),
        x,
        0.5 * (3.0 * x * x - 1.0),
        0.5 * (5.0 * x * x * x - 3.0 * x),
    ]


def inverse_gram(channels):
    f = np.arange(channels, dtype=np.float64)
    x = (2.0 * f - (channels - 1)) / max(channels - 1, 1)
    basis = np.stack([np.ones_like(x), x, 0.5 * (3 * x * x - 1), 0.5 * (5 * x * x * x - 3 * x)])
    return np.linalg.inv(basis @ basis.T)


def end_rows(real, imag, seen_real, seen_imag, upper, turn, sign):
    directions = real.shape[0]

    def pair(first, second):
        return jnp.concatenate([first, second], axis=0).astype(jnp.bfloat16)

    def turned(value, shift):
        return pltpu.roll(value, directions - shift, axis=0)

    left, right = pair(real, real), pair(imag, imag)
    ahead_real = pair(turned(real, 1), turned(real, 2))
    ahead_imag = pair(turned(imag, 1), turned(imag, 2))
    both = left * ahead_real + right * ahead_imag
    third_real, third_imag = turned(real, 3), turned(imag, 3)
    fourth_real, fourth_imag = turned(real, 4), turned(imag, 4)
    ahead_one = pair(third_imag, jnp.where(upper, fourth_real, fourth_imag))
    ahead_two = pair(third_real, jnp.where(upper, fourth_imag, fourth_real))
    if sign > 0:
        cross = left * ahead_imag - right * ahead_real
        mixed = left * ahead_one + right * turn * ahead_two
        side_imag = real * seen_imag - imag * seen_real
    else:
        cross = right * ahead_real - left * ahead_imag
        mixed = left * turn * ahead_one + right * ahead_two
        side_imag = imag * seen_real - real * seen_imag
    plain = left * pair(third_real, real) + right * pair(third_imag, imag)
    side_real = real * seen_real + imag * seen_imag
    return jnp.concatenate([both, cross, mixed, plain, pair(side_real, side_imag)], axis=0)


def solve_hermitian(groups_real, groups_imag, mixed, ridge, side_real, side_imag):
    directions = side_real.shape[0]
    middle = directions // 2
    row = lax.broadcasted_iota(jnp.int32, side_real.shape, 0)
    upper = row < middle
    swapped = pltpu.roll(mixed, middle, axis=0)
    real = {0: groups_real[0] + ridge, middle: jnp.where(upper, mixed, swapped)}
    imag = {0: jnp.zeros_like(ridge), middle: jnp.where(upper, -swapped, mixed)}
    for d in range(1, middle):
        real[d], imag[d] = groups_real[d], groups_imag[d - 1]
        real[directions - d] = pltpu.roll(groups_real[d], d, axis=0)
        imag[directions - d] = -pltpu.roll(groups_imag[d - 1], d, axis=0)
    columns = []
    for l in range(directions):
        column_real, column_imag = real[l], imag[l]
        for k in range(1, directions):
            here = row == k
            d = (l - k) % directions
            column_real = jnp.where(here, real[d], column_real)
            column_imag = jnp.where(here, imag[d], column_imag)
        columns.append((column_real, column_imag))
    columns.append((side_real, side_imag))
    scale = jnp.zeros_like(ridge)
    for j in range(directions):
        pivot_real, pivot_imag = columns[j]
        inverse = 1.0 / pivot_real[j : j + 1]
        here = row == j
        scale = jnp.where(here, jnp.broadcast_to(inverse, scale.shape), scale)
        factor_real = jnp.where(here, 0.0, pivot_real * inverse)
        factor_imag = jnp.where(here, 0.0, pivot_imag * inverse)
        for l in range(j + 1, directions + 1):
            value_real, value_imag = columns[l]
            head_real, head_imag = value_real[j : j + 1], value_imag[j : j + 1]
            columns[l] = (
                value_real - (factor_real * head_real - factor_imag * head_imag),
                value_imag - (factor_real * head_imag + factor_imag * head_real),
            )
    return columns[-1][0] * scale, columns[-1][1] * scale


def encode(sums, directions):
    normal_rows = directions * directions
    side = sums[normal_rows:]
    high = side.astype(jnp.bfloat16)
    low = (side - high.astype(jnp.float32)).astype(jnp.bfloat16)
    return jnp.concatenate([sums[:normal_rows].astype(jnp.bfloat16), high, low], axis=0)


def decode(coded, directions):
    wide = coded.astype(jnp.float32)
    normal_rows = directions * directions
    side_rows = 2 * directions
    high, low = wide[normal_rows : normal_rows + side_rows], wide[normal_rows + side_rows :]
    return jnp.concatenate([wide[:normal_rows], high + low], axis=0)


def sort_tiles(rank, channel, base, codes, owners, sub_count, half, groups, entries):
    tiles = rank.shape[1]
    slots = groups * GROUP
    sub = jnp.zeros_like(channel)
    for number in range(1, sub_count):
        sub = sub + jnp.where(channel >= number * half, 1, 0)
    place = channel - sub * half
    key = rank * sub_count + sub
    entry = base * half + place
    same = jnp.where(
        lax.broadcasted_iota(jnp.int32, (owners, tiles), 0) == jnp.broadcast_to(key, (owners, tiles)), 1.0, 0.0
    )
    same_b = same.astype(jnp.bfloat16)
    until = jnp.where(
        lax.broadcasted_iota(jnp.int32, (tiles, tiles), 0) <= lax.broadcasted_iota(jnp.int32, (tiles, tiles), 1),
        1.0,
        0.0,
    ).astype(jnp.bfloat16)
    nt = (((1,), (1,)), ((), ()))
    count = jnp.dot(same_b, until, preferred_element_type=jnp.float32)

    def pieces(value):
        return jnp.floor((value + float(GROUP - 1)) * (1.0 / GROUP))

    wide = (owners, LANES)
    used = pieces(jnp.broadcast_to(count[:, tiles - 1 : tiles], wide))
    square = (owners, owners)
    row, column = lax.broadcasted_iota(jnp.int32, square, 0), lax.broadcasted_iota(jnp.int32, square, 1)
    before = jnp.where(column < row, 1.0, 0.0).astype(jnp.bfloat16)
    start = jnp.dot(before, used.astype(jnp.bfloat16), preferred_element_type=jnp.float32)
    position = jnp.sum(same * (start[:, :1] * float(GROUP) + count), axis=0, keepdims=True) - 1.0
    left = tiles - lax.broadcasted_iota(jnp.int32, (1, tiles), 1)
    features = jnp.concatenate(
        [left & 255, lax.shift_right_logical(left, 8), entry, key, jnp.zeros((4, tiles), jnp.int32)], axis=0
    )
    chosen = jnp.where(
        lax.broadcasted_iota(jnp.int32, (slots, tiles), 0)
        == jnp.broadcast_to(position.astype(jnp.int32), (slots, tiles)),
        1.0,
        0.0,
    ).astype(jnp.bfloat16)
    sorted_features = lax.dot_general(
        features.astype(jnp.float32).astype(jnp.bfloat16), chosen, nt, preferred_element_type=jnp.float32
    )
    tile = float(tiles) - (sorted_features[0:1] + 256.0 * sorted_features[1:2])
    codes[0:1, :slots] = jnp.clip(tile.astype(jnp.int32), 0, tiles)
    codes[1:2, :slots] = jnp.clip(sorted_features[2:3].astype(jnp.int32), 0, entries - 1)
    codes[2:3, :slots] = jnp.clip(sorted_features[3:4].astype(jnp.int32), 0, owners - 1)
    spread = -(-groups // LANES) * LANES
    number = lax.broadcasted_iota(jnp.int32, (owners, spread), 1).astype(jnp.float32)
    first = (jnp.broadcast_to(start[:, :1], number.shape) == number) & (
        jnp.broadcast_to(used[:, :1], number.shape) > 0.5
    )
    carried = 1.0 - jnp.max(jnp.where(first, 1.0, 0.0), axis=0, keepdims=True)
    codes[3:4, :spread] = carried.astype(jnp.int32)
    used_row = pieces(lax.dot_general(jnp.ones((8, tiles), jnp.bfloat16), same_b, nt, preferred_element_type=jnp.float32))
    upto = jnp.where(row <= column, 1.0, 0.0).astype(jnp.bfloat16)
    end = jnp.dot(used_row.astype(jnp.bfloat16), upto, preferred_element_type=jnp.float32)
    last = jnp.where(used_row > 0.5, end, 0.0).astype(jnp.int32)
    codes[4:5, :owners] = jnp.clip(last[0:1], 0, groups)


def whole_kernel(
    chan_count,
    sub_count,
    half,
    groups,
    rho_hbm,
    owner_hbm,
    channel_hbm,
    base_hbm,
    coupling_hbm,
    observed_hbm,
    keep_hbm,
    pairs_hbm,
    gains_hbm,
    duals_hbm,
    consensus_hbm,
    out_ref,
    rho_ref,
    owner_ref,
    channel_ref,
    base_ref,
    coupling_ref,
    observed_ref,
    keep_ref,
    pairs_ref,
    gains_ref,
    duals_ref,
    consensus_ref,
    gain_table,
    gain_codes,
    table,
    turned,
    stations_of,
    coupling_f,
    coupling_t,
    observed_f,
    lane_mask,
    codes_v,
    codes,
    sums_ref,
    pad,
    near_src,
    near_buf,
    send_buf,
    far_buf,
    weights,
    basis_buf,
    local_sem,
    gains_send,
    gains_recv,
    near_send,
    near_recv,
    far_send,
    far_recv,
    last_send,
    last_recv,
):
    chan, sub = lax.axis_index("chan"), lax.axis_index("sub")
    owners = chan_count * sub_count
    channels = owners * half
    width = LANES // half
    directions, stations = duals_ref.shape[2], duals_ref.shape[3]
    degree = consensus_ref.shape[0]
    tiles = keep_ref.shape[0]
    tile_rows = keep_ref.shape[1]
    bases = pairs_ref.shape[0]
    me = chan * sub_count + sub
    mesh_id = pl.DeviceIdType.MESH

    top = chan_count - 1

    def partner(rank):
        flips, result, bit = top - rank, chan, 1
        while bit < chan_count:
            if flips & bit:
                result = result + bit * (1 - 2 * lax.rem(lax.div(chan, bit), 2))
            bit *= 2
        return result

    partners = [partner(rank) for rank in range(chan_count)]

    barrier = pltpu.get_barrier_semaphore()
    for rank in range(chan_count):
        for shift in range(sub_count):
            if rank < top or shift:
                pl.semaphore_signal(
                    barrier,
                    inc=1,
                    device_id={"chan": partners[rank], "sub": lax.rem(sub + shift, sub_count)},
                    device_id_type=mesh_id,
                )

    loads = []
    for number, (source, target) in enumerate(
        [
            (gains_hbm, gains_ref),
            (owner_hbm, owner_ref),
            (channel_hbm, channel_ref),
            (base_hbm, base_ref),
            (pairs_hbm, pairs_ref),
            (coupling_hbm, coupling_ref),
            (observed_hbm, observed_ref),
            (keep_hbm, keep_ref),
            (duals_hbm, duals_ref),
            (consensus_hbm, consensus_ref),
            (rho_hbm, rho_ref),
        ]
    ):
        copy = pltpu.make_async_copy(source, target, local_sem.at[number])
        copy.start()
        loads.append(copy)

    pad[...] = jnp.zeros_like(pad)
    loads[0].wait()
    for owner in range(sub_count):
        for part in range(2):
            here = lay_pair(lambda number: gains_ref[owner * half + number, part], pad, half, width)
            gain_table[top * sub_count + owner, part] = here
            gain_codes[top * sub_count + owner, part] = (
                jnp.round(jnp.clip(here, -GAIN_MOST, GAIN_MOST) * (CODE_MOST / GAIN_MOST))
                .astype(jnp.int32)
                .astype(jnp.int16)
            )
    pl.semaphore_wait(barrier, owners - 1)
    gathers = []
    for rank in range(top):
        copy = pltpu.make_async_remote_copy(
            src_ref=gain_codes.at[pl.ds(top * sub_count, sub_count)],
            dst_ref=gain_codes.at[pl.ds(rank * sub_count, sub_count)],
            send_sem=gains_send.at[rank],
            recv_sem=gains_recv.at[rank],
            device_id={"chan": partners[rank]},
            device_id_type=mesh_id,
        )
        copy.start()
        gathers.append(copy)

    for copy in loads[1:4]:
        copy.wait()
    codes_v[...] = jnp.zeros_like(codes_v)
    named = owner_ref[...]
    rank_of = top - (named + chan - 2 * (named & chan))
    sort_tiles(rank_of, channel_ref[...], base_ref[...], codes_v, owners, sub_count, half, groups, bases * half)
    to_scalar = pltpu.make_async_copy(codes_v, codes, local_sem.at[len(loads)])
    to_scalar.start()

    loads[4].wait()
    turned[...] = jnp.zeros_like(turned)
    for base in range(bases):
        both = pairs_ref[base]
        turned[2 * base : 2 * base + 2, :] = both.astype(jnp.float32)
        for part in range(half):
            stations_of[base * half + part] = both + part * width
    columns = jnp.transpose(turned[...])
    lane = lax.broadcasted_iota(jnp.int32, (tile_rows, LANES), 1).astype(jnp.float32)
    for base in range(bases):
        for end in range(2):
            station = jnp.broadcast_to(columns[:, 2 * base + end : 2 * base + end + 1], lane.shape)
            for part in range(half):
                table[base * half + part, end * tile_rows : (end + 1) * tile_rows, :] = jnp.where(
                    station == lane - float(part * width), 1.0, 0.0
                ).astype(jnp.bfloat16)

    for copy in loads[5:]:
        copy.wait()
    step_rows = 2 * directions

    def widen(step, carry):
        span = pl.ds(pl.multiple_of(step * 8 * step_rows, 8 * step_rows), 8 * step_rows)
        coupling_t[...] = coupling_ref[span, :].astype(jnp.float32)
        for number in range(2):
            value = coupling_t[pl.ds(number, 8 * directions, stride=2), :]
            coupling_f[number, pl.ds(step * 8, 8)] = value.reshape(8, directions, tile_rows)
        return carry

    lax.fori_loop(0, tiles // 8, widen, 0)
    coupling_f[:, tiles:] = jnp.zeros((2, 1, directions, tile_rows), jnp.float32)
    observed_f[: 2 * tiles, :] = observed_ref[...].astype(jnp.float32)
    observed_f[2 * tiles :, :] = jnp.zeros((8, tile_rows), jnp.float32)
    lane_mask[:tiles, :] = jnp.where(keep_ref[...] > 0, 0, width - 1)
    lane_mask[tiles:, :] = jnp.zeros((8, tile_rows), jnp.int32)

    shape = (directions, LANES)
    row = lax.broadcasted_iota(jnp.int32, shape, 0)
    rho = jnp.zeros(shape, jnp.float32)
    for k in range(directions):
        rho = jnp.where(row == k, rho_ref[k], rho)
    place = lax.broadcasted_iota(jnp.int32, (owners, LANES), 1)
    of = lax.broadcasted_iota(jnp.int32, (owners, LANES), 0)
    everyone = basis_of((of * half + lax.div(place, width)).astype(jnp.float32), channels)
    for d in range(degree):
        basis_buf[d] = everyone[d]

    normal_rows = directions * directions
    out_rows = normal_rows + 2 * directions
    sums_ref[0] = jnp.zeros((out_rows, LANES), jnp.float32)
    upper = row < directions // 2
    tall = lax.broadcasted_iota(jnp.int32, (2 * directions, LANES), 0)
    turn = jnp.where((tall >= directions) & (tall < directions + directions // 2), 1.0, -1.0).astype(jnp.bfloat16)
    to_scalar.wait()
    for rank, copy in enumerate(gathers):
        copy.wait_recv()
        span = pl.ds(rank * sub_count, sub_count)
        gain_table[span] = gain_codes[span].astype(jnp.int32).astype(jnp.float32) * (GAIN_MOST / CODE_MOST)

    def spread(values):
        return jnp.broadcast_to(values, shape)

    def pick(values, index):
        return lax.gather(
            values,
            index[..., None],
            lax.GatherDimensionNumbers(
                offset_dims=(),
                collapsed_slice_dims=(1,),
                start_index_map=(1,),
                operand_batching_dims=(0,),
                start_indices_batching_dims=(0,),
            ),
            slice_sizes=(1, 1),
            mode=lax.GatherScatterMode.PROMISE_IN_BOUNDS,
        )

    def one_tile(slot):
        tile = jnp.clip(codes[0, slot], 0, tiles)
        entry = jnp.clip(codes[1, slot], 0, bases * half - 1)
        owner = jnp.clip(codes[2, slot], 0, owners - 1)
        real, imag = coupling_f[0, tile], coupling_f[1, tile]
        seen_real = spread(observed_f[pl.ds(2 * tile, 1), :])
        seen_imag = spread(observed_f[pl.ds(2 * tile + 1, 1), :])
        masked = spread(lane_mask[pl.ds(tile, 1), :])
        near = spread(stations_of[entry, pl.ds(0, 1), :]) | masked
        far = spread(stations_of[entry, pl.ds(1, 1), :]) | masked
        gain_real, gain_imag = gain_table[owner, 0], gain_table[owner, 1]
        near_real, near_imag = pick(gain_real, near), pick(gain_imag, near)
        far_real, far_imag = pick(gain_real, far), pick(gain_imag, far)
        slope_real = real * far_real + imag * far_imag
        slope_imag = imag * far_real - real * far_imag
        other_real = real * near_real - imag * near_imag
        other_imag = real * near_imag + imag * near_real
        return [
            end_rows(slope_real, slope_imag, seen_real, seen_imag, upper, turn, 1),
            end_rows(other_real, other_imag, seen_real, seen_imag, upper, turn, -1),
        ], table[entry]

    def sums_of(rank, which):
        return sums_ref[jnp.clip(codes[4, rank * sub_count + which], 0, groups)]

    def near_copy(rank, shift):
        return pltpu.make_async_remote_copy(
            src_ref=near_src.at[shift - 1, rank],
            dst_ref=near_buf.at[shift - 1, rank],
            send_sem=near_send.at[shift - 1, rank],
            recv_sem=near_recv.at[shift - 1, rank],
            device_id={"sub": lax.rem(sub + shift, sub_count)},
            device_id_type=mesh_id,
        )

    def far_copy(rank):
        return pltpu.make_async_remote_copy(
            src_ref=send_buf.at[rank],
            dst_ref=far_buf.at[rank],
            send_sem=far_send.at[rank],
            recv_sem=far_recv.at[rank],
            device_id={"chan": partners[rank]},
            device_id_type=mesh_id,
        )

    def start_near(rank):
        for shift in range(1, sub_count):
            near_src[shift - 1, rank] = encode(sums_of(rank, lax.rem(sub + shift, sub_count)), directions)
            near_copy(rank, shift).start()

    def add_near(rank):
        total = sums_of(rank, sub)
        for shift in range(1, sub_count):
            near_copy(rank, shift).wait_recv()
            total = total + decode(near_buf[shift - 1, rank], directions)
        return total

    def start_far(rank):
        send_buf[rank] = encode(add_near(rank), directions)
        far_copy(rank).start()

    def some_groups(step, carry):
        for rank, ready in enumerate(early):

            @pl.when(step == ready)
            def _():
                start_near(rank)

            if ready + 1 < steps:

                @pl.when(step == ready + 1)
                def _():
                    start_far(rank)

        base_group = step * UNROLL
        running = sums_ref[base_group]
        for number in range(UNROLL):
            group = base_group + number
            rows, entries = [], []
            for inner in range(GROUP):
                ends, entry = one_tile(group * GROUP + inner)
                rows.append(jnp.concatenate(ends, axis=1))
                entries.append(entry)
            total = None
            for inner in range(0, GROUP, 2):
                value = jnp.dot(
                    jnp.concatenate(rows[inner : inner + 2], axis=0),
                    jnp.concatenate(entries[inner : inner + 2], axis=1),
                    preferred_element_type=jnp.float32,
                )
                value = value[:out_rows, :LANES] + value[out_rows:, LANES:]
                total = value if total is None else total + value
            running = running * codes[3, group].astype(jnp.float32) + total
            sums_ref[group + 1] = running
        return carry

    steps = groups // UNROLL
    most = 3 * tiles // chan_count + sub_count * (GROUP - 1)
    early = []
    for rank in range(top):
        ready = -(-(rank + 1) * most // (GROUP * UNROLL))
        if ready < steps:
            early.append(ready)
    lax.fori_loop(0, steps, some_groups, 0)

    for rank in range(len(early), chan_count):
        start_near(rank)

    mine = [jnp.broadcast_to(basis_buf[d, pl.ds(me, 1), :], shape) for d in range(degree)]
    duals = [
        lay_pair(lambda number: duals_ref[number, part], pad, half, width) for part in range(2)
    ]
    anchors = []
    for part in range(2):
        anchor = jnp.zeros(shape, jnp.float32)
        for d in range(degree):
            anchor = anchor + mine[d] * lay_pair(
                lambda number: consensus_ref[d, part], pad, half, width
            )
        anchors.append(anchor)

    for rank in range(top):
        if rank >= len(early) or early[rank] + 1 >= steps:
            start_far(rank)
    total = add_near(top)
    for rank in range(top):
        far_copy(rank).wait_recv()
        total = total + decode(far_buf[rank], directions)

    group = [total[i * directions : (i + 1) * directions] for i in range(directions + 2)]
    solved = solve_hermitian(
        [group[7], group[0], group[1], group[6]],
        [group[2], group[3], group[4]],
        group[5],
        rho,
        group[directions] - duals[0] + rho * anchors[0],
        group[directions + 1] - duals[1] + rho * anchors[1],
    )
    weights[me] = jnp.concatenate(
        [solved[part] + duals[part] / rho for part in range(2)], axis=0
    ).astype(jnp.bfloat16)

    last = []
    for rank in range(chan_count):
        for shift in range(sub_count):
            if rank == top and shift == 0:
                continue
            number = rank * sub_count + shift
            copy = pltpu.make_async_remote_copy(
                src_ref=weights.at[me],
                dst_ref=weights.at[me],
                send_sem=last_send.at[number],
                recv_sem=last_recv.at[number],
                device_id={"chan": partners[rank], "sub": lax.rem(sub + shift, sub_count)},
                device_id_type=mesh_id,
            )
            copy.start()
            last.append(copy)

    def store(first, part, value):
        for number in range(half):
            out_ref[first + number, part] = (
                pltpu.roll(value, LANES - number * width, axis=1) if number else value
            )

    for part in range(2):
        store(0, part, solved[part])
    for copy in last:
        copy.wait_recv()
    inverse = inverse_gram(channels)
    totals = []
    for d in range(degree):
        value = jnp.zeros((2 * directions, LANES), jnp.float32)
        for number in range(owners):
            value = value + basis_buf[d, number : number + 1, :] * weights[number].astype(jnp.float32)
        folded = value
        for number in range(1, half):
            folded = folded + pltpu.roll(value, number * width, axis=1)
        totals.append(folded)
    fitted = jnp.zeros((2 * directions, LANES), jnp.float32)
    for d in range(degree):
        value = sum(float(inverse[d, e]) * totals[e] for e in range(degree))
        for part in range(2):
            out_ref[half + d, part] = value[part * directions : (part + 1) * directions]
        fitted = fitted + jnp.concatenate([mine[d], mine[d]], axis=0) * value
    for part in range(2):
        fit = fitted[part * directions : (part + 1) * directions]
        store(half + degree, part, duals[part] + rho * (solved[part] - fit))
    for copy in gathers:
        copy.wait_send()
    for rank in range(chan_count):
        for shift in range(1, sub_count):
            near_copy(rank, shift).wait_send()
        if rank < top:
            far_copy(rank).wait_send()
    for copy in last:
        copy.wait_send()


def deliver_kernel(result_ref, gains_out, consensus_out, duals_out):
    first = 0
    for ref in (gains_out, consensus_out, duals_out):
        count, _, _, stations = ref.shape
        for number in range(count):
            ref[number] = result_ref[first + number][:, :, :stations]
        first += count


def body(
    predicted_sky_response,
    measured_correlation,
    keep_indicator,
    tile_owner,
    tile_channel,
    tile_base,
    pairs,
    gains,
    duals,
    consensus,
    rho,
):
    channels_here, _, stations, directions = gains.shape
    chan_count = lax.axis_size("chan")
    sub_count = lax.axis_size("sub")
    half = channels_here // sub_count
    owners = chan_count * sub_count
    tiles, _, _, tile_rows = predicted_sky_response.shape
    bases = pairs.shape[0]
    degree = consensus.shape[0]
    width = LANES // half
    if chan_count & (chan_count - 1) or width & (width - 1) or stations >= width or tile_rows != LANES or directions != 8:
        raise ValueError("unsupported sizes")
    groups = -(-(tiles + owners * (GROUP - 1)) // GROUP)
    groups = -(-groups // UNROLL) * UNROLL
    code_width = -(-max(groups * GROUP, owners) // LANES) * LANES
    out_rows = directions * directions + 2 * directions
    coded = out_rows + 2 * directions
    gains_t = jnp.swapaxes(gains, 2, 3)
    duals_t = jnp.swapaxes(duals, 2, 3)
    consensus_t = jnp.swapaxes(consensus, 2, 3)
    operands = [
        tile_owner.reshape(1, tiles),
        tile_channel.reshape(1, tiles),
        tile_base.reshape(1, tiles),
        predicted_sky_response.reshape(tiles * 2 * directions, tile_rows),
        measured_correlation.reshape(tiles * 2, tile_rows),
        keep_indicator,
        pairs,
        gains_t,
        duals_t,
        consensus_t,
    ]
    vmem, dma = pltpu.VMEM, pltpu.SemaphoreType.DMA
    f32, bf16, i32 = jnp.float32, jnp.bfloat16, jnp.int32
    result = pl.pallas_call(
        functools.partial(whole_kernel, chan_count, sub_count, half, groups),
        out_shape=pltpu.VMEM((2 * half + degree, 2, directions, LANES), f32),
        in_specs=[pl.BlockSpec(memory_space=pl.ANY)] * (len(operands) + 1),
        out_specs=pl.BlockSpec(memory_space=pltpu.VMEM),
        scratch_shapes=[pltpu.SMEM(rho.shape, f32)]
        + [vmem(x.shape, x.dtype) for x in operands]
        + [
            vmem((owners, 2, directions, LANES), f32),
            vmem((owners, 2, directions, LANES), jnp.int16),
            vmem((bases * half, 2 * tile_rows, LANES), bf16),
            vmem((LANES, tile_rows), f32),
            vmem((bases * half, 2, tile_rows), i32),
            vmem((2, tiles + 1, directions, tile_rows), f32),
            vmem((8 * 2 * directions, tile_rows), f32),
            vmem((2 * tiles + 8, tile_rows), f32),
            vmem((tiles + 8, tile_rows), i32),
            vmem((8, code_width), i32),
            pltpu.SMEM((8, code_width), i32),
            vmem((groups + 1, out_rows, LANES), f32),
            vmem((2, directions, LANES), f32),
            vmem((sub_count - 1, chan_count, coded, LANES), bf16),
            vmem((sub_count - 1, chan_count, coded, LANES), bf16),
            vmem((chan_count, coded, LANES), bf16),
            vmem((chan_count, coded, LANES), bf16),
            vmem((owners, 2 * directions, LANES), bf16),
            vmem((degree, owners, LANES), f32),
            dma((len(operands) + 2,)),
            dma((chan_count,)),
            dma((chan_count,)),
            dma((sub_count - 1, chan_count)),
            dma((sub_count - 1, chan_count)),
            dma((chan_count,)),
            dma((chan_count,)),
            dma((owners,)),
            dma((owners,)),
        ],
        compiler_params=pltpu.CompilerParams(
            collective_id=1, has_side_effects=True, vmem_limit_bytes=60 << 20
        ),
    )(rho, *operands)
    outputs = pl.pallas_call(
        deliver_kernel,
        out_shape=tuple(
            jax.ShapeDtypeStruct(x.shape, f32) for x in (duals_t, consensus_t, duals_t)
        ),
        in_specs=[pl.BlockSpec(memory_space=pltpu.VMEM)],
        out_specs=tuple(pl.BlockSpec(memory_space=pltpu.VMEM) for _ in range(3)),
    )(pltpu.with_memory_space_constraint(result, pltpu.VMEM))
    return tuple(jnp.swapaxes(x, 2, 3) for x in outputs)


def solution(mesh):
    placed = (
        P(("groups", "chan", "sub"), None, None, None),
        P(("groups", "chan", "sub"), None, None),
        P(("groups", "chan", "sub"), None),
        P(("groups", "chan", "sub"), None),
        P(("groups", "chan", "sub")),
        P(("groups", "chan", "sub")),
        P(),
        P(("groups", "chan"), None, None, None),
        P(("groups", "chan", "sub"), None, None, None),
        P("groups", None, None, None),
        P(),
    )
    return jax.shard_map(
        body,
        mesh=mesh,
        in_specs=placed,
        out_specs=(
            P(("groups", "chan", "sub"), None, None, None),
            P("groups", None, None, None),
            P(("groups", "chan", "sub"), None, None, None),
        ),
        check_vma=False,
    )
```

```python
import functools

import jax
import jax.numpy as jnp
import numpy as np
from jax import lax
from jax.experimental import pallas as pl
from jax.experimental.pallas import tpu as pltpu
from jax.sharding import PartitionSpec as P

LANES = 128
GROUP = 2
UNROLL = 66
GAIN_MOST = 5.0
CODE_MOST = 32767.0


def lay_pair(load, pad, half, width):
    total = None
    for part in range(half):
        block = load(part)
        pad[part % 2, :, : block.shape[1]] = block
        value = pad[part % 2]
        if part:
            value = pltpu.roll(value, part * width, axis=1)
        total = value if total is None else total + value
    return total


def basis_of(channel, channels):
    x = (2.0 * channel - (channels - 1)) / max(channels - 1, 1)
    return [
        jnp.ones_like(x),
        x,
        0.5 * (3.0 * x * x - 1.0),
        0.5 * (5.0 * x * x * x - 3.0 * x),
    ]


def inverse_gram(channels):
    f = np.arange(channels, dtype=np.float64)
    x = (2.0 * f - (channels - 1)) / max(channels - 1, 1)
    basis = np.stack([np.ones_like(x), x, 0.5 * (3 * x * x - 1), 0.5 * (5 * x * x * x - 3 * x)])
    return np.linalg.inv(basis @ basis.T)


def end_rows(real, imag, seen_real, seen_imag, upper, turn, sign):
    directions = real.shape[0]

    def pair(first, second):
        return jnp.concatenate([first, second], axis=0).astype(jnp.bfloat16)

    def turned(value, shift):
        return pltpu.roll(value, directions - shift, axis=0)

    left, right = pair(real, real), pair(imag, imag)
    ahead_real = pair(turned(real, 1), turned(real, 2))
    ahead_imag = pair(turned(imag, 1), turned(imag, 2))
    both = left * ahead_real + right * ahead_imag
    third_real, third_imag = turned(real, 3), turned(imag, 3)
    fourth_real, fourth_imag = turned(real, 4), turned(imag, 4)
    ahead_one = pair(third_imag, jnp.where(upper, fourth_real, fourth_imag))
    ahead_two = pair(third_real, jnp.where(upper, fourth_imag, fourth_real))
    if sign > 0:
        cross = left * ahead_imag - right * ahead_real
        mixed = left * ahead_one + right * turn * ahead_two
        side_imag = real * seen_imag - imag * seen_real
    else:
        cross = right * ahead_real - left * ahead_imag
        mixed = left * turn * ahead_one + right * ahead_two
        side_imag = imag * seen_real - real * seen_imag
    plain = left * pair(third_real, real) + right * pair(third_imag, imag)
    side_real = real * seen_real + imag * seen_imag
    return jnp.concatenate([both, cross, mixed, plain, pair(side_real, side_imag)], axis=0)


def solve_hermitian(groups_real, groups_imag, mixed, ridge, side_real, side_imag):
    directions = side_real.shape[0]
    middle = directions // 2
    row = lax.broadcasted_iota(jnp.int32, side_real.shape, 0)
    upper = row < middle
    swapped = pltpu.roll(mixed, middle, axis=0)
    real = {0: groups_real[0] + ridge, middle: jnp.where(upper, mixed, swapped)}
    imag = {0: jnp.zeros_like(ridge), middle: jnp.where(upper, -swapped, mixed)}
    for d in range(1, middle):
        real[d], imag[d] = groups_real[d], groups_imag[d - 1]
        real[directions - d] = pltpu.roll(groups_real[d], d, axis=0)
        imag[directions - d] = -pltpu.roll(groups_imag[d - 1], d, axis=0)
    columns = []
    for l in range(directions):
        column_real, column_imag = real[l], imag[l]
        for k in range(1, directions):
            here = row == k
            d = (l - k) % directions
            column_real = jnp.where(here, real[d], column_real)
            column_imag = jnp.where(here, imag[d], column_imag)
        columns.append((column_real, column_imag))
    columns.append((side_real, side_imag))
    scale = jnp.zeros_like(ridge)
    for j in range(directions):
        pivot_real, pivot_imag = columns[j]
        inverse = 1.0 / pivot_real[j : j + 1]
        here = row == j
        scale = jnp.where(here, jnp.broadcast_to(inverse, scale.shape), scale)
        factor_real = jnp.where(here, 0.0, pivot_real * inverse)
        factor_imag = jnp.where(here, 0.0, pivot_imag * inverse)
        for l in range(j + 1, directions + 1):
            value_real, value_imag = columns[l]
            head_real, head_imag = value_real[j : j + 1], value_imag[j : j + 1]
            columns[l] = (
                value_real - (factor_real * head_real - factor_imag * head_imag),
                value_imag - (factor_real * head_imag + factor_imag * head_real),
            )
    return columns[-1][0] * scale, columns[-1][1] * scale


def encode(sums, directions):
    normal_rows = directions * directions
    side = sums[normal_rows:]
    high = side.astype(jnp.bfloat16)
    low = (side - high.astype(jnp.float32)).astype(jnp.bfloat16)
    return jnp.concatenate([sums[:normal_rows].astype(jnp.bfloat16), high, low], axis=0)


def decode(coded, directions):
    wide = coded.astype(jnp.float32)
    normal_rows = directions * directions
    side_rows = 2 * directions
    high, low = wide[normal_rows : normal_rows + side_rows], wide[normal_rows + side_rows :]
    return jnp.concatenate([wide[:normal_rows], high + low], axis=0)


def sort_tiles(rank, channel, base, codes, owners, sub_count, half, groups, entries):
    tiles = rank.shape[1]
    slots = groups * GROUP
    sub = jnp.zeros_like(channel)
    for number in range(1, sub_count):
        sub = sub + jnp.where(channel >= number * half, 1, 0)
    place = channel - sub * half
    key = rank * sub_count + sub
    entry = base * half + place
    same = jnp.where(
        lax.broadcasted_iota(jnp.int32, (owners, tiles), 0) == jnp.broadcast_to(key, (owners, tiles)), 1.0, 0.0
    )
    same_b = same.astype(jnp.bfloat16)
    until = jnp.where(
        lax.broadcasted_iota(jnp.int32, (tiles, tiles), 0) <= lax.broadcasted_iota(jnp.int32, (tiles, tiles), 1),
        1.0,
        0.0,
    ).astype(jnp.bfloat16)
    nt = (((1,), (1,)), ((), ()))
    count = jnp.dot(same_b, until, preferred_element_type=jnp.float32)

    def pieces(value):
        return jnp.floor((value + float(GROUP - 1)) * (1.0 / GROUP))

    wide = (owners, LANES)
    used = pieces(jnp.broadcast_to(count[:, tiles - 1 : tiles], wide))
    square = (owners, owners)
    row, column = lax.broadcasted_iota(jnp.int32, square, 0), lax.broadcasted_iota(jnp.int32, square, 1)
    before = jnp.where(column < row, 1.0, 0.0).astype(jnp.bfloat16)
    start = jnp.dot(before, used.astype(jnp.bfloat16), preferred_element_type=jnp.float32)
    position = jnp.sum(same * (start[:, :1] * float(GROUP) + count), axis=0, keepdims=True) - 1.0
    left = tiles - lax.broadcasted_iota(jnp.int32, (1, tiles), 1)
    features = jnp.concatenate(
        [left & 255, lax.shift_right_logical(left, 8), entry, key, jnp.zeros((4, tiles), jnp.int32)], axis=0
    )
    chosen = jnp.where(
        lax.broadcasted_iota(jnp.int32, (slots, tiles), 0)
        == jnp.broadcast_to(position.astype(jnp.int32), (slots, tiles)),
        1.0,
        0.0,
    ).astype(jnp.bfloat16)
    sorted_features = lax.dot_general(
        features.astype(jnp.float32).astype(jnp.bfloat16), chosen, nt, preferred_element_type=jnp.float32
    )
    tile = float(tiles) - (sorted_features[0:1] + 256.0 * sorted_features[1:2])
    codes[0:1, :slots] = jnp.clip(tile.astype(jnp.int32), 0, tiles)
    codes[1:2, :slots] = jnp.clip(sorted_features[2:3].astype(jnp.int32), 0, entries - 1)
    codes[2:3, :slots] = jnp.clip(sorted_features[3:4].astype(jnp.int32), 0, owners - 1)
    spread = -(-groups // LANES) * LANES
    number = lax.broadcasted_iota(jnp.int32, (owners, spread), 1).astype(jnp.float32)
    first = (jnp.broadcast_to(start[:, :1], number.shape) == number) & (
        jnp.broadcast_to(used[:, :1], number.shape) > 0.5
    )
    carried = 1.0 - jnp.max(jnp.where(first, 1.0, 0.0), axis=0, keepdims=True)
    codes[3:4, :spread] = carried.astype(jnp.int32)
    used_row = pieces(lax.dot_general(jnp.ones((8, tiles), jnp.bfloat16), same_b, nt, preferred_element_type=jnp.float32))
    upto = jnp.where(row <= column, 1.0, 0.0).astype(jnp.bfloat16)
    end = jnp.dot(used_row.astype(jnp.bfloat16), upto, preferred_element_type=jnp.float32)
    last = jnp.where(used_row > 0.5, end, 0.0).astype(jnp.int32)
    codes[4:5, :owners] = jnp.clip(last[0:1], 0, groups)


def whole_kernel(
    chan_count,
    sub_count,
    half,
    groups,
    rho_hbm,
    owner_hbm,
    channel_hbm,
    base_hbm,
    coupling_hbm,
    observed_hbm,
    keep_hbm,
    pairs_hbm,
    gains_hbm,
    duals_hbm,
    consensus_hbm,
    out_ref,
    rho_ref,
    owner_ref,
    channel_ref,
    base_ref,
    coupling_ref,
    observed_ref,
    keep_ref,
    pairs_ref,
    gains_ref,
    duals_ref,
    consensus_ref,
    gain_table,
    gain_codes,
    table,
    turned,
    stations_of,
    coupling_f,
    coupling_t,
    observed_f,
    lane_mask,
    codes_v,
    codes,
    sums_ref,
    pad,
    near_src,
    near_buf,
    send_buf,
    far_buf,
    weights,
    basis_buf,
    local_sem,
    gains_send,
    gains_recv,
    near_send,
    near_recv,
    far_send,
    far_recv,
    last_send,
    last_recv,
):
    chan, sub = lax.axis_index("chan"), lax.axis_index("sub")
    owners = chan_count * sub_count
    channels = owners * half
    width = LANES // half
    directions, stations = duals_ref.shape[2], duals_ref.shape[3]
    degree = consensus_ref.shape[0]
    tiles = keep_ref.shape[0]
    tile_rows = keep_ref.shape[1]
    bases = pairs_ref.shape[0]
    me = chan * sub_count + sub
    mesh_id = pl.DeviceIdType.MESH

    top = chan_count - 1

    def partner(rank):
        flips, result, bit = top - rank, chan, 1
        while bit < chan_count:
            if flips & bit:
                result = result + bit * (1 - 2 * lax.rem(lax.div(chan, bit), 2))
            bit *= 2
        return result

    partners = [partner(rank) for rank in range(chan_count)]

    barrier = pltpu.get_barrier_semaphore()
    for rank in range(chan_count):
        for shift in range(sub_count):
            if rank < top or shift:
                pl.semaphore_signal(
                    barrier,
                    inc=1,
                    device_id={"chan": partners[rank], "sub": lax.rem(sub + shift, sub_count)},
                    device_id_type=mesh_id,
                )

    loads = []
    for number, (source, target) in enumerate(
        [
            (gains_hbm, gains_ref),
            (owner_hbm, owner_ref),
            (channel_hbm, channel_ref),
            (base_hbm, base_ref),
            (pairs_hbm, pairs_ref),
            (coupling_hbm, coupling_ref),
            (observed_hbm, observed_ref),
            (keep_hbm, keep_ref),
            (duals_hbm, duals_ref),
            (consensus_hbm, consensus_ref),
            (rho_hbm, rho_ref),
        ]
    ):
        copy = pltpu.make_async_copy(source, target, local_sem.at[number])
        copy.start()
        loads.append(copy)

    pad[...] = jnp.zeros_like(pad)
    loads[0].wait()
    for owner in range(sub_count):
        for part in range(2):
            here = lay_pair(lambda number: gains_ref[owner * half + number, part], pad, half, width)
            gain_table[top * sub_count + owner, part] = here
            gain_codes[top * sub_count + owner, part] = (
                jnp.round(jnp.clip(here, -GAIN_MOST, GAIN_MOST) * (CODE_MOST / GAIN_MOST))
                .astype(jnp.int32)
                .astype(jnp.int16)
            )
    pl.semaphore_wait(barrier, owners - 1)
    gathers = []
    for rank in range(top):
        copy = pltpu.make_async_remote_copy(
            src_ref=gain_codes.at[pl.ds(top * sub_count, sub_count)],
            dst_ref=gain_codes.at[pl.ds(rank * sub_count, sub_count)],
            send_sem=gains_send.at[rank],
            recv_sem=gains_recv.at[rank],
            device_id={"chan": partners[rank]},
            device_id_type=mesh_id,
        )
        copy.start()
        gathers.append(copy)

    for copy in loads[1:4]:
        copy.wait()
    codes_v[...] = jnp.zeros_like(codes_v)
    named = owner_ref[...]
    rank_of = top - (named + chan - 2 * (named & chan))
    sort_tiles(rank_of, channel_ref[...], base_ref[...], codes_v, owners, sub_count, half, groups, bases * half)
    to_scalar = pltpu.make_async_copy(codes_v, codes, local_sem.at[len(loads)])
    to_scalar.start()

    loads[4].wait()
    turned[...] = jnp.zeros_like(turned)
    for base in range(bases):
        both = pairs_ref[base]
        turned[2 * base : 2 * base + 2, :] = both.astype(jnp.float32)
        for part in range(half):
            stations_of[base * half + part] = both + part * width
    columns = jnp.transpose(turned[...])
    lane = lax.broadcasted_iota(jnp.int32, (tile_rows, LANES), 1).astype(jnp.float32)
    for base in range(bases):
        for end in range(2):
            station = jnp.broadcast_to(columns[:, 2 * base + end : 2 * base + end + 1], lane.shape)
            for part in range(half):
                table[base * half + part, end * tile_rows : (end + 1) * tile_rows, :] = jnp.where(
                    station == lane - float(part * width), 1.0, 0.0
                ).astype(jnp.bfloat16)

    for copy in loads[5:]:
        copy.wait()
    step_rows = 2 * directions

    def widen(step, carry):
        span = pl.ds(pl.multiple_of(step * 8 * step_rows, 8 * step_rows), 8 * step_rows)
        coupling_t[...] = coupling_ref[span, :].astype(jnp.float32)
        for number in range(2):
            value = coupling_t[pl.ds(number, 8 * directions, stride=2), :]
            coupling_f[number, pl.ds(step * 8, 8)] = value.reshape(8, directions, tile_rows)
        return carry

    lax.fori_loop(0, tiles // 8, widen, 0)
    coupling_f[:, tiles:] = jnp.zeros((2, 1, directions, tile_rows), jnp.float32)
    observed_f[: 2 * tiles, :] = observed_ref[...].astype(jnp.float32)
    observed_f[2 * tiles :, :] = jnp.zeros((8, tile_rows), jnp.float32)
    lane_mask[:tiles, :] = jnp.where(keep_ref[...] > 0, 0, width - 1)
    lane_mask[tiles:, :] = jnp.zeros((8, tile_rows), jnp.int32)

    shape = (directions, LANES)
    row = lax.broadcasted_iota(jnp.int32, shape, 0)
    rho = jnp.zeros(shape, jnp.float32)
    for k in range(directions):
        rho = jnp.where(row == k, rho_ref[k], rho)
    place = lax.broadcasted_iota(jnp.int32, (owners, LANES), 1)
    of = lax.broadcasted_iota(jnp.int32, (owners, LANES), 0)
    everyone = basis_of((of * half + lax.div(place, width)).astype(jnp.float32), channels)
    for d in range(degree):
        basis_buf[d] = everyone[d]

    normal_rows = directions * directions
    out_rows = normal_rows + 2 * directions
    sums_ref[0] = jnp.zeros((out_rows, LANES), jnp.float32)
    upper = row < directions // 2
    tall = lax.broadcasted_iota(jnp.int32, (2 * directions, LANES), 0)
    turn = jnp.where((tall >= directions) & (tall < directions + directions // 2), 1.0, -1.0).astype(jnp.bfloat16)
    mine = [jnp.broadcast_to(basis_buf[d, pl.ds(me, 1), :], shape) for d in range(degree)]
    duals = [
        lay_pair(lambda number: duals_ref[number, part], pad, half, width) for part in range(2)
    ]
    anchors = []
    for part in range(2):
        anchor = jnp.zeros(shape, jnp.float32)
        for d in range(degree):
            anchor = anchor + mine[d] * lay_pair(
                lambda number: consensus_ref[d, part], pad, half, width
            )
        anchors.append(anchor)

    to_scalar.wait()
    for rank, copy in enumerate(gathers):
        copy.wait_recv()
        span = pl.ds(rank * sub_count, sub_count)
        gain_table[span] = gain_codes[span].astype(jnp.int32).astype(jnp.float32) * (GAIN_MOST / CODE_MOST)

    def spread(values):
        return jnp.broadcast_to(values, shape)

    def pick(values, index):
        return lax.gather(
            values,
            index[..., None],
            lax.GatherDimensionNumbers(
                offset_dims=(),
                collapsed_slice_dims=(1,),
                start_index_map=(1,),
                operand_batching_dims=(0,),
                start_indices_batching_dims=(0,),
            ),
            slice_sizes=(1, 1),
            mode=lax.GatherScatterMode.PROMISE_IN_BOUNDS,
        )

    def one_tile(slot):
        tile = jnp.clip(codes[0, slot], 0, tiles)
        entry = jnp.clip(codes[1, slot], 0, bases * half - 1)
        owner = jnp.clip(codes[2, slot], 0, owners - 1)
        real, imag = coupling_f[0, tile], coupling_f[1, tile]
        seen_real = spread(observed_f[pl.ds(2 * tile, 1), :])
        seen_imag = spread(observed_f[pl.ds(2 * tile + 1, 1), :])
        masked = spread(lane_mask[pl.ds(tile, 1), :])
        near = spread(stations_of[entry, pl.ds(0, 1), :]) | masked
        far = spread(stations_of[entry, pl.ds(1, 1), :]) | masked
        gain_real, gain_imag = gain_table[owner, 0], gain_table[owner, 1]
        near_real, near_imag = pick(gain_real, near), pick(gain_imag, near)
        far_real, far_imag = pick(gain_real, far), pick(gain_imag, far)
        slope_real = real * far_real + imag * far_imag
        slope_imag = imag * far_real - real * far_imag
        other_real = real * near_real - imag * near_imag
        other_imag = real * near_imag + imag * near_real
        return [
            end_rows(slope_real, slope_imag, seen_real, seen_imag, upper, turn, 1),
            end_rows(other_real, other_imag, seen_real, seen_imag, upper, turn, -1),
        ], table[entry]

    def sums_of(rank, which):
        return sums_ref[jnp.clip(codes[4, rank * sub_count + which], 0, groups)]

    def near_copy(rank, shift):
        return pltpu.make_async_remote_copy(
            src_ref=near_src.at[shift - 1, rank],
            dst_ref=near_buf.at[shift - 1, rank],
            send_sem=near_send.at[shift - 1, rank],
            recv_sem=near_recv.at[shift - 1, rank],
            device_id={"sub": lax.rem(sub + shift, sub_count)},
            device_id_type=mesh_id,
        )

    def far_copy(rank):
        return pltpu.make_async_remote_copy(
            src_ref=send_buf.at[rank],
            dst_ref=far_buf.at[rank],
            send_sem=far_send.at[rank],
            recv_sem=far_recv.at[rank],
            device_id={"chan": partners[rank]},
            device_id_type=mesh_id,
        )

    def start_near(rank):
        for shift in range(1, sub_count):
            near_src[shift - 1, rank] = encode(sums_of(rank, lax.rem(sub + shift, sub_count)), directions)
            near_copy(rank, shift).start()

    def add_near(rank):
        total = sums_of(rank, sub)
        for shift in range(1, sub_count):
            near_copy(rank, shift).wait_recv()
            total = total + decode(near_buf[shift - 1, rank], directions)
        return total

    def start_far(rank):
        send_buf[rank] = encode(add_near(rank), directions)
        far_copy(rank).start()

    def some_groups(step, carry):
        for rank, ready in enumerate(early):

            @pl.when(step == ready)
            def _():
                start_near(rank)

            if ready + 1 < steps:

                @pl.when(step == ready + 1)
                def _():
                    start_far(rank)

        base_group = step * UNROLL
        running = sums_ref[base_group]
        for number in range(UNROLL):
            group = base_group + number
            rows, entries = [], []
            for inner in range(GROUP):
                ends, entry = one_tile(group * GROUP + inner)
                rows.append(jnp.concatenate(ends, axis=1))
                entries.append(entry)
            total = None
            for inner in range(0, GROUP, 2):
                value = jnp.dot(
                    jnp.concatenate(rows[inner : inner + 2], axis=0),
                    jnp.concatenate(entries[inner : inner + 2], axis=1),
                    preferred_element_type=jnp.float32,
                )
                value = value[:out_rows, :LANES] + value[out_rows:, LANES:]
                total = value if total is None else total + value
            running = running * codes[3, group].astype(jnp.float32) + total
            sums_ref[group + 1] = running
        return carry

    steps = groups // UNROLL
    most = 3 * tiles // chan_count + sub_count * (GROUP - 1)
    early = []
    for rank in range(top):
        ready = -(-(rank + 1) * most // (GROUP * UNROLL))
        if ready < steps:
            early.append(ready)
    lax.fori_loop(0, steps, some_groups, 0)

    for rank in range(len(early), chan_count):
        start_near(rank)

    for rank in range(top):
        if rank >= len(early) or early[rank] + 1 >= steps:
            start_far(rank)
    total = add_near(top)
    for rank in range(top):
        far_copy(rank).wait_recv()
        total = total + decode(far_buf[rank], directions)

    group = [total[i * directions : (i + 1) * directions] for i in range(directions + 2)]
    solved = solve_hermitian(
        [group[7], group[0], group[1], group[6]],
        [group[2], group[3], group[4]],
        group[5],
        rho,
        group[directions] - duals[0] + rho * anchors[0],
        group[directions + 1] - duals[1] + rho * anchors[1],
    )
    weights[me] = jnp.concatenate(
        [solved[part] + duals[part] / rho for part in range(2)], axis=0
    ).astype(jnp.bfloat16)

    last = []
    for rank in range(chan_count):
        for shift in range(sub_count):
            if rank == top and shift == 0:
                continue
            number = rank * sub_count + shift
            copy = pltpu.make_async_remote_copy(
                src_ref=weights.at[me],
                dst_ref=weights.at[me],
                send_sem=last_send.at[number],
                recv_sem=last_recv.at[number],
                device_id={"chan": partners[rank], "sub": lax.rem(sub + shift, sub_count)},
                device_id_type=mesh_id,
            )
            copy.start()
            last.append(copy)

    def store(first, part, value):
        for number in range(half):
            out_ref[first + number, part] = (
                pltpu.roll(value, LANES - number * width, axis=1) if number else value
            )

    for part in range(2):
        store(0, part, solved[part])
    for copy in last:
        copy.wait_recv()
    inverse = inverse_gram(channels)
    totals = []
    for d in range(degree):
        value = jnp.zeros((2 * directions, LANES), jnp.float32)
        for number in range(owners):
            value = value + basis_buf[d, number : number + 1, :] * weights[number].astype(jnp.float32)
        folded = value
        for number in range(1, half):
            folded = folded + pltpu.roll(value, number * width, axis=1)
        totals.append(folded)
    fitted = jnp.zeros((2 * directions, LANES), jnp.float32)
    for d in range(degree):
        value = sum(float(inverse[d, e]) * totals[e] for e in range(degree))
        for part in range(2):
            out_ref[half + d, part] = value[part * directions : (part + 1) * directions]
        fitted = fitted + jnp.concatenate([mine[d], mine[d]], axis=0) * value
    for part in range(2):
        fit = fitted[part * directions : (part + 1) * directions]
        store(half + degree, part, duals[part] + rho * (solved[part] - fit))
    for copy in gathers:
        copy.wait_send()
    for rank in range(chan_count):
        for shift in range(1, sub_count):
            near_copy(rank, shift).wait_send()
        if rank < top:
            far_copy(rank).wait_send()
    for copy in last:
        copy.wait_send()


def deliver_kernel(result_ref, gains_out, consensus_out, duals_out):
    first = 0
    for ref in (gains_out, consensus_out, duals_out):
        count, _, _, stations = ref.shape
        for number in range(count):
            ref[number] = result_ref[first + number][:, :, :stations]
        first += count


def body(
    predicted_sky_response,
    measured_correlation,
    keep_indicator,
    tile_owner,
    tile_channel,
    tile_base,
    pairs,
    gains,
    duals,
    consensus,
    rho,
):
    channels_here, _, stations, directions = gains.shape
    chan_count = lax.axis_size("chan")
    sub_count = lax.axis_size("sub")
    half = channels_here // sub_count
    owners = chan_count * sub_count
    tiles, _, _, tile_rows = predicted_sky_response.shape
    bases = pairs.shape[0]
    degree = consensus.shape[0]
    width = LANES // half
    if chan_count & (chan_count - 1) or width & (width - 1) or stations >= width or tile_rows != LANES or directions != 8:
        raise ValueError("unsupported sizes")
    groups = -(-(tiles + owners * (GROUP - 1)) // GROUP)
    groups = -(-groups // UNROLL) * UNROLL
    code_width = -(-max(groups * GROUP, owners) // LANES) * LANES
    out_rows = directions * directions + 2 * directions
    coded = out_rows + 2 * directions
    gains_t = jnp.swapaxes(gains, 2, 3)
    duals_t = jnp.swapaxes(duals, 2, 3)
    consensus_t = jnp.swapaxes(consensus, 2, 3)
    operands = [
        tile_owner.reshape(1, tiles),
        tile_channel.reshape(1, tiles),
        tile_base.reshape(1, tiles),
        predicted_sky_response.reshape(tiles * 2 * directions, tile_rows),
        measured_correlation.reshape(tiles * 2, tile_rows),
        keep_indicator,
        pairs,
        gains_t,
        duals_t,
        consensus_t,
    ]
    vmem, dma = pltpu.VMEM, pltpu.SemaphoreType.DMA
    f32, bf16, i32 = jnp.float32, jnp.bfloat16, jnp.int32
    result = pl.pallas_call(
        functools.partial(whole_kernel, chan_count, sub_count, half, groups),
        out_shape=pltpu.VMEM((2 * half + degree, 2, directions, LANES), f32),
        in_specs=[pl.BlockSpec(memory_space=pl.ANY)] * (len(operands) + 1),
        out_specs=pl.BlockSpec(memory_space=pltpu.VMEM),
        scratch_shapes=[pltpu.SMEM(rho.shape, f32)]
        + [vmem(x.shape, x.dtype) for x in operands]
        + [
            vmem((owners, 2, directions, LANES), f32),
            vmem((owners, 2, directions, LANES), jnp.int16),
            vmem((bases * half, 2 * tile_rows, LANES), bf16),
            vmem((LANES, tile_rows), f32),
            vmem((bases * half, 2, tile_rows), i32),
            vmem((2, tiles + 1, directions, tile_rows), f32),
            vmem((8 * 2 * directions, tile_rows), f32),
            vmem((2 * tiles + 8, tile_rows), f32),
            vmem((tiles + 8, tile_rows), i32),
            vmem((8, code_width), i32),
            pltpu.SMEM((8, code_width), i32),
            vmem((groups + 1, out_rows, LANES), f32),
            vmem((2, directions, LANES), f32),
            vmem((sub_count - 1, chan_count, coded, LANES), bf16),
            vmem((sub_count - 1, chan_count, coded, LANES), bf16),
            vmem((chan_count, coded, LANES), bf16),
            vmem((chan_count, coded, LANES), bf16),
            vmem((owners, 2 * directions, LANES), bf16),
            vmem((degree, owners, LANES), f32),
            dma((len(operands) + 2,)),
            dma((chan_count,)),
            dma((chan_count,)),
            dma((sub_count - 1, chan_count)),
            dma((sub_count - 1, chan_count)),
            dma((chan_count,)),
            dma((chan_count,)),
            dma((owners,)),
            dma((owners,)),
        ],
        compiler_params=pltpu.CompilerParams(
            collective_id=1, has_side_effects=True, vmem_limit_bytes=60 << 20
        ),
    )(rho, *operands)
    outputs = pl.pallas_call(
        deliver_kernel,
        out_shape=tuple(
            jax.ShapeDtypeStruct(x.shape, f32) for x in (duals_t, consensus_t, duals_t)
        ),
        in_specs=[pl.BlockSpec(memory_space=pltpu.VMEM)],
        out_specs=tuple(pl.BlockSpec(memory_space=pltpu.VMEM) for _ in range(3)),
    )(pltpu.with_memory_space_constraint(result, pltpu.VMEM))
    return tuple(jnp.swapaxes(x, 2, 3) for x in outputs)


def solution(mesh):
    placed = (
        P(("groups", "chan", "sub"), None, None, None),
        P(("groups", "chan", "sub"), None, None),
        P(("groups", "chan", "sub"), None),
        P(("groups", "chan", "sub"), None),
        P(("groups", "chan", "sub")),
        P(("groups", "chan", "sub")),
        P(),
        P(("groups", "chan"), None, None, None),
        P(("groups", "chan", "sub"), None, None, None),
        P("groups", None, None, None),
        P(),
    )
    return jax.shard_map(
        body,
        mesh=mesh,
        in_specs=placed,
        out_specs=(
            P(("groups", "chan", "sub"), None, None, None),
            P("groups", None, None, None),
            P(("groups", "chan", "sub"), None, None, None),
        ),
        check_vma=False,
    )
```
